32 devices in a mesh: geo: 4 (over x, core), comp: 8 (over z, y).
Axes of the slice: x: 2, y: 2, z: 4, core: 2. Of those that a mesh axis runs over, the one named last changes fastest.
Arguments:
- spectrum: bfloat16 [1152, 512, 128], P('comp', 'geo'), may hold values from 0.049804688 to 1
- land_mask: int32 [512, 128], P('geo'), may hold values 0 or 1
- wind_speed: float32 [512, 128], P('geo'), may hold values from 0.5 to 2
- wind_dir: float32 [512, 128], P('geo'), may hold values from -3.140625 to 3.140625
- input_rate: float32 [1152], P('comp'), may hold values from 0.05 to 0.5
- dissipation: float32 [1152], replicated, may hold values from 0.05 to 0.5
- pair_first: bfloat16 [1728, 1152], replicated, may hold values from -0.1875 to 0.1875
- pair_second: bfloat16 [1728, 1152], replicated, may hold values from -0.1875 to 0.1875
- merge_weight: bfloat16 [1152, 1728], replicated, may hold values from -0.15625 to 0.15625
Outputs:
- spectrum_next: bfloat16 [1152, 512, 128], P('comp', 'geo')
The draws below stay inside these ranges and needn't reach their ends.
All inputs are finite; a program needn't handle non-finite values. No bound on the sum of `land_mask` on one device may be relied on, other than what follows from the above.
Results may differ from the reference program's by a relative error of at most 0.0038.
Values may be sent and summed in bfloat16 or wider, within the bound.
A program may use at most 128 MiB of HBM per device.

```python
import math
import jax
import jax.numpy as jnp
from jax import lax

NF = 32
ND = 36
M = 1152
Q = 1728
X = 128
PROP_STEPS = 6
NY = 512


def place_ends(drawn, own_key, smallest, high):
    shape = drawn.shape
    index_at = [jax.random.randint(jax.random.fold_in(own_key, axis), (), 0, shape[axis]) for axis in range(len(shape))]
    drawn = drawn.at[tuple(index_at)].set(smallest)
    longest = shape.index(max(shape))
    index_at[longest] = (index_at[longest] + 1) % shape[longest]
    return drawn.at[tuple(index_at)].set(high)


def block_levels(key, shape, pieces, smallest, top_value):
    factor_of = 1.0
    for axis_at, blocks in pieces:
        draws = jax.random.uniform(jax.random.fold_in(jax.random.fold_in(key, 6), axis_at), (blocks,), jnp.float32, smallest / len(pieces), top_value / len(pieces))
        factor_of = factor_of * jnp.repeat(jnp.exp(draws), shape[axis_at] // blocks).reshape((-1,) + (1,) * (len(shape) - 1 - axis_at))
    return factor_of


def bell_draw(rng, shape, width, limit, kind=jnp.bfloat16):
    return jnp.clip(width * jax.random.normal(rng, shape, jnp.float32), -limit, limit).astype(kind)


def setup_inputs(seed: int = 0) -> dict:
    arg_keys = jax.random.split(jax.random.key(seed), 10)
    return {
        "spectrum": jnp.clip(jnp.exp(math.log(1.0) - 2.9996462 * jax.random.uniform(arg_keys[0], (M, NY, X), jnp.float32) ** block_levels(arg_keys[0], (M, NY, X), ((0, 8), (1, 4)), -0.2, 0.2)), 0.049804688, 1.0).astype(jnp.bfloat16),
        "land_mask": place_ends((jax.random.randint(arg_keys[1], (NY, X), 0, 4) < 3).astype(jnp.int32), jax.random.fold_in(arg_keys[1], 1), 0, 1),
        "wind_speed": jnp.clip(jnp.exp(math.log(2.0) - 1.3862944 * jax.random.uniform(arg_keys[2], (NY, X), jnp.float32) ** block_levels(arg_keys[2], (NY, X), ((0, 4),), -0.2, 0.2)), 0.5, 2.0),
        "wind_dir": jnp.clip(jax.random.uniform(arg_keys[3], (NY, X), jnp.float32, -3.140625, 3.140625), -3.140625, 3.140625),
        "input_rate": jnp.clip(jnp.exp(math.log(0.5) - 2.3025851 * jax.random.uniform(arg_keys[4], (M,), jnp.float32) ** block_levels(arg_keys[4], (M,), ((0, 8),), -0.2, 0.2)), 0.05, 0.5),
        "dissipation": jnp.clip(jnp.exp(jax.random.uniform(arg_keys[5], (M,), jnp.float32, math.log(0.05), math.log(0.5))), 0.05, 0.5),
        "pair_first": bell_draw(arg_keys[6], (Q, M), M ** -0.5, 0.1875),
        "pair_second": bell_draw(arg_keys[7], (Q, M), M ** -0.5, 0.1875),
        "merge_weight": bell_draw(arg_keys[8], (M, Q), Q ** -0.5, 0.15625),
    }


def upwind(padded, sea_mask, speed_x, speed_y):
    center = padded[:, 1:-1]
    lower = padded[:, :-2]
    upper = padded[:, 2:]
    western = jnp.roll(center, 1, axis=2)
    eastern = jnp.roll(center, -1, axis=2)
    change = jnp.maximum(speed_x, 0.0) * (center - western) + jnp.maximum(-speed_x, 0.0) * (center - eastern)
    change = change + jnp.maximum(speed_y, 0.0) * (center - lower) + jnp.maximum(-speed_y, 0.0) * (center - upper)
    return (center - change) * sea_mask

def speeds(comp_ids):
    frequency = (comp_ids // ND).astype(jnp.float32)
    heading = 2.0 * math.pi * (comp_ids % ND).astype(jnp.float32) / ND
    courant = 0.7 * jnp.power(jnp.float32(1.1), -frequency)
    speed_x = (courant * jnp.cos(heading))[:, None, None]
    speed_y = (courant * jnp.sin(heading))[:, None, None]
    return (heading, speed_x, speed_y)

def propagate(density, sea_mask, substeps):
    blocks = density.reshape(NF, ND, NY, X)

    def along(args):
        block, freq_index = args
        comp_ids = freq_index * ND + jnp.arange(ND, dtype=jnp.int32)
        heading, speed_x, speed_y = speeds(comp_ids)
        for repeat in range(substeps):
            padded = jnp.pad(block, ((0, 0), (1, 1), (0, 0)))
            block = upwind(padded, sea_mask, speed_x, speed_y)
        return block
    return lax.map(along, (blocks, jnp.arange(NF, dtype=jnp.int32))).reshape(M, NY, X)

def point_sources(spectra, dissipation, pair_first, pair_second, merge_weight):
    values = spectra.astype(jnp.float32)
    first_proj = jnp.dot(pair_first.astype(jnp.float32), values, precision=lax.Precision.HIGHEST)
    second_proj = jnp.dot(pair_second.astype(jnp.float32), values, precision=lax.Precision.HIGHEST)
    product = (first_proj * second_proj).astype(jnp.bfloat16)
    transfer = jnp.dot(merge_weight.astype(jnp.float32), product.astype(jnp.float32), precision=lax.Precision.HIGHEST)
    energy = lax.optimization_barrier(jnp.sum(values, axis=0))
    whitecap = -dissipation[:, None] * jnp.sqrt(energy / M + 1e-06)[None, :] * values
    return (transfer + whitecap).astype(jnp.bfloat16)

def reference(spectrum, land_mask, wind_speed, wind_dir, input_rate, dissipation, pair_first, pair_second, merge_weight):
    sea_mask = land_mask.astype(jnp.float32)
    density = propagate(spectrum.astype(jnp.float32), sea_mask, PROP_STEPS)
    outgoing = density.astype(jnp.bfloat16)
    groups = NY // 8
    stacked = outgoing.reshape(M, groups, 8 * X).transpose(1, 0, 2)
    increment = lax.map(lambda spectra: point_sources(spectra, dissipation, pair_first, pair_second, merge_weight), stacked)
    increment = increment.transpose(1, 0, 2).reshape(M, NY, X)
    heading, speed_x, speed_y = speeds(jnp.arange(M, dtype=jnp.int32))
    facing = jnp.maximum(jnp.cos(heading[:, None, None] - wind_dir[None]), 0.0)
    growth = input_rate[:, None, None] * wind_speed[None] * facing * facing
    density = density + growth * density + increment.astype(jnp.float32)
    density = propagate(density, sea_mask, 1)
    return density.astype(jnp.bfloat16)
```

```python
import functools
import math

import jax
import jax.numpy as jnp
from jax import lax
from jax.experimental import pallas as pl
from jax.experimental.pallas import tpu as pltpu
from jax.sharding import PartitionSpec as P

ND = 36
PROP_STEPS = 6
HALO = 8
SENDS = 3
RETURNS = 2
F32 = jnp.float32
BF16 = jnp.bfloat16
VMEM = pltpu.VMEM
ANY = pl.BlockSpec(memory_space=pl.ANY)
WHOLE = pl.BlockSpec(memory_space=pltpu.VMEM)
MESH = pl.DeviceIdType.MESH
DMA = pltpu.SemaphoreType.DMA
PAD = 16
CHUNK = 2
SMEM = pltpu.SMEM


def edges(cells, axis_dim):
    count = lax.axis_size("geo")
    ends = count - 1
    size = cells.shape[axis_dim]
    head = lax.slice_in_dim(cells, 0, HALO, axis=axis_dim)
    tail = lax.slice_in_dim(cells, size - HALO, size, axis=axis_dim)
    lower = lax.ppermute(tail, "geo", [(i, i + 1) for i in range(ends)])
    upper = lax.ppermute(head, "geo", [(i + 1, i) for i in range(ends)])
    return lower, upper


def block_of(comps):
    return 16 if comps % 16 == 0 else comps


def stride_of(block):
    return -(-block // 8) * 8


def upwind(v, mask, coef, at):
    center, west, east, south, north = (coef[at + k] for k in range(5))
    rows = v.shape[0]
    moved = west * pltpu.roll(v, 1, 1) + east * pltpu.roll(v, v.shape[1] - 1, 1)
    moved = moved + south * pltpu.roll(v, 1, 0) + north * pltpu.roll(v, rows - 1, 0)
    return (center * v + moved) * mask


def prop_kernel(coef, lower, cells, upper, mask, density, outgoing, turned):
    block, rows, cols = cells.shape
    stride = stride_of(block)
    first = pl.program_id(0) * block

    def one(c, carry):
        v = jnp.concatenate(
            [lower[c].astype(F32), cells[c].astype(F32), upper[c].astype(F32)], axis=0
        )
        sea = mask[...]
        for _ in range(PROP_STEPS):
            v = upwind(v, sea, coef, (first + c) * 8)
        density[c] = v
        turned[pl.ds(c, rows, stride=stride), :] = v[HALO : HALO + rows]
        return carry

    lax.fori_loop(0, block, one, 0)

    def pack(r, carry):
        start = pl.multiple_of(r * stride, 8)
        outgoing[r] = turned[pl.ds(start, block), :].astype(BF16)
        return carry

    lax.fori_loop(0, rows, pack, 0, unroll=8)


def propagate(coef, lower, cells, upper, mask):
    comps, rows, cols = cells.shape
    block = block_of(comps)
    tall = rows + 2 * HALO
    return pl.pallas_call(
        prop_kernel,
        grid=(comps // block,),
        in_specs=[
            pl.BlockSpec(memory_space=SMEM),
            pl.BlockSpec((block, HALO, cols), lambda i: (i, 0, 0)),
            pl.BlockSpec((block, rows, cols), lambda i: (i, 0, 0)),
            pl.BlockSpec((block, HALO, cols), lambda i: (i, 0, 0)),
            pl.BlockSpec((tall, cols), lambda i: (0, 0)),
        ],
        out_specs=[
            pl.BlockSpec((block, tall, cols), lambda i: (i, 0, 0)),
            pl.BlockSpec((rows, block, cols), lambda i: (0, i, 0)),
        ],
        out_shape=[
            jax.ShapeDtypeStruct((comps, tall, cols), F32),
            jax.ShapeDtypeStruct((rows, comps, cols), BF16),
        ],
        scratch_shapes=[VMEM((rows * stride_of(block), cols), F32)],
        cost_estimate=pl.CostEstimate(
            flops=comps * tall * cols * 100,
            bytes_accessed=comps * tall * cols * 8,
            transcendentals=0,
        ),
        name="propagate",
    )(coef, lower, cells, upper, mask)


def point_kernel(sends, *refs):
    near, far = refs[:sends], refs[sends : 2 * sends]
    loss, first, second, merge, out, spectra, product = refs[2 * sends :]
    peers, _, part, cols = near[0].shape
    local = sends * part
    comps, terms = merge.shape
    for side, group in enumerate((near, far)):
        lanes = slice(side * cols, (side + 1) * cols)
        for k in range(sends):
            for s in range(peers):
                at = s * local + k * part
                spectra[at : at + part, lanes] = group[k][s, 0]
    tile = max(t for t in range(16, 600, 16) if terms % t == 0)

    def multiply(t, carry):
        rows = pl.ds(pl.multiple_of(t * tile, 16), tile)
        x = spectra[...]
        one = jnp.dot(first[rows, :], x, preferred_element_type=F32)
        two = jnp.dot(second[rows, :], x, preferred_element_type=F32)
        product[rows, :] = (one * two).astype(BF16)
        return carry

    lax.fori_loop(0, terms // tile, multiply, 0)
    energy = jnp.sum(spectra[...].astype(F32), axis=0, keepdims=True)
    root = jnp.sqrt(energy / comps + 1e-06)
    if peers == 1:
        step = max(t for t in range(16, 600, 16) if comps % t == 0)
        for d in range(0, comps, step):
            rows = slice(d, d + step)
            moved = jnp.dot(merge[rows, :], product[...], preferred_element_type=F32)
            total = moved - loss[rows, :] * root * spectra[rows, :].astype(F32)
            out[0, 0, rows] = total[:, :cols].astype(BF16)
            out[0, 1, rows] = total[:, cols:].astype(BF16)
        return
    share = max(g for g in range(1, peers + 1) if peers % g == 0 and g * local <= 600)
    for d in range(0, peers, share):
        rows = slice(d * local, (d + share) * local)
        moved = jnp.dot(merge[rows, :], product[...], preferred_element_type=F32)
        total = moved - loss[rows, :] * root * spectra[rows, :].astype(F32)
        for g in range(share):
            piece = total[g * local : (g + 1) * local].astype(BF16)
            out[d + g, 0] = piece[:, :cols]
            out[d + g, 1] = piece[:, cols:]


def point_terms(chunks, start, pairs, loss, first, second, merge):
    sends = len(chunks)
    peers, rows, part, cols = chunks[0].shape
    local = sends * part
    comps, terms = merge.shape
    whole = lambda shape: pl.BlockSpec(shape, lambda i: (0, 0))
    near = pl.BlockSpec((peers, 1, part, cols), lambda i: (0, start + i, 0, 0))
    far = pl.BlockSpec((peers, 1, part, cols), lambda i: (0, rows - 1 - start - i, 0, 0))
    return pl.pallas_call(
        functools.partial(point_kernel, sends),
        grid=(pairs,),
        in_specs=[near] * sends
        + [far] * sends
        + [whole((comps, 1)), whole((terms, comps)), whole((terms, comps)), whole((comps, terms))],
        out_specs=pl.BlockSpec((peers, 2, local, cols), lambda i: (0, i, 0, 0)),
        out_shape=jax.ShapeDtypeStruct((peers, 2 * pairs, local, cols), BF16),
        scratch_shapes=[VMEM((comps, 2 * cols), BF16), VMEM((terms, 2 * cols), BF16)],
        cost_estimate=pl.CostEstimate(
            flops=pairs * 12 * comps * terms * cols,
            bytes_accessed=6 * comps * terms + pairs * 8 * comps * cols,
            transcendentals=0,
        ),
        compiler_params=pltpu.CompilerParams(vmem_limit_bytes=60 * 1024 * 1024),
        name="points",
    )(*chunks, *chunks, loss, first, second, merge)


def final_kernel(returns, coef, density, low_inc, high_inc, wind, mask, *refs):
    incs = refs[:returns]
    out, turned = refs[returns:]
    block, rows, cols = out.shape
    peers, held = incs[0].shape[:2]
    band = rows // peers
    stride = stride_of(block)
    first = pl.program_id(0) * block

    def place(s, carry):
        for k in range(returns):
            for j in range(held):
                a = k * (held // 2) + j // 2
                row = a if j % 2 == 0 else band - 1 - a
                at = pl.multiple_of((s * band + row) * stride, 8)
                turned[pl.ds(at, block), :] = incs[k][s, j].astype(F32)
        return carry

    lax.fori_loop(0, peers, place, 0)

    def one(c, carry):
        at = (first + c) * 8
        inc = jnp.concatenate(
            [low_inc[c], turned[pl.ds(c, rows, stride=stride), :], high_inc[c]], axis=0
        )
        v = density[c]
        facing = jnp.maximum(coef[at + 6] * wind[1] + coef[at + 7] * wind[2], 0.0)
        growth = coef[at + 5] * wind[0] * facing * facing
        v = v + growth * v + inc
        v = upwind(v, mask[...], coef, at)
        out[c] = v[HALO : HALO + rows].astype(BF16)
        return carry

    lax.fori_loop(0, block, one, 0)


def finish(coef, density, low_inc, high_inc, wind, mask, incs, lead):
    local, tall, cols = density.shape
    rows = tall - 2 * HALO
    block = block_of(local)
    peers, held = incs[0].shape[:2]
    return pl.pallas_call(
        functools.partial(final_kernel, len(incs)),
        grid=(local // block,),
        in_specs=[
            pl.BlockSpec(memory_space=SMEM),
            pl.BlockSpec((block, tall, cols), lambda i: (i, 0, 0)),
            pl.BlockSpec((block, HALO, cols), lambda i: (i, 0, 0)),
            pl.BlockSpec((block, HALO, cols), lambda i: (i, 0, 0)),
            pl.BlockSpec((3, tall, cols), lambda i: (0, 0, 0)),
            pl.BlockSpec((tall, cols), lambda i: (0, 0)),
        ]
        + [pl.BlockSpec((peers, held, block, cols), lambda i: (0, 0, i, 0))] * len(incs),
        out_specs=pl.BlockSpec((block, rows, cols), lambda i: (i, 0, 0)),
        out_shape=jax.ShapeDtypeStruct((local, rows, cols), BF16),
        scratch_shapes=[VMEM((rows * stride_of(block), cols), F32)],
        name="finish",
    )(coef, density, low_inc, high_inc, wind, mask, *incs)


def plain_body(spectrum, land_mask, wind_speed, wind_dir, input_rate, dissipation, pair_first, pair_second, merge_weight):
    local, rows, cols = spectrum.shape
    peers = lax.axis_size("comp")
    band = rows // peers
    ids = lax.axis_index("comp") * local + jnp.arange(local, dtype=jnp.int32)
    frequency = (ids // ND).astype(F32)
    heading = 2.0 * math.pi * (ids % ND).astype(F32) / ND
    courant = 0.7 * jnp.power(F32(1.1), -frequency)
    cos_h, sin_h = jnp.cos(heading), jnp.sin(heading)
    west, east = jnp.maximum(courant * cos_h, 0.0), jnp.maximum(-courant * cos_h, 0.0)
    south, north = jnp.maximum(courant * sin_h, 0.0), jnp.maximum(-courant * sin_h, 0.0)
    center = 1.0 - west - east - south - north
    coef = jnp.stack([center, west, east, south, north, input_rate, cos_h, sin_h], axis=1).reshape(-1)

    lower, upper = edges(spectrum, 1)
    fields = jnp.stack([wind_speed, jnp.cos(wind_dir), jnp.sin(wind_dir), land_mask.astype(F32)])
    low_f, high_f = edges(fields, 1)
    fields = jnp.concatenate([low_f, fields, high_f], axis=1)
    wind, mask = fields[:3], fields[3]

    whole_tiles = local % (16 * SENDS) == 0
    sends = SENDS if whole_tiles else 1
    part = local // sends
    density, chunks = [], []
    for k in range(sends):
        cut = slice(k * part, (k + 1) * part)
        d, out = propagate(coef[k * part * 8 : (k + 1) * part * 8], lower[cut], spectrum[cut], upper[cut], mask)
        density.append(d)
        out = out.reshape(peers, band, part, cols)
        chunks.append(lax.all_to_all(out, "comp", split_axis=0, concat_axis=0, tiled=True))
    density = jnp.concatenate(density, axis=0)

    loss = dissipation[:, None]
    if not whole_tiles:
        chunks = [c.transpose(1, 0, 2, 3).reshape(1, band, peers * local, cols) for c in chunks]
    returns = max(1, min(RETURNS, band // 2))
    pairs = band // 2 // returns
    incs = []
    for k in range(returns):
        inc = point_terms(chunks, k * pairs, pairs, loss, pair_first, pair_second, merge_weight)
        if not whole_tiles:
            inc = inc.reshape(2 * pairs, peers, local, cols).transpose(1, 0, 2, 3)
        incs.append(lax.all_to_all(inc, "comp", split_axis=0, concat_axis=0, tiled=True))
    count = lax.axis_size("geo")
    ends = count - 1
    low = lax.ppermute(incs[0][peers - 1, 1], "geo", [(i, i + 1) for i in range(ends)])
    high = lax.ppermute(incs[0][0, 0], "geo", [(i + 1, i) for i in range(ends)])
    low = jnp.pad(low.astype(F32)[:, None], ((0, 0), (HALO - 1, 0), (0, 0)))
    high = jnp.pad(high.astype(F32)[:, None], ((0, 0), (0, HALO - 1), (0, 0)))
    return finish(coef, density, low, high, wind, mask, incs, HALO)


def geo_halo_kernel(spectrum, mask, speed, angle, near, near_mask, near_speed, near_angle, send, recv):
    geo, ends = lax.axis_index("geo"), lax.axis_size("geo") - 1
    rows = spectrum.shape[1]
    barrier = pltpu.get_barrier_semaphore()
    has_low, has_high = geo > 0, geo < ends

    @pl.when(has_low)
    def _():
        pl.semaphore_signal(barrier, inc=1, device_id={"geo": geo - 1}, device_id_type=MESH)

    @pl.when(has_high)
    def _():
        pl.semaphore_signal(barrier, inc=1, device_id={"geo": geo + 1}, device_id_type=MESH)

    pl.semaphore_wait(barrier, jnp.minimum(geo, 1) + jnp.minimum(ends - geo, 1))

    def copies(side):
        at = pl.ds(0, HALO) if side else pl.ds(rows - HALO, HALO)
        to = {"geo": geo - 1} if side else {"geo": geo + 1}
        pairs = [
            (spectrum.at[:, at], near.at[side]),
            (mask.at[at], near_mask.at[side]),
            (speed.at[at], near_speed.at[side]),
            (angle.at[at], near_angle.at[side]),
        ]
        return [
            pltpu.make_async_remote_copy(
                src_ref=src, dst_ref=dst, send_sem=send.at[side, k], recv_sem=recv.at[side, k],
                device_id=to, device_id_type=MESH,
            )
            for k, (src, dst) in enumerate(pairs)
        ]

    down, up = copies(1), copies(0)

    @pl.when(has_low)
    def _():
        for c in down:
            c.start()

    @pl.when(has_high)
    def _():
        for c in up:
            c.start()

    for side, missing in ((0, geo == 0), (1, geo == ends)):

        @pl.when(missing)
        def _(side=side):
            for ref in (near, near_mask, near_speed, near_angle):
                ref[side] = jnp.zeros(ref.shape[1:], ref.dtype)

    @pl.when(has_low)
    def _():
        for c in down:
            c.wait_send()
        for c in up:
            c.wait_recv()

    @pl.when(has_high)
    def _():
        for c in up:
            c.wait_send()
        for c in down:
            c.wait_recv()


def geo_halo(spectrum, mask, speed, angle):
    comps, _, cols = spectrum.shape
    flat = lambda a: jax.ShapeDtypeStruct((2, HALO, cols), a.dtype)
    return pl.pallas_call(
        geo_halo_kernel,
        in_specs=[ANY] * 4,
        out_specs=[WHOLE] * 4,
        out_shape=[jax.ShapeDtypeStruct((2, comps, HALO, cols), spectrum.dtype), flat(mask), flat(speed), flat(angle)],
        scratch_shapes=[DMA((2, 4)), DMA((2, 4))],
        compiler_params=pltpu.CompilerParams(collective_id=1, has_side_effects=True),
        name="geo_halo",
    )(spectrum, mask, speed, angle)


def directions(comps, periodic):
    if not periodic:
        return True, True, True, True
    cos = [math.cos(2 * math.pi * c / ND) for c in comps]
    sin = [math.sin(2 * math.pi * c / ND) for c in comps]
    tiny = 1e-3
    south = any(s > -tiny and c % ND for s, c in zip(sin, comps))
    north = any(s < tiny and c % ND for s, c in zip(sin, comps))
    return any(c > -tiny for c in cos), any(c < tiny for c in cos), south, north


def march(cells, mask, coef, groups, ways, low, count, stride):
    west, east, south, north = ways
    cols = cells.shape[1]
    steps = PROP_STEPS
    lag = 2 if south and north else 1
    depth = 3 if lag == 2 else 2
    down = north and not south
    size = len(groups)
    factor = [[coef[k, pl.ds(g * 8, 8), :] for k in range(5)] for g in groups]
    span = count + 2 * steps if lag == 2 else count + steps
    first = low - steps if lag == 2 or not down else low
    last = first + span - 1
    trips = span + lag * steps
    unroll = 6 if lag == 2 else 4
    trips = -(-trips // unroll) * unroll

    def place(i):
        return last - i if down else first + i

    def one(i, state):
        fresh = []
        for j, g in enumerate(groups):
            levels = state[j]
            c, w, e, s, n = factor[j]
            made = [cells[pl.ds(pl.multiple_of(place(i) * stride + g * 8, 8), 8), :]]
            for k in range(1, steps + 1):
                past = levels[k - 1]
                here = past[0] if lag == 1 else past[1]
                v = c * here
                if west:
                    v = v + w * pltpu.roll(here, 1, 1)
                if east:
                    v = v + e * pltpu.roll(here, cols - 1, 1)
                if lag == 2:
                    v = v + s * past[2] + n * past[0]
                elif south:
                    v = v + s * past[1]
                elif north:
                    v = v + n * past[1]
                made.append(v * mask[place(i - lag * k)])
            at = pl.multiple_of(place(i - lag * steps) * stride + g * 8, 8)
            cells[pl.ds(at, 8), :] = made[steps]
            fresh.append(tuple((made[k],) + levels[k][:-1] for k in range(steps)))
        return tuple(fresh)

    zero = jnp.zeros((8, cols), F32)
    start = tuple(tuple((zero,) * depth for _ in range(steps)) for _ in range(size))

    def several(t, state):
        for u in range(unroll):
            state = one(t * unroll + u, state)
        return state

    lax.fori_loop(0, trips // unroll, several, start)


def spread_kernel(periodic, spectrum, near, mask, coef, density, tiles, staged, cells, packed, sems, out_sems):
    comps, rows, cols = staged.shape
    stride = stride_of(comps) + 8
    block = 16
    blocks = comps // block
    bands = out_sems.shape[0] - 1
    band = rows // bands

    def fetch(b):
        at = pl.ds(b * block, block)
        return pltpu.make_async_copy(spectrum.at[at], staged.at[at], sems.at[b])

    for b in range(blocks):
        fetch(b).start()

    def turn(b, carry):
        fetch(b).wait()

        def one(k, carry):
            c = b * block + k
            v = jnp.concatenate([near[0, c].astype(F32), staged[c].astype(F32), near[1, c].astype(F32)], axis=0)
            cells[pl.ds(PAD * stride + c, rows + 2 * HALO, stride=stride), :] = v
            return carry

        return lax.fori_loop(0, block, one, carry)

    lax.fori_loop(0, blocks, turn, 0)

    low = PAD + HALO - 1
    groups = comps // 8
    half = groups // 2 if groups % 2 == 0 else 0
    for g in range(half if half else groups):
        pair = [g, g + half] if half else [g]
        ways = directions([8 * p + k for p in pair for k in range(8)], periodic)
        march(cells, mask, coef, pair, ways, low, rows + 2, stride)

    whole = pltpu.make_async_copy(
        cells.at[pl.ds(low * stride, (rows + 2) * stride)], density, out_sems.at[bands]
    )
    whole.start()

    def give(b):
        at = pl.ds(b * band, band)
        return pltpu.make_async_copy(packed.at[at], tiles.at[at], out_sems.at[b])

    def pack(b, carry):
        def one(k, carry):
            t = b * band + k
            row = jnp.where(t == 0, 0, jnp.where(t == 1, rows - 1, t - 1))
            at = pl.multiple_of((PAD + HALO + row) * stride, 8)
            packed[t] = cells[pl.ds(at, comps), :].astype(BF16)
            return carry

        lax.fori_loop(0, band, one, 0)
        give(b).start()
        return carry

    lax.fori_loop(0, bands, pack, 0)

    def drain(b, carry):
        give(b).wait()
        return carry

    lax.fori_loop(0, bands, drain, 0)
    whole.wait()


def spread(spectrum, near, mask, coef, periodic):
    comps, rows, cols = spectrum.shape
    stride = stride_of(comps) + 8
    bands = 8 if rows % 8 == 0 else 1
    return pl.pallas_call(
        functools.partial(spread_kernel, periodic),
        in_specs=[ANY, WHOLE, WHOLE, WHOLE],
        out_specs=[ANY, ANY],
        out_shape=[
            jax.ShapeDtypeStruct(((rows + 2) * stride, cols), F32),
            jax.ShapeDtypeStruct((rows, comps, cols), BF16),
        ],
        scratch_shapes=[
            VMEM((comps, rows, cols), BF16),
            VMEM(((rows + 2 * HALO + 2 * PAD) * stride, cols), F32),
            VMEM((rows, comps, cols), BF16),
            DMA((comps // 16,)),
            DMA((bands + 1,)),
        ],
        compiler_params=pltpu.CompilerParams(vmem_limit_bytes=48 * 1024 * 1024),
        name="spread",
    )(spectrum, near, mask, coef)


def partner(me, k, peers):
    if peers & (peers - 1):
        return lax.rem(me + k, peers)
    other, bit = me, 1
    while bit < peers:
        if k & bit:
            other = other + bit - 2 * bit * lax.rem(lax.div(other, bit), 2)
        bit *= 2
    return other


def exchange_kernel(
    order, tiles, loss, first_in, second_in, merge_in, back, edge,
    spectra, incs, first, second, merge, product,
    weight_sems, send_sem, recv_sem, return_sem, back_sem, edge_send, edge_recv,
):
    peers = lax.axis_size("comp")
    me = lax.axis_index("comp")
    geo, ends = lax.axis_index("geo"), lax.axis_size("geo") - 1
    chunks, width, comps, cols = spectra.shape
    local = comps // peers
    terms = product.shape[0]
    has_low, has_high = geo > 0, geo < ends

    barrier = pltpu.get_barrier_semaphore()
    for k in range(1, peers):
        pl.semaphore_signal(barrier, inc=1, device_id={"comp": partner(me, k, peers)}, device_id_type=MESH)

    @pl.when(has_low)
    def _():
        pl.semaphore_signal(barrier, inc=1, device_id={"geo": geo - 1}, device_id_type=MESH)

    @pl.when(has_high)
    def _():
        pl.semaphore_signal(barrier, inc=1, device_id={"geo": geo + 1}, device_id_type=MESH)

    pl.semaphore_wait(barrier, peers - 1 + jnp.minimum(geo, 1) + jnp.minimum(ends - geo, 1))

    def part(who):
        return pl.ds(pl.multiple_of(who * local, 16), local)

    def outward(c, who):
        return pltpu.make_async_remote_copy(
            src_ref=tiles.at[pl.ds(c * width, width), who],
            dst_ref=spectra.at[c, :, part(me)],
            send_sem=send_sem, recv_sem=recv_sem.at[c],
            device_id={"comp": who}, device_id_type=MESH,
        )

    def homeward(c, who):
        return pltpu.make_async_remote_copy(
            src_ref=incs.at[c, :, part(who)],
            dst_ref=back.at[pl.ds(c * width, width), me],
            send_sem=return_sem, recv_sem=back_sem.at[c],
            device_id={"comp": who}, device_id_type=MESH,
        )

    def own_out(c):
        return pltpu.make_async_copy(tiles.at[pl.ds(c * width, width), me], spectra.at[c, :, part(me)], recv_sem.at[c])

    def own_home(c):
        return pltpu.make_async_copy(incs.at[c, :, part(me)], back.at[pl.ds(c * width, width), me], back_sem.at[c])

    for group in order:

        def launch(c, carry, group=group):
            for k in group:
                outward(c, partner(me, k, peers)).start()
            return carry

        lax.fori_loop(0, chunks, launch, 0)

    def launch_own(c, carry):
        own_out(c).start()
        return carry

    lax.fori_loop(0, chunks, launch_own, 0)
    loads = [
        pltpu.make_async_copy(src, dst, weight_sems.at[k])
        for k, (src, dst) in enumerate(((first_in, first), (second_in, second), (merge_in, merge)))
    ]
    for load in loads:
        load.start()
    for load in loads:
        load.wait()

    tile = max(t for t in range(16, 600, 16) if terms % t == 0)
    step = max(g for g in range(1, peers + 1) if peers % g == 0 and g * local <= 600) * local

    def work(c, carry):
        pltpu.make_async_copy(spectra.at[c], spectra.at[c], recv_sem.at[c]).wait()

        def both():
            return jnp.concatenate([spectra[c, h] for h in range(width)], axis=1)

        def multiply(t, carry):
            rows = pl.ds(pl.multiple_of(t * tile, 16), tile)
            x = both()
            one = jnp.dot(first[rows, :], x, preferred_element_type=F32)
            two = jnp.dot(second[rows, :], x, preferred_element_type=F32)
            product[rows, :] = (one * two).astype(BF16)
            return carry

        lax.fori_loop(0, terms // tile, multiply, 0)
        roots = []
        for h in range(width):
            energy = jnp.sum(spectra[c, h].astype(F32), axis=0, keepdims=True)
            roots.append(jnp.sqrt(energy / comps + 1e-06))
        for d in range(0, comps, step):
            rows = slice(d, d + step)
            moved = jnp.dot(merge[rows, :], product[...], preferred_element_type=F32)
            for h in range(width):
                lanes = slice(h * cols, (h + 1) * cols)
                total = moved[:, lanes] - loss[rows, :] * roots[h] * spectra[c, h, rows, :].astype(F32)
                incs[c, h, rows, :] = total.astype(BF16)
        for group in order:
            for k in group:
                homeward(c, partner(me, k, peers)).start()
        own_home(c).start()
        return carry

    lax.fori_loop(0, chunks, work, 0)

    def landed(c):
        there = back.at[pl.ds(c * width, width)]
        pltpu.make_async_copy(there, there, back_sem.at[c]).wait()

    landed(0)
    to_low = pltpu.make_async_remote_copy(
        src_ref=back.at[0, 0], dst_ref=edge.at[1], send_sem=edge_send.at[1], recv_sem=edge_recv.at[1],
        device_id={"geo": geo - 1}, device_id_type=MESH,
    )
    to_high = pltpu.make_async_remote_copy(
        src_ref=back.at[0, 1], dst_ref=edge.at[0], send_sem=edge_send.at[0], recv_sem=edge_recv.at[0],
        device_id={"geo": geo + 1}, device_id_type=MESH,
    )

    @pl.when(has_low)
    def _():
        to_low.start()

    @pl.when(has_high)
    def _():
        to_high.start()

    def rest(c, carry):
        landed(c)
        return carry

    lax.fori_loop(1, chunks, rest, 0)

    @pl.when(has_low)
    def _():
        to_low.wait_send()
        to_high.wait_recv()

    @pl.when(has_high)
    def _():
        to_high.wait_send()
        to_low.wait_recv()

    def sent(c, carry):
        for k in range(1, peers):
            outward(c, partner(me, k, peers)).wait_send()
            homeward(c, partner(me, k, peers)).wait_send()
        return carry

    lax.fori_loop(0, chunks, sent, 0)


def exchange(tiles, loss, first, second, merge):
    rows, local, cols = tiles.shape
    peers = lax.axis_size("comp")
    depth = rows // peers
    chunks = depth // CHUNK
    comps, terms = merge.shape
    tiles = tiles.reshape(depth, peers, local, cols)
    if peers == 8:
        order = [(1, 2, 3), (4, 5, 6, 7)]
    else:
        order = [tuple(range(1, peers))]
    return pl.pallas_call(
        functools.partial(exchange_kernel, order),
        in_specs=[ANY, WHOLE, ANY, ANY, ANY],
        out_specs=[ANY, ANY],
        out_shape=[
            jax.ShapeDtypeStruct((depth, peers, local, cols), BF16),
            jax.ShapeDtypeStruct((2, local, cols), BF16),
        ],
        scratch_shapes=[
            VMEM((chunks, CHUNK, comps, cols), BF16),
            VMEM((chunks, CHUNK, comps, cols), BF16),
            VMEM((terms, comps), BF16),
            VMEM((terms, comps), BF16),
            VMEM((comps, terms), BF16),
            VMEM((terms, CHUNK * cols), BF16),
            DMA((3,)),
            DMA,
            DMA((chunks,)),
            DMA,
            DMA((chunks,)),
            DMA((2,)),
            DMA((2,)),
        ],
        cost_estimate=pl.CostEstimate(
            flops=6 * comps * terms * depth * cols, bytes_accessed=6 * comps * terms, transcendentals=0
        ),
        compiler_params=pltpu.CompilerParams(
            collective_id=2, has_side_effects=True, vmem_limit_bytes=60 * 1024 * 1024
        ),
        name="exchange",
    )(tiles, loss, first, second, merge)


def close_kernel(periodic, ends, density, back, edge, wind, mask, coef, out, cells, incs, staged, sems, out_sems):
    comps, rows, cols = staged.shape
    stride = cells.shape[0] // (rows + 2)
    block = 16
    blocks = comps // block
    turned = cells.reshape(rows + 2, stride, cols)
    source = density.reshape(rows + 2, stride, cols)

    def fetches(b):
        at = pl.ds(pl.multiple_of(b * block, block), block)
        moves = [
            (source.at[:, at], turned.at[:, at]),
            (edge.at[0, at], incs.at[0, at]),
            (back.at[0, at], incs.at[1, at]),
            (back.at[pl.ds(2, rows - 2), at], incs.at[pl.ds(2, rows - 2), at]),
            (back.at[1, at], incs.at[rows, at]),
            (edge.at[1, at], incs.at[rows + 1, at]),
        ]
        return [pltpu.make_async_copy(src, dst, sems.at[b, k]) for k, (src, dst) in enumerate(moves)]

    def give(b):
        at = pl.ds(b * block, block)
        return pltpu.make_async_copy(staged.at[at], out.at[at], out_sems.at[b])

    for b in range(blocks):
        for f in fetches(b):
            f.start()

    for b in range(blocks):
        for f in fetches(b):
            f.wait()
        span = slice(b * block, (b + 1) * block)
        for side, at in ((0, 0), (1, rows + 1)):

            @pl.when(ends[side] == 1)
            def _(at=at, span=span):
                incs[at, span, :] = jnp.zeros((block, cols), BF16)

        pair = [2 * b, 2 * b + 1]
        ways = [directions([8 * g + k for k in range(8)], periodic) for g in pair]
        factor = [[coef[k, pl.ds(g * 8, 8), :] for k in range(8)] for g in pair]

        def one(i, state):
            both = incs[i, span, :].astype(F32)
            blow, turn_x, turn_y = wind[0, i], wind[1, i], wind[2, i]
            sea = mask[i - 1]
            fresh = []
            for j, g in enumerate(pair):
                c, w, e, s, n, rate, cos_h, sin_h = factor[j]
                west, east, south, north = ways[j]
                here, past = state[j]
                at = pl.multiple_of(i * stride + g * 8, 8)
                d = cells[pl.ds(at, 8), :]
                facing = jnp.maximum(cos_h * turn_x + sin_h * turn_y, 0.0)
                growth = rate * blow * (facing * facing)
                new = d + growth * d + both[j * 8 : (j + 1) * 8]
                v = c * here
                if west:
                    v = v + w * pltpu.roll(here, 1, 1)
                if east:
                    v = v + e * pltpu.roll(here, cols - 1, 1)
                if south:
                    v = v + s * past
                if north:
                    v = v + n * new
                back_at = pl.multiple_of((i - 1) * stride + g * 8, 8)
                cells[pl.ds(back_at, 8), :] = v * sea
                fresh.append((new, here))
            return tuple(fresh)

        def first(i):
            both = incs[i, span, :].astype(F32)
            made = []
            for j, g in enumerate(pair):
                rate, cos_h, sin_h = factor[j][5:8]
                d = cells[pl.ds(i * stride + g * 8, 8), :]
                facing = jnp.maximum(cos_h * wind[1, i] + sin_h * wind[2, i], 0.0)
                growth = rate * wind[0, i] * (facing * facing)
                made.append((d + growth * d + both[j * 8 : (j + 1) * 8], jnp.zeros((8, cols), F32)))
            return tuple(made)

        def two(t, state):
            return one(2 * t + 2, one(2 * t + 1, state))

        state = lax.fori_loop(0, (rows + 1) // 2, two, first(0))
        if (rows + 1) % 2:
            one(rows + 1, state)

    def finish_block(b, carry):
        def lift(k, carry):
            c = b * block + k
            staged[c] = cells[pl.ds(stride + c, rows, stride=stride), :].astype(BF16)
            return carry

        lax.fori_loop(0, block, lift, 0)
        give(b).start()
        return carry

    lax.fori_loop(0, blocks, finish_block, 0)

    def drain(b, carry):
        give(b).wait()
        return carry

    lax.fori_loop(0, blocks, drain, 0)


def close(density, back, edge, wind, mask, coef, ends, periodic):
    rows, comps, cols = back.shape
    stride = stride_of(comps) + 8
    return pl.pallas_call(
        functools.partial(close_kernel, periodic),
        in_specs=[pl.BlockSpec(memory_space=SMEM), ANY, ANY, ANY, WHOLE, WHOLE, WHOLE],
        out_specs=ANY,
        out_shape=jax.ShapeDtypeStruct((comps, rows, cols), BF16),
        scratch_shapes=[
            VMEM(((rows + 2) * stride, cols), F32),
            VMEM((rows + 2, comps, cols), BF16),
            VMEM((comps, rows, cols), BF16),
            DMA((comps // 16, 6)),
            DMA((comps // 16,)),
        ],
        compiler_params=pltpu.CompilerParams(vmem_limit_bytes=48 * 1024 * 1024),
        name="close",
    )(ends, density, back, edge, wind, mask, coef)


def tall(rows_of, lead):
    rows_of = jnp.pad(rows_of, ((lead, lead), (0, 0)))
    return jnp.broadcast_to(rows_of[:, None, :], (rows_of.shape[0], 8, rows_of.shape[1]))


def body(spectrum, land_mask, wind_speed, wind_dir, input_rate, dissipation, pair_first, pair_second, merge_weight):
    local, rows, cols = spectrum.shape
    peers = lax.axis_size("comp")
    fits = local % 16 == 0 and rows % (peers * CHUNK) == 0 and rows % 16 == 0 and cols == 128
    if not fits:
        return plain_body(
            spectrum, land_mask, wind_speed, wind_dir, input_rate, dissipation, pair_first, pair_second, merge_weight
        )
    periodic = local % ND == 0
    near, near_mask, near_speed, near_angle = geo_halo(spectrum, land_mask, wind_speed, wind_dir)

    ids = lax.axis_index("comp") * local + jnp.arange(local, dtype=jnp.int32)
    frequency = (ids // ND).astype(F32)
    heading = 2.0 * math.pi * (ids % ND).astype(F32) / ND
    courant = 0.7 * jnp.power(F32(1.1), -frequency)
    cos_h, sin_h = jnp.cos(heading), jnp.sin(heading)
    west, east = jnp.maximum(courant * cos_h, 0.0), jnp.maximum(-courant * cos_h, 0.0)
    south, north = jnp.maximum(courant * sin_h, 0.0), jnp.maximum(-courant * sin_h, 0.0)
    center = 1.0 - west - east - south - north
    coef = jnp.stack([center, west, east, south, north, input_rate, cos_h, sin_h])
    coef = jnp.broadcast_to(coef[:, :, None], (8, local, cols))

    sea = jnp.concatenate([near_mask[0], land_mask, near_mask[1]]).astype(F32)
    sea = tall(sea, PAD)
    angle = jnp.concatenate([near_angle[0, HALO - 1 :], wind_dir, near_angle[1, :1]])
    speed = jnp.concatenate([near_speed[0, HALO - 1 :], wind_speed, near_speed[1, :1]])
    wind = jnp.stack([tall(speed, 0), tall(jnp.cos(angle), 0), tall(jnp.sin(angle), 0)])
    geo = lax.axis_index("geo")
    ends = jnp.stack([geo == 0, geo == lax.axis_size("geo") - 1]).astype(jnp.int32)

    density, tiles = spread(spectrum, near, sea, coef, periodic)
    back, edge = exchange(tiles, dissipation[:, None], pair_first, pair_second, merge_weight)
    below = PAD + HALO - 1
    return close(density, back.reshape(rows, local, cols), edge, wind, sea[below : below + rows + 2], coef, ends, periodic)


def solution(mesh):
    placed = (P("comp", "geo", None), P("geo", None), P("geo", None), P("geo", None), P("comp"), P(), P(), P(), P())
    return jax.shard_map(
        body, mesh=mesh, in_specs=placed, out_specs=P("comp", "geo", None), check_vma=False
    )
```

```python
import functools
import math

import jax
import jax.numpy as jnp
from jax import lax
from jax.experimental import pallas as pl
from jax.experimental.pallas import tpu as pltpu
from jax.sharding import PartitionSpec as P

ND = 36
PROP_STEPS = 6
HALO = 8
SENDS = 3
RETURNS = 2
F32 = jnp.float32
BF16 = jnp.bfloat16
VMEM = pltpu.VMEM
ANY = pl.BlockSpec(memory_space=pl.ANY)
WHOLE = pl.BlockSpec(memory_space=pltpu.VMEM)
MESH = pl.DeviceIdType.MESH
DMA = pltpu.SemaphoreType.DMA
CHUNK = 2
BAND = 32
RUN = 12
SPAN = BAND + 2 * HALO
SMEM = pltpu.SMEM


def edges(cells, axis_dim):
    count = lax.axis_size("geo")
    ends = count - 1
    size = cells.shape[axis_dim]
    head = lax.slice_in_dim(cells, 0, HALO, axis=axis_dim)
    tail = lax.slice_in_dim(cells, size - HALO, size, axis=axis_dim)
    lower = lax.ppermute(tail, "geo", [(i, i + 1) for i in range(ends)])
    upper = lax.ppermute(head, "geo", [(i + 1, i) for i in range(ends)])
    return lower, upper


def block_of(comps):
    return 16 if comps % 16 == 0 else comps


def stride_of(block):
    return -(-block // 8) * 8


def upwind(v, mask, coef, at):
    center, west, east, south, north = (coef[at + k] for k in range(5))
    rows = v.shape[0]
    moved = west * pltpu.roll(v, 1, 1) + east * pltpu.roll(v, v.shape[1] - 1, 1)
    moved = moved + south * pltpu.roll(v, 1, 0) + north * pltpu.roll(v, rows - 1, 0)
    return (center * v + moved) * mask


def prop_kernel(coef, lower, cells, upper, mask, density, outgoing, turned):
    block, rows, cols = cells.shape
    stride = stride_of(block)
    first = pl.program_id(0) * block

    def one(c, carry):
        v = jnp.concatenate(
            [lower[c].astype(F32), cells[c].astype(F32), upper[c].astype(F32)], axis=0
        )
        sea = mask[...]
        for _ in range(PROP_STEPS):
            v = upwind(v, sea, coef, (first + c) * 8)
        density[c] = v
        turned[pl.ds(c, rows, stride=stride), :] = v[HALO : HALO + rows]
        return carry

    lax.fori_loop(0, block, one, 0)

    def pack(r, carry):
        start = pl.multiple_of(r * stride, 8)
        outgoing[r] = turned[pl.ds(start, block), :].astype(BF16)
        return carry

    lax.fori_loop(0, rows, pack, 0, unroll=8)


def propagate(coef, lower, cells, upper, mask):
    comps, rows, cols = cells.shape
    block = block_of(comps)
    tall = rows + 2 * HALO
    return pl.pallas_call(
        prop_kernel,
        grid=(comps // block,),
        in_specs=[
            pl.BlockSpec(memory_space=SMEM),
            pl.BlockSpec((block, HALO, cols), lambda i: (i, 0, 0)),
            pl.BlockSpec((block, rows, cols), lambda i: (i, 0, 0)),
            pl.BlockSpec((block, HALO, cols), lambda i: (i, 0, 0)),
            pl.BlockSpec((tall, cols), lambda i: (0, 0)),
        ],
        out_specs=[
            pl.BlockSpec((block, tall, cols), lambda i: (i, 0, 0)),
            pl.BlockSpec((rows, block, cols), lambda i: (0, i, 0)),
        ],
        out_shape=[
            jax.ShapeDtypeStruct((comps, tall, cols), F32),
            jax.ShapeDtypeStruct((rows, comps, cols), BF16),
        ],
        scratch_shapes=[VMEM((rows * stride_of(block), cols), F32)],
        cost_estimate=pl.CostEstimate(
            flops=comps * tall * cols * 100,
            bytes_accessed=comps * tall * cols * 8,
            transcendentals=0,
        ),
        name="propagate",
    )(coef, lower, cells, upper, mask)


def point_kernel(sends, *refs):
    near, far = refs[:sends], refs[sends : 2 * sends]
    loss, first, second, merge, out, spectra, product = refs[2 * sends :]
    peers, _, part, cols = near[0].shape
    local = sends * part
    comps, terms = merge.shape
    for side, group in enumerate((near, far)):
        lanes = slice(side * cols, (side + 1) * cols)
        for k in range(sends):
            for s in range(peers):
                at = s * local + k * part
                spectra[at : at + part, lanes] = group[k][s, 0]
    tile = max(t for t in range(16, 600, 16) if terms % t == 0)

    def multiply(t, carry):
        rows = pl.ds(pl.multiple_of(t * tile, 16), tile)
        x = spectra[...]
        one = jnp.dot(first[rows, :], x, preferred_element_type=F32)
        two = jnp.dot(second[rows, :], x, preferred_element_type=F32)
        product[rows, :] = (one * two).astype(BF16)
        return carry

    lax.fori_loop(0, terms // tile, multiply, 0)
    energy = jnp.sum(spectra[...].astype(F32), axis=0, keepdims=True)
    root = jnp.sqrt(energy / comps + 1e-06)
    if peers == 1:
        step = max(t for t in range(16, 600, 16) if comps % t == 0)
        for d in range(0, comps, step):
            rows = slice(d, d + step)
            moved = jnp.dot(merge[rows, :], product[...], preferred_element_type=F32)
            total = moved - loss[rows, :] * root * spectra[rows, :].astype(F32)
            out[0, 0, rows] = total[:, :cols].astype(BF16)
            out[0, 1, rows] = total[:, cols:].astype(BF16)
        return
    share = max(g for g in range(1, peers + 1) if peers % g == 0 and g * local <= 600)
    for d in range(0, peers, share):
        rows = slice(d * local, (d + share) * local)
        moved = jnp.dot(merge[rows, :], product[...], preferred_element_type=F32)
        total = moved - loss[rows, :] * root * spectra[rows, :].astype(F32)
        for g in range(share):
            piece = total[g * local : (g + 1) * local].astype(BF16)
            out[d + g, 0] = piece[:, :cols]
            out[d + g, 1] = piece[:, cols:]


def point_terms(chunks, start, pairs, loss, first, second, merge):
    sends = len(chunks)
    peers, rows, part, cols = chunks[0].shape
    local = sends * part
    comps, terms = merge.shape
    whole = lambda shape: pl.BlockSpec(shape, lambda i: (0, 0))
    near = pl.BlockSpec((peers, 1, part, cols), lambda i: (0, start + i, 0, 0))
    far = pl.BlockSpec((peers, 1, part, cols), lambda i: (0, rows - 1 - start - i, 0, 0))
    return pl.pallas_call(
        functools.partial(point_kernel, sends),
        grid=(pairs,),
        in_specs=[near] * sends
        + [far] * sends
        + [whole((comps, 1)), whole((terms, comps)), whole((terms, comps)), whole((comps, terms))],
        out_specs=pl.BlockSpec((peers, 2, local, cols), lambda i: (0, i, 0, 0)),
        out_shape=jax.ShapeDtypeStruct((peers, 2 * pairs, local, cols), BF16),
        scratch_shapes=[VMEM((comps, 2 * cols), BF16), VMEM((terms, 2 * cols), BF16)],
        cost_estimate=pl.CostEstimate(
            flops=pairs * 12 * comps * terms * cols,
            bytes_accessed=6 * comps * terms + pairs * 8 * comps * cols,
            transcendentals=0,
        ),
        compiler_params=pltpu.CompilerParams(vmem_limit_bytes=60 * 1024 * 1024),
        name="points",
    )(*chunks, *chunks, loss, first, second, merge)


def final_kernel(returns, coef, density, low_inc, high_inc, wind, mask, *refs):
    incs = refs[:returns]
    out, turned = refs[returns:]
    block, rows, cols = out.shape
    peers, held = incs[0].shape[:2]
    band = rows // peers
    stride = stride_of(block)
    first = pl.program_id(0) * block

    def place(s, carry):
        for k in range(returns):
            for j in range(held):
                a = k * (held // 2) + j // 2
                row = a if j % 2 == 0 else band - 1 - a
                at = pl.multiple_of((s * band + row) * stride, 8)
                turned[pl.ds(at, block), :] = incs[k][s, j].astype(F32)
        return carry

    lax.fori_loop(0, peers, place, 0)

    def one(c, carry):
        at = (first + c) * 8
        inc = jnp.concatenate(
            [low_inc[c], turned[pl.ds(c, rows, stride=stride), :], high_inc[c]], axis=0
        )
        v = density[c]
        facing = jnp.maximum(coef[at + 6] * wind[1] + coef[at + 7] * wind[2], 0.0)
        growth = coef[at + 5] * wind[0] * facing * facing
        v = v + growth * v + inc
        v = upwind(v, mask[...], coef, at)
        out[c] = v[HALO : HALO + rows].astype(BF16)
        return carry

    lax.fori_loop(0, block, one, 0)


def finish(coef, density, low_inc, high_inc, wind, mask, incs, lead):
    local, tall, cols = density.shape
    rows = tall - 2 * HALO
    block = block_of(local)
    peers, held = incs[0].shape[:2]
    return pl.pallas_call(
        functools.partial(final_kernel, len(incs)),
        grid=(local // block,),
        in_specs=[
            pl.BlockSpec(memory_space=SMEM),
            pl.BlockSpec((block, tall, cols), lambda i: (i, 0, 0)),
            pl.BlockSpec((block, HALO, cols), lambda i: (i, 0, 0)),
            pl.BlockSpec((block, HALO, cols), lambda i: (i, 0, 0)),
            pl.BlockSpec((3, tall, cols), lambda i: (0, 0, 0)),
            pl.BlockSpec((tall, cols), lambda i: (0, 0)),
        ]
        + [pl.BlockSpec((peers, held, block, cols), lambda i: (0, 0, i, 0))] * len(incs),
        out_specs=pl.BlockSpec((block, rows, cols), lambda i: (i, 0, 0)),
        out_shape=jax.ShapeDtypeStruct((local, rows, cols), BF16),
        scratch_shapes=[VMEM((rows * stride_of(block), cols), F32)],
        name="finish",
    )(coef, density, low_inc, high_inc, wind, mask, *incs)


def plain_body(spectrum, land_mask, wind_speed, wind_dir, input_rate, dissipation, pair_first, pair_second, merge_weight):
    local, rows, cols = spectrum.shape
    peers = lax.axis_size("comp")
    band = rows // peers
    ids = lax.axis_index("comp") * local + jnp.arange(local, dtype=jnp.int32)
    frequency = (ids // ND).astype(F32)
    heading = 2.0 * math.pi * (ids % ND).astype(F32) / ND
    courant = 0.7 * jnp.power(F32(1.1), -frequency)
    cos_h, sin_h = jnp.cos(heading), jnp.sin(heading)
    west, east = jnp.maximum(courant * cos_h, 0.0), jnp.maximum(-courant * cos_h, 0.0)
    south, north = jnp.maximum(courant * sin_h, 0.0), jnp.maximum(-courant * sin_h, 0.0)
    center = 1.0 - west - east - south - north
    coef = jnp.stack([center, west, east, south, north, input_rate, cos_h, sin_h], axis=1).reshape(-1)

    lower, upper = edges(spectrum, 1)
    fields = jnp.stack([wind_speed, jnp.cos(wind_dir), jnp.sin(wind_dir), land_mask.astype(F32)])
    low_f, high_f = edges(fields, 1)
    fields = jnp.concatenate([low_f, fields, high_f], axis=1)
    wind, mask = fields[:3], fields[3]

    whole_tiles = local % (16 * SENDS) == 0
    sends = SENDS if whole_tiles else 1
    part = local // sends
    density, chunks = [], []
    for k in range(sends):
        cut = slice(k * part, (k + 1) * part)
        d, out = propagate(coef[k * part * 8 : (k + 1) * part * 8], lower[cut], spectrum[cut], upper[cut], mask)
        density.append(d)
        out = out.reshape(peers, band, part, cols)
        chunks.append(lax.all_to_all(out, "comp", split_axis=0, concat_axis=0, tiled=True))
    density = jnp.concatenate(density, axis=0)

    loss = dissipation[:, None]
    if not whole_tiles:
        chunks = [c.transpose(1, 0, 2, 3).reshape(1, band, peers * local, cols) for c in chunks]
    returns = max(1, min(RETURNS, band // 2))
    pairs = band // 2 // returns
    incs = []
    for k in range(returns):
        inc = point_terms(chunks, k * pairs, pairs, loss, pair_first, pair_second, merge_weight)
        if not whole_tiles:
            inc = inc.reshape(2 * pairs, peers, local, cols).transpose(1, 0, 2, 3)
        incs.append(lax.all_to_all(inc, "comp", split_axis=0, concat_axis=0, tiled=True))
    count = lax.axis_size("geo")
    ends = count - 1
    low = lax.ppermute(incs[0][peers - 1, 1], "geo", [(i, i + 1) for i in range(ends)])
    high = lax.ppermute(incs[0][0, 0], "geo", [(i + 1, i) for i in range(ends)])
    low = jnp.pad(low.astype(F32)[:, None], ((0, 0), (HALO - 1, 0), (0, 0)))
    high = jnp.pad(high.astype(F32)[:, None], ((0, 0), (0, HALO - 1), (0, 0)))
    return finish(coef, density, low, high, wind, mask, incs, HALO)


def geo_halo_kernel(spectrum, mask, speed, angle, near, near_mask, near_speed, near_angle, send, recv):
    geo, ends = lax.axis_index("geo"), lax.axis_size("geo") - 1
    rows = spectrum.shape[1]
    barrier = pltpu.get_barrier_semaphore()
    has_low, has_high = geo > 0, geo < ends

    @pl.when(has_low)
    def _():
        pl.semaphore_signal(barrier, inc=1, device_id={"geo": geo - 1}, device_id_type=MESH)

    @pl.when(has_high)
    def _():
        pl.semaphore_signal(barrier, inc=1, device_id={"geo": geo + 1}, device_id_type=MESH)

    pl.semaphore_wait(barrier, jnp.minimum(geo, 1) + jnp.minimum(ends - geo, 1))

    def copies(side):
        at = pl.ds(0, HALO) if side else pl.ds(rows - HALO, HALO)
        to = {"geo": geo - 1} if side else {"geo": geo + 1}
        pairs = [
            (spectrum.at[:, at], near.at[side]),
            (mask.at[at], near_mask.at[side]),
            (speed.at[at], near_speed.at[side]),
            (angle.at[at], near_angle.at[side]),
        ]
        return [
            pltpu.make_async_remote_copy(
                src_ref=src, dst_ref=dst, send_sem=send.at[side, k], recv_sem=recv.at[side, k],
                device_id=to, device_id_type=MESH,
            )
            for k, (src, dst) in enumerate(pairs)
        ]

    down, up = copies(1), copies(0)

    @pl.when(has_low)
    def _():
        for c in down:
            c.start()

    @pl.when(has_high)
    def _():
        for c in up:
            c.start()

    for side, missing in ((0, geo == 0), (1, geo == ends)):

        @pl.when(missing)
        def _(side=side):
            for ref in (near, near_mask, near_speed, near_angle):
                ref[side] = jnp.zeros(ref.shape[1:], ref.dtype)

    @pl.when(has_low)
    def _():
        for c in down:
            c.wait_send()
        for c in up:
            c.wait_recv()

    @pl.when(has_high)
    def _():
        for c in up:
            c.wait_send()
        for c in down:
            c.wait_recv()


def geo_halo(spectrum, mask, speed, angle):
    comps, _, cols = spectrum.shape
    flat = lambda a: jax.ShapeDtypeStruct((2, HALO, cols), a.dtype)
    return pl.pallas_call(
        geo_halo_kernel,
        in_specs=[ANY] * 4,
        out_specs=[WHOLE] * 4,
        out_shape=[jax.ShapeDtypeStruct((2, comps, HALO, cols), spectrum.dtype), flat(mask), flat(speed), flat(angle)],
        scratch_shapes=[DMA((2, 4)), DMA((2, 4))],
        compiler_params=pltpu.CompilerParams(collective_id=1, has_side_effects=True),
        name="geo_halo",
    )(spectrum, mask, speed, angle)


def directions(comps, periodic):
    if not periodic:
        return True, True, True, True
    cos = [math.cos(2 * math.pi * c / ND) for c in comps]
    sin = [math.sin(2 * math.pi * c / ND) for c in comps]
    tiny = 1e-3
    south = any(s > -tiny and c % ND for s, c in zip(sin, comps))
    north = any(s < tiny and c % ND for s, c in zip(sin, comps))
    return any(c > -tiny for c in cos), any(c < tiny for c in cos), south, north


def column_terms(x, w, e, west, east):
    cols = x.shape[1]
    if west and east:
        return w * pltpu.roll(x, 1, 1) + e * pltpu.roll(x, cols - 1, 1)
    return w * pltpu.roll(x, 1, 1) if west else e * pltpu.roll(x, cols - 1, 1)


def group_sets(comps, periodic):
    groups = comps // 8
    count = max(k for k in range(1, 7) if groups % k == 0)
    sets = [list(range(k * count, (k + 1) * count)) for k in range(groups // count)]
    ways = [directions([8 * g + k for k in range(8)], periodic) for g in range(groups)]
    return sets, ways


def substeps(field, work, done, mask, coef, side, group_set, ways, top, base_of, done_at, stride):
    factor = {g: [coef[k, pl.ds(g * 8, 8), :] for k in range(5)] for g in group_set}
    size = len(group_set)
    plans = []
    for p in range(PROP_STEPS):
        trim = RUN // 2 if p >= PROP_STEPS - 2 else 0
        source = (field, base_of) if p == 0 else (work[(p - 1) % 2], 1)
        target = (done, done_at - trim) if p == PROP_STEPS - 1 else (work[p % 2], 1)
        plans.append((source, target, trim, (SPAN - 2 * trim) // RUN))

    def at(base, row, g):
        return pl.ds(pl.multiple_of((base + row) * stride + g * 8, 8), 8)

    def ahead(source, row):
        ref, base = source
        made = []
        for r in range(RUN):
            for g in group_set:
                west, east = ways[g][:2]
                made.append(column_terms(ref[at(base, row + r, g), :], factor[g][1], factor[g][2], west, east))
        return made

    def keep(made):
        for k, v in enumerate(made):
            side[k] = v

    def finish(source, target, row):
        ref, base = source
        out, out_base = target
        for j, g in enumerate(group_set):
            c, _, _, s, n = factor[g]
            south, north = ways[g][2:]
            held = ref[at(base, row - 1, g), :] if south else None
            here = ref[at(base, row, g), :]
            for r in range(RUN):
                after = ref[at(base, row + r + 1, g), :] if north or r < RUN - 1 else None
                v = c * here + side[r * size + j]
                if south:
                    v = v + s * held
                if north:
                    v = v + n * after
                out[at(out_base, row + r, g), :] = v * mask[top + row + r]
                held, here = here, after

    keep(ahead(plans[0][0], plans[0][2]))
    for p, (source, target, trim, trips) in enumerate(plans):

        def trip(t, carry, source=source, target=target, trim=trim):
            row = trim + t * RUN
            made = ahead(source, row + RUN)
            finish(source, target, row)
            keep(made)
            return carry

        lax.fori_loop(0, trips - 1, trip, 0)
        row = trim + (trips - 1) * RUN
        made = ahead(plans[p + 1][0], plans[p + 1][2]) if p + 1 < PROP_STEPS else None
        finish(source, target, row)
        if made is not None:
            keep(made)


def turn_in(spectrum, near, staged, field, sems, stride):
    comps, rows, cols = spectrum.shape
    slots, block = staged.shape[:2]
    blocks = comps // block
    for at in (0, (rows + 2 * HALO + 1) * stride):
        field[pl.ds(at, stride), :] = jnp.zeros((stride, cols), F32)

    def fetch(b):
        slot = lax.rem(b, slots)
        return pltpu.make_async_copy(spectrum.at[pl.ds(b * block, block)], staged.at[slot], sems.at[slot])

    for b in range(min(slots, blocks)):
        fetch(b).start()

    def turn(b, carry):
        fetch(b).wait()
        slot = lax.rem(b, slots)

        def one(k, carry):
            c = b * block + k
            v = jnp.concatenate(
                [near[0, c].astype(F32), staged[slot, k].astype(F32), near[1, c].astype(F32)], axis=0
            )
            field[pl.ds(stride + c, rows + 2 * HALO, stride=stride), :] = v
            return carry

        lax.fori_loop(0, block, one, 0)

        @pl.when(b + slots < blocks)
        def _():
            fetch(b + slots).start()

        return carry

    lax.fori_loop(0, blocks, turn, 0)


def band_at(k, bands):
    return jnp.where(k == 0, 0, jnp.where(k == 1, bands - 1, k - 1))


def partner(me, k, peers):
    if peers & (peers - 1):
        return lax.rem(me + k, peers)
    other, bit = me, 1
    while bit < peers:
        if k & bit:
            other = other + bit - 2 * bit * lax.rem(lax.div(other, bit), 2)
        bit *= 2
    return other


def advance_kernel(
    order, periodic, spectrum, near, mask, coef, loss, first_in, second_in, merge_in, density, back, edge,
    staged, field, work_a, work_b, done, side, tiles,
    spectra, incs, first, second, merge, product,
    stage_sems, density_sems, end_sems,
    weight_sems, send_sem, recv_sem, return_sem, back_sem, edge_send, edge_recv,
):
    peers = lax.axis_size("comp")
    me = lax.axis_index("comp")
    geo, ends = lax.axis_index("geo"), lax.axis_size("geo") - 1
    chunks, width, comps, cols = spectra.shape
    local = comps // peers
    terms = product.shape[0]
    has_low, has_high = geo > 0, geo < ends

    barrier = pltpu.get_barrier_semaphore()
    for k in range(1, peers):
        pl.semaphore_signal(barrier, inc=1, device_id={"comp": partner(me, k, peers)}, device_id_type=MESH)

    @pl.when(has_low)
    def _():
        pl.semaphore_signal(barrier, inc=1, device_id={"geo": geo - 1}, device_id_type=MESH)

    @pl.when(has_high)
    def _():
        pl.semaphore_signal(barrier, inc=1, device_id={"geo": geo + 1}, device_id_type=MESH)

    pl.semaphore_wait(barrier, peers - 1 + jnp.minimum(geo, 1) + jnp.minimum(ends - geo, 1))

    def part(who):
        return pl.ds(pl.multiple_of(who * local, 16), local)

    def outward(c, who):
        return pltpu.make_async_remote_copy(
            src_ref=tiles.at[pl.ds(c * width, width), who],
            dst_ref=spectra.at[c, :, part(me)],
            send_sem=send_sem, recv_sem=recv_sem.at[c],
            device_id={"comp": who}, device_id_type=MESH,
        )

    def homeward(c, who):
        return pltpu.make_async_remote_copy(
            src_ref=incs.at[c, :, part(who)],
            dst_ref=back.at[pl.ds(c * width, width), me],
            send_sem=return_sem, recv_sem=back_sem.at[c],
            device_id={"comp": who}, device_id_type=MESH,
        )

    def own_home(c):
        return pltpu.make_async_copy(incs.at[c, :, part(me)], back.at[pl.ds(c * width, width), me], back_sem.at[c])

    loads = [
        pltpu.make_async_copy(src, dst, weight_sems.at[k])
        for k, (src, dst) in enumerate(((first_in, first), (second_in, second), (merge_in, merge)))
    ]
    rows = mask.shape[0] - 2 * HALO
    stride = stride_of(local) + 8
    bands = rows // BAND
    turn_in(spectrum, near, staged, field, stage_sems, stride)
    for load in loads:
        load.start()
    zeros = jnp.zeros((stride, cols), F32)
    for work in (work_a, work_b):
        work[pl.ds(0, stride), :] = zeros
        work[pl.ds((SPAN + 1) * stride, stride), :] = zeros

    sets, ways = group_sets(local, periodic)

    def whole(k):
        at = lax.rem(k, 2) * (SPAN - RUN)
        band = band_at(k, bands)
        return pltpu.make_async_copy(
            done.at[pl.ds((at + 2) * stride, BAND * stride)],
            density.at[pl.ds((band * BAND + 1) * stride, BAND * stride)],
            density_sems.at[k],
        )

    def end(side_of):
        k = 1 if side_of and bands > 1 else 0
        at = (k % 2) * (SPAN - RUN) + (BAND + 2 if side_of else 1)
        row = rows + 1 if side_of else 0
        return pltpu.make_async_copy(
            done.at[pl.ds(at * stride, stride)], density.at[pl.ds(row * stride, stride)], end_sems.at[side_of]
        )

    def form(k, carry):
        band = band_at(k, bands)
        at = lax.rem(k, 2) * (SPAN - RUN)

        @pl.when(k >= 2)
        def _():
            whole(k - 2).wait()

        @pl.when(k == 2)
        def _():
            end(0).wait()

        if bands > 3:

            @pl.when(k == 3)
            def _():
                end(1).wait()

        for group_set in sets:
            substeps(
                field, (work_a, work_b), done, mask, coef, side, group_set, ways,
                band * BAND, band * BAND + 1, at, stride,
            )
        whole(k).start()

        @pl.when(k == 0)
        def _():
            end(0).start()

        @pl.when(k == min(1, bands - 1))
        def _():
            end(1).start()

        def pack(r, carry):
            t = k * BAND + r
            from_at = pl.multiple_of((at + 2 + r) * stride, 8)
            tiles[lax.div(t, peers), lax.rem(t, peers)] = done[pl.ds(from_at, local), :].astype(BF16)
            return carry

        lax.fori_loop(0, BAND, pack, 0)
        per = BAND // (peers * width)
        for group in order:
            for j in range(per):
                for who in group:
                    outward(k * per + j, partner(me, who, peers)).start()
        for j in range(per):
            for h in range(width):
                spectra[k * per + j, h, part(me), :] = tiles[(k * per + j) * width + h, me]
        return carry

    lax.fori_loop(0, bands, form, 0)
    for load in loads:
        load.wait()

    tile = max(t for t in range(16, 600, 16) if terms % t == 0)
    step = max(g for g in range(1, peers + 1) if peers % g == 0 and g * local <= 600) * local

    def work(c, carry):
        arrived = spectra.at[c, :, pl.ds(0, comps - local)]
        pltpu.make_async_copy(arrived, arrived, recv_sem.at[c]).wait()

        def both():
            return jnp.concatenate([spectra[c, h] for h in range(width)], axis=1)

        def multiply(t, carry):
            rows = pl.ds(pl.multiple_of(t * tile, 16), tile)
            x = both()
            one = jnp.dot(first[rows, :], x, preferred_element_type=F32)
            two = jnp.dot(second[rows, :], x, preferred_element_type=F32)
            product[rows, :] = (one * two).astype(BF16)
            return carry

        lax.fori_loop(0, terms // tile, multiply, 0)
        roots = []
        for h in range(width):
            energy = jnp.sum(spectra[c, h].astype(F32), axis=0, keepdims=True)
            roots.append(jnp.sqrt(energy / comps + 1e-06))
        for d in range(0, comps, step):
            rows = slice(d, d + step)
            moved = jnp.dot(merge[rows, :], product[...], preferred_element_type=F32)
            for h in range(width):
                lanes = slice(h * cols, (h + 1) * cols)
                total = moved[:, lanes] - loss[rows, :] * roots[h] * spectra[c, h, rows, :].astype(F32)
                incs[c, h, rows, :] = total.astype(BF16)
        for group in order:
            for k in group:
                homeward(c, partner(me, k, peers)).start()
        own_home(c).start()
        return carry

    lax.fori_loop(0, chunks, work, 0)

    def landed(c):
        there = back.at[pl.ds(c * width, width)]
        pltpu.make_async_copy(there, there, back_sem.at[c]).wait()

    far_chunk = (min(2, bands) * BAND - 1) // (peers * width)

    def land(c, carry):
        landed(c)
        return carry

    lax.fori_loop(0, far_chunk + 1, land, 0)
    last = min(2, bands) * BAND - 1
    to_low = pltpu.make_async_remote_copy(
        src_ref=back.at[0, 0], dst_ref=edge.at[1], send_sem=edge_send.at[1], recv_sem=edge_recv.at[1],
        device_id={"geo": geo - 1}, device_id_type=MESH,
    )
    to_high = pltpu.make_async_remote_copy(
        src_ref=back.at[last // peers, last % peers], dst_ref=edge.at[0], send_sem=edge_send.at[0], recv_sem=edge_recv.at[0],
        device_id={"geo": geo + 1}, device_id_type=MESH,
    )

    @pl.when(has_low)
    def _():
        to_low.start()

    @pl.when(has_high)
    def _():
        to_high.start()

    lax.fori_loop(far_chunk + 1, chunks, land, 0)
    for k in range(max(0, bands - 2), bands):
        whole(k).wait()
    if bands <= 2:
        end(0).wait()
    if bands <= 3:
        end(1).wait()

    @pl.when(has_low)
    def _():
        to_low.wait_send()
        to_high.wait_recv()

    @pl.when(has_high)
    def _():
        to_high.wait_send()
        to_low.wait_recv()

    def sent(c, carry):
        for k in range(1, peers):
            outward(c, partner(me, k, peers)).wait_send()
            homeward(c, partner(me, k, peers)).wait_send()
        return carry

    lax.fori_loop(0, chunks, sent, 0)


def advance(spectrum, near, mask, coef, loss, first, second, merge, periodic):
    local, rows, cols = spectrum.shape
    peers = lax.axis_size("comp")
    depth = rows // peers
    chunks = depth // CHUNK
    comps, terms = merge.shape
    stride = stride_of(local) + 8
    if peers == 8:
        order = [(1, 2, 3), (4, 5, 6, 7)]
    else:
        order = [tuple(range(1, peers))]
    sets, _ = group_sets(local, periodic)
    return pl.pallas_call(
        functools.partial(advance_kernel, order, periodic),
        in_specs=[ANY, WHOLE, WHOLE, WHOLE, WHOLE, ANY, ANY, ANY],
        out_specs=[ANY, ANY, ANY],
        out_shape=[
            jax.ShapeDtypeStruct(((rows + 2) * stride, cols), F32),
            jax.ShapeDtypeStruct((depth, peers, local, cols), BF16),
            jax.ShapeDtypeStruct((2, local, cols), BF16),
        ],
        scratch_shapes=[
            VMEM((4, 16, rows, cols), BF16),
            VMEM(((rows + 2 * HALO + 2) * stride, cols), F32),
            VMEM(((SPAN + 2) * stride, cols), F32),
            VMEM(((SPAN + 2) * stride, cols), F32),
            VMEM((2 * (SPAN - RUN) * stride, cols), F32),
            VMEM((RUN * len(sets[0]), 8, cols), F32),
            VMEM((depth, peers, local, cols), BF16),
            VMEM((chunks, CHUNK, comps, cols), BF16),
            VMEM((chunks, CHUNK, comps, cols), BF16),
            VMEM((terms, comps), BF16),
            VMEM((terms, comps), BF16),
            VMEM((comps, terms), BF16),
            VMEM((terms, CHUNK * cols), BF16),
            DMA((4,)),
            DMA((rows // BAND,)),
            DMA((2,)),
            DMA((3,)),
            DMA,
            DMA((chunks,)),
            DMA,
            DMA((chunks,)),
            DMA((2,)),
            DMA((2,)),
        ],
        cost_estimate=pl.CostEstimate(
            flops=6 * comps * terms * depth * cols, bytes_accessed=6 * comps * terms, transcendentals=0
        ),
        compiler_params=pltpu.CompilerParams(
            collective_id=2, has_side_effects=True, vmem_limit_bytes=63 * 1024 * 1024
        ),
        name="advance",
    )(spectrum, near, mask, coef, loss, first, second, merge)


def close_kernel(periodic, ends, density, back, edge, wind, mask, coef, out, cells, forced, turned, incs, side, staged, sems, out_sems):
    comps, rows, cols = staged.shape
    stride = stride_of(comps) + 8
    sets, ways = group_sets(comps, periodic)
    size = len(sets[0])
    bands = rows // BAND
    views = [ref.reshape(rows + 2, stride, cols) for ref in (density, cells)]

    def fetches(b):
        at = pl.ds(sets[b][0] * 8, size * 8)
        moves = [
            (views[0].at[:, at], views[1].at[:, at]),
            (edge.at[0, at], incs.at[0, at]),
            (back.at[pl.ds(0, BAND), at], incs.at[pl.ds(1, BAND), at]),
            (edge.at[1, at], incs.at[rows + 1, at]),
        ]
        if bands > 1:
            moves.append((back.at[pl.ds(BAND, BAND), at], incs.at[pl.ds(rows + 1 - BAND, BAND), at]))
        if bands > 2:
            between = rows - 2 * BAND
            moves.append((back.at[pl.ds(2 * BAND, between), at], incs.at[pl.ds(1 + BAND, between), at]))
        return [pltpu.make_async_copy(src, dst, sems.at[b, k]) for k, (src, dst) in enumerate(moves)]

    for b in range(len(sets)):
        for f in fetches(b):
            f.start()

    run = max(k for k in range(1, 17) if (rows + 2) % k == 0)
    trips = (rows + 2) // run

    def at(row, g):
        return pl.ds(pl.multiple_of(row * stride + g * 8, 8), 8)

    def set_of(b):
        group_set = sets[b]
        for f in fetches(b):
            f.wait()
        span = pl.ds(group_set[0] * 8, size * 8)
        for end, row in ((0, 0), (1, rows + 1)):

            @pl.when(ends[end] == 1)
            def _(row=row):
                incs[row, span, :] = jnp.zeros((size * 8, cols), BF16)

        factor = {g: [coef[k, pl.ds(g * 8, 8), :] for k in range(8)] for g in group_set}

        def ahead(row):
            made = []
            for r in range(run):
                blow, turn_x, turn_y = wind[0, row + r], wind[1, row + r], wind[2, row + r]
                for g in group_set:
                    if g % 2 == 0:
                        both = incs[row + r, pl.ds(g * 8, 16), :].astype(F32)
                    rate, cos_h, sin_h = factor[g][5:8]
                    d = cells[at(row + r, g), :]
                    facing = jnp.maximum(cos_h * turn_x + sin_h * turn_y, 0.0)
                    growth = rate * blow * (facing * facing)
                    new = d + growth * d + both[(g % 2) * 8 : (g % 2) * 8 + 8]
                    forced[at(row + r + 1, g), :] = new
                    west, east = ways[g][:2]
                    made.append(column_terms(new, factor[g][1], factor[g][2], west, east))
            return made

        def keep(made):
            for k, v in enumerate(made):
                side[k] = v

        def finish(row):
            for j, g in enumerate(group_set):
                c, _, _, s, n = factor[g][:5]
                south, north = ways[g][2:]
                held = forced[at(row, g), :] if south else None
                here = forced[at(row + 1, g), :]
                for r in range(run):
                    after = forced[at(row + r + 2, g), :] if north or r < run - 1 else None
                    v = c * here + side[r * size + j]
                    if south:
                        v = v + s * held
                    if north:
                        v = v + n * after
                    turned[at(row + r, g), :] = v * mask[row + r]
                    held, here = here, after

        def trip(t, carry):
            made = ahead((t + 1) * run)
            finish(t * run)
            keep(made)
            return carry

        keep(ahead(0))
        lax.fori_loop(0, trips - 1, trip, 0)
        finish((trips - 1) * run)

    def give(b):
        part = pl.ds(b * size * 8, size * 8)
        return pltpu.make_async_copy(staged.at[part], out.at[part], out_sems.at[b])

    zeros = jnp.zeros((stride, cols), F32)
    forced[pl.ds(0, stride), :] = zeros
    forced[pl.ds((rows + 3) * stride, stride), :] = zeros
    for b in range(len(sets)):
        set_of(b)

        def lift(k, carry, b=b):
            c = b * size * 8 + k
            staged[c] = turned[pl.ds(stride + c, rows, stride=stride), :].astype(BF16)
            return carry

        lax.fori_loop(0, size * 8, lift, 0)
        give(b).start()
    for b in range(len(sets)):
        give(b).wait()


def close(density, back, edge, wind, mask, coef, ends, periodic):
    rows, comps, cols = back.shape
    stride = stride_of(comps) + 8
    sets, _ = group_sets(comps, periodic)
    run = max(k for k in range(1, 17) if (rows + 2) % k == 0)
    return pl.pallas_call(
        functools.partial(close_kernel, periodic),
        in_specs=[pl.BlockSpec(memory_space=SMEM), ANY, ANY, ANY, WHOLE, WHOLE, WHOLE],
        out_specs=ANY,
        out_shape=jax.ShapeDtypeStruct((comps, rows, cols), BF16),
        scratch_shapes=[
            VMEM(((rows + 2) * stride, cols), F32),
            VMEM(((rows + 4) * stride, cols), F32),
            VMEM(((rows + 2) * stride, cols), F32),
            VMEM((rows + 2, comps, cols), BF16),
            VMEM((run * len(sets[0]), 8, cols), F32),
            VMEM((comps, rows, cols), BF16),
            DMA((len(sets), 6)),
            DMA((len(sets),)),
        ],
        compiler_params=pltpu.CompilerParams(vmem_limit_bytes=56 * 1024 * 1024),
        name="close",
    )(ends, density, back, edge, wind, mask, coef)


def tall(rows_of):
    return jnp.broadcast_to(rows_of[:, None, :], (rows_of.shape[0], 8, rows_of.shape[1]))


def body(spectrum, land_mask, wind_speed, wind_dir, input_rate, dissipation, pair_first, pair_second, merge_weight):
    local, rows, cols = spectrum.shape
    peers = lax.axis_size("comp")
    fits = local % 16 == 0 and rows % BAND == 0 and BAND % (peers * CHUNK) == 0 and cols == 128
    if not fits:
        return plain_body(
            spectrum, land_mask, wind_speed, wind_dir, input_rate, dissipation, pair_first, pair_second, merge_weight
        )
    periodic = local % ND == 0
    near, near_mask, near_speed, near_angle = geo_halo(spectrum, land_mask, wind_speed, wind_dir)

    ids = lax.axis_index("comp") * local + jnp.arange(local, dtype=jnp.int32)
    frequency = (ids // ND).astype(F32)
    heading = 2.0 * math.pi * (ids % ND).astype(F32) / ND
    courant = 0.7 * jnp.power(F32(1.1), -frequency)
    cos_h, sin_h = jnp.cos(heading), jnp.sin(heading)
    west, east = jnp.maximum(courant * cos_h, 0.0), jnp.maximum(-courant * cos_h, 0.0)
    south, north = jnp.maximum(courant * sin_h, 0.0), jnp.maximum(-courant * sin_h, 0.0)
    center = 1.0 - west - east - south - north
    coef = jnp.stack([center, west, east, south, north, input_rate, cos_h, sin_h])
    coef = jnp.broadcast_to(coef[:, :, None], (8, local, cols))

    sea = jnp.concatenate([near_mask[0], land_mask, near_mask[1]]).astype(F32)
    sea = tall(sea)
    angle = jnp.concatenate([near_angle[0, HALO - 1 :], wind_dir, near_angle[1, :1]])
    speed = jnp.concatenate([near_speed[0, HALO - 1 :], wind_speed, near_speed[1, :1]])
    wind = jnp.stack([tall(speed), tall(jnp.cos(angle)), tall(jnp.sin(angle))])
    geo = lax.axis_index("geo")
    ends = jnp.stack([geo == 0, geo == lax.axis_size("geo") - 1]).astype(jnp.int32)

    density, back, edge = advance(
        spectrum, near, sea, coef, dissipation[:, None], pair_first, pair_second, merge_weight, periodic
    )
    below = HALO - 1
    return close(density, back.reshape(rows, local, cols), edge, wind, sea[below : below + rows + 2], coef, ends, periodic)


def solution(mesh):
    placed = (P("comp", "geo", None), P("geo", None), P("geo", None), P("geo", None), P("comp"), P(), P(), P(), P())
    return jax.shard_map(
        body, mesh=mesh, in_specs=placed, out_specs=P("comp", "geo", None), check_vma=False
    )
```

```python
import functools
import math

import jax
import jax.numpy as jnp
from jax import lax
from jax.experimental import pallas as pl
from jax.experimental.pallas import tpu as pltpu
from jax.sharding import PartitionSpec as P

ND = 36
PROP_STEPS = 6
HALO = 8
SENDS = 3
RETURNS = 2
F32 = jnp.float32
BF16 = jnp.bfloat16
VMEM = pltpu.VMEM
ANY = pl.BlockSpec(memory_space=pl.ANY)
WHOLE = pl.BlockSpec(memory_space=pltpu.VMEM)
MESH = pl.DeviceIdType.MESH
DMA = pltpu.SemaphoreType.DMA
CHUNK = 2
BAND = 32
BLOCK = 16
TILES = 13
RUN = 12
SPAN = BAND + 2 * HALO
SMEM = pltpu.SMEM


def edges(cells, axis_dim):
    count = lax.axis_size("geo")
    ends = count - 1
    size = cells.shape[axis_dim]
    head = lax.slice_in_dim(cells, 0, HALO, axis=axis_dim)
    tail = lax.slice_in_dim(cells, size - HALO, size, axis=axis_dim)
    lower = lax.ppermute(tail, "geo", [(i, i + 1) for i in range(ends)])
    upper = lax.ppermute(head, "geo", [(i + 1, i) for i in range(ends)])
    return lower, upper


def block_of(comps):
    return 16 if comps % 16 == 0 else comps


def stride_of(block):
    return -(-block // 8) * 8


def upwind(v, mask, coef, at):
    center, west, east, south, north = (coef[at + k] for k in range(5))
    rows = v.shape[0]
    moved = west * pltpu.roll(v, 1, 1) + east * pltpu.roll(v, v.shape[1] - 1, 1)
    moved = moved + south * pltpu.roll(v, 1, 0) + north * pltpu.roll(v, rows - 1, 0)
    return (center * v + moved) * mask


def prop_kernel(coef, lower, cells, upper, mask, density, outgoing, turned):
    block, rows, cols = cells.shape
    stride = stride_of(block)
    first = pl.program_id(0) * block

    def one(c, carry):
        v = jnp.concatenate(
            [lower[c].astype(F32), cells[c].astype(F32), upper[c].astype(F32)], axis=0
        )
        sea = mask[...]
        for _ in range(PROP_STEPS):
            v = upwind(v, sea, coef, (first + c) * 8)
        density[c] = v
        turned[pl.ds(c, rows, stride=stride), :] = v[HALO : HALO + rows]
        return carry

    lax.fori_loop(0, block, one, 0)

    def pack(r, carry):
        start = pl.multiple_of(r * stride, 8)
        outgoing[r] = turned[pl.ds(start, block), :].astype(BF16)
        return carry

    lax.fori_loop(0, rows, pack, 0, unroll=8)


def propagate(coef, lower, cells, upper, mask):
    comps, rows, cols = cells.shape
    block = block_of(comps)
    tall = rows + 2 * HALO
    return pl.pallas_call(
        prop_kernel,
        grid=(comps // block,),
        in_specs=[
            pl.BlockSpec(memory_space=SMEM),
            pl.BlockSpec((block, HALO, cols), lambda i: (i, 0, 0)),
            pl.BlockSpec((block, rows, cols), lambda i: (i, 0, 0)),
            pl.BlockSpec((block, HALO, cols), lambda i: (i, 0, 0)),
            pl.BlockSpec((tall, cols), lambda i: (0, 0)),
        ],
        out_specs=[
            pl.BlockSpec((block, tall, cols), lambda i: (i, 0, 0)),
            pl.BlockSpec((rows, block, cols), lambda i: (0, i, 0)),
        ],
        out_shape=[
            jax.ShapeDtypeStruct((comps, tall, cols), F32),
            jax.ShapeDtypeStruct((rows, comps, cols), BF16),
        ],
        scratch_shapes=[VMEM((rows * stride_of(block), cols), F32)],
        cost_estimate=pl.CostEstimate(
            flops=comps * tall * cols * 100,
            bytes_accessed=comps * tall * cols * 8,
            transcendentals=0,
        ),
        name="propagate",
    )(coef, lower, cells, upper, mask)


def point_kernel(sends, *refs):
    near, far = refs[:sends], refs[sends : 2 * sends]
    loss, first, second, merge, out, spectra, product = refs[2 * sends :]
    peers, _, part, cols = near[0].shape
    local = sends * part
    comps, terms = merge.shape
    for side, group in enumerate((near, far)):
        lanes = slice(side * cols, (side + 1) * cols)
        for k in range(sends):
            for s in range(peers):
                at = s * local + k * part
                spectra[at : at + part, lanes] = group[k][s, 0]
    tile = max(t for t in range(16, 600, 16) if terms % t == 0)

    def multiply(t, carry):
        rows = pl.ds(pl.multiple_of(t * tile, 16), tile)
        x = spectra[...]
        one = jnp.dot(first[rows, :], x, preferred_element_type=F32)
        two = jnp.dot(second[rows, :], x, preferred_element_type=F32)
        product[rows, :] = (one * two).astype(BF16)
        return carry

    lax.fori_loop(0, terms // tile, multiply, 0)
    energy = jnp.sum(spectra[...].astype(F32), axis=0, keepdims=True)
    root = jnp.sqrt(energy / comps + 1e-06)
    if peers == 1:
        step = max(t for t in range(16, 600, 16) if comps % t == 0)
        for d in range(0, comps, step):
            rows = slice(d, d + step)
            moved = jnp.dot(merge[rows, :], product[...], preferred_element_type=F32)
            total = moved - loss[rows, :] * root * spectra[rows, :].astype(F32)
            out[0, 0, rows] = total[:, :cols].astype(BF16)
            out[0, 1, rows] = total[:, cols:].astype(BF16)
        return
    share = max(g for g in range(1, peers + 1) if peers % g == 0 and g * local <= 600)
    for d in range(0, peers, share):
        rows = slice(d * local, (d + share) * local)
        moved = jnp.dot(merge[rows, :], product[...], preferred_element_type=F32)
        total = moved - loss[rows, :] * root * spectra[rows, :].astype(F32)
        for g in range(share):
            piece = total[g * local : (g + 1) * local].astype(BF16)
            out[d + g, 0] = piece[:, :cols]
            out[d + g, 1] = piece[:, cols:]


def point_terms(chunks, start, pairs, loss, first, second, merge):
    sends = len(chunks)
    peers, rows, part, cols = chunks[0].shape
    local = sends * part
    comps, terms = merge.shape
    whole = lambda shape: pl.BlockSpec(shape, lambda i: (0, 0))
    near = pl.BlockSpec((peers, 1, part, cols), lambda i: (0, start + i, 0, 0))
    far = pl.BlockSpec((peers, 1, part, cols), lambda i: (0, rows - 1 - start - i, 0, 0))
    return pl.pallas_call(
        functools.partial(point_kernel, sends),
        grid=(pairs,),
        in_specs=[near] * sends
        + [far] * sends
        + [whole((comps, 1)), whole((terms, comps)), whole((terms, comps)), whole((comps, terms))],
        out_specs=pl.BlockSpec((peers, 2, local, cols), lambda i: (0, i, 0, 0)),
        out_shape=jax.ShapeDtypeStruct((peers, 2 * pairs, local, cols), BF16),
        scratch_shapes=[VMEM((comps, 2 * cols), BF16), VMEM((terms, 2 * cols), BF16)],
        cost_estimate=pl.CostEstimate(
            flops=pairs * 12 * comps * terms * cols,
            bytes_accessed=6 * comps * terms + pairs * 8 * comps * cols,
            transcendentals=0,
        ),
        compiler_params=pltpu.CompilerParams(vmem_limit_bytes=60 * 1024 * 1024),
        name="points",
    )(*chunks, *chunks, loss, first, second, merge)


def final_kernel(returns, coef, density, low_inc, high_inc, wind, mask, *refs):
    incs = refs[:returns]
    out, turned = refs[returns:]
    block, rows, cols = out.shape
    peers, held = incs[0].shape[:2]
    band = rows // peers
    stride = stride_of(block)
    first = pl.program_id(0) * block

    def place(s, carry):
        for k in range(returns):
            for j in range(held):
                a = k * (held // 2) + j // 2
                row = a if j % 2 == 0 else band - 1 - a
                at = pl.multiple_of((s * band + row) * stride, 8)
                turned[pl.ds(at, block), :] = incs[k][s, j].astype(F32)
        return carry

    lax.fori_loop(0, peers, place, 0)

    def one(c, carry):
        at = (first + c) * 8
        inc = jnp.concatenate(
            [low_inc[c], turned[pl.ds(c, rows, stride=stride), :], high_inc[c]], axis=0
        )
        v = density[c]
        facing = jnp.maximum(coef[at + 6] * wind[1] + coef[at + 7] * wind[2], 0.0)
        growth = coef[at + 5] * wind[0] * facing * facing
        v = v + growth * v + inc
        v = upwind(v, mask[...], coef, at)
        out[c] = v[HALO : HALO + rows].astype(BF16)
        return carry

    lax.fori_loop(0, block, one, 0)


def finish(coef, density, low_inc, high_inc, wind, mask, incs, lead):
    local, tall, cols = density.shape
    rows = tall - 2 * HALO
    block = block_of(local)
    peers, held = incs[0].shape[:2]
    return pl.pallas_call(
        functools.partial(final_kernel, len(incs)),
        grid=(local // block,),
        in_specs=[
            pl.BlockSpec(memory_space=SMEM),
            pl.BlockSpec((block, tall, cols), lambda i: (i, 0, 0)),
            pl.BlockSpec((block, HALO, cols), lambda i: (i, 0, 0)),
            pl.BlockSpec((block, HALO, cols), lambda i: (i, 0, 0)),
            pl.BlockSpec((3, tall, cols), lambda i: (0, 0, 0)),
            pl.BlockSpec((tall, cols), lambda i: (0, 0)),
        ]
        + [pl.BlockSpec((peers, held, block, cols), lambda i: (0, 0, i, 0))] * len(incs),
        out_specs=pl.BlockSpec((block, rows, cols), lambda i: (i, 0, 0)),
        out_shape=jax.ShapeDtypeStruct((local, rows, cols), BF16),
        scratch_shapes=[VMEM((rows * stride_of(block), cols), F32)],
        name="finish",
    )(coef, density, low_inc, high_inc, wind, mask, *incs)


def plain_body(spectrum, land_mask, wind_speed, wind_dir, input_rate, dissipation, pair_first, pair_second, merge_weight):
    local, rows, cols = spectrum.shape
    peers = lax.axis_size("comp")
    band = rows // peers
    ids = lax.axis_index("comp") * local + jnp.arange(local, dtype=jnp.int32)
    frequency = (ids // ND).astype(F32)
    heading = 2.0 * math.pi * (ids % ND).astype(F32) / ND
    courant = 0.7 * jnp.power(F32(1.1), -frequency)
    cos_h, sin_h = jnp.cos(heading), jnp.sin(heading)
    west, east = jnp.maximum(courant * cos_h, 0.0), jnp.maximum(-courant * cos_h, 0.0)
    south, north = jnp.maximum(courant * sin_h, 0.0), jnp.maximum(-courant * sin_h, 0.0)
    center = 1.0 - west - east - south - north
    coef = jnp.stack([center, west, east, south, north, input_rate, cos_h, sin_h], axis=1).reshape(-1)

    lower, upper = edges(spectrum, 1)
    fields = jnp.stack([wind_speed, jnp.cos(wind_dir), jnp.sin(wind_dir), land_mask.astype(F32)])
    low_f, high_f = edges(fields, 1)
    fields = jnp.concatenate([low_f, fields, high_f], axis=1)
    wind, mask = fields[:3], fields[3]

    whole_tiles = local % (16 * SENDS) == 0
    sends = SENDS if whole_tiles else 1
    part = local // sends
    density, chunks = [], []
    for k in range(sends):
        cut = slice(k * part, (k + 1) * part)
        d, out = propagate(coef[k * part * 8 : (k + 1) * part * 8], lower[cut], spectrum[cut], upper[cut], mask)
        density.append(d)
        out = out.reshape(peers, band, part, cols)
        chunks.append(lax.all_to_all(out, "comp", split_axis=0, concat_axis=0, tiled=True))
    density = jnp.concatenate(density, axis=0)

    loss = dissipation[:, None]
    if not whole_tiles:
        chunks = [c.transpose(1, 0, 2, 3).reshape(1, band, peers * local, cols) for c in chunks]
    returns = max(1, min(RETURNS, band // 2))
    pairs = band // 2 // returns
    incs = []
    for k in range(returns):
        inc = point_terms(chunks, k * pairs, pairs, loss, pair_first, pair_second, merge_weight)
        if not whole_tiles:
            inc = inc.reshape(2 * pairs, peers, local, cols).transpose(1, 0, 2, 3)
        incs.append(lax.all_to_all(inc, "comp", split_axis=0, concat_axis=0, tiled=True))
    count = lax.axis_size("geo")
    ends = count - 1
    low = lax.ppermute(incs[0][peers - 1, 1], "geo", [(i, i + 1) for i in range(ends)])
    high = lax.ppermute(incs[0][0, 0], "geo", [(i + 1, i) for i in range(ends)])
    low = jnp.pad(low.astype(F32)[:, None], ((0, 0), (HALO - 1, 0), (0, 0)))
    high = jnp.pad(high.astype(F32)[:, None], ((0, 0), (0, HALO - 1), (0, 0)))
    return finish(coef, density, low, high, wind, mask, incs, HALO)


def geo_halo_kernel(spectrum, mask, speed, angle, near, near_mask, near_speed, near_angle, seas, send, recv, sea_send, sea_recv):
    geo, ends = lax.axis_index("geo"), lax.axis_size("geo") - 1
    rows = spectrum.shape[1]
    barrier = pltpu.get_barrier_semaphore()
    has_low, has_high = geo > 0, geo < ends
    others = [lax.rem(geo + k, ends + 1) for k in range(1, ends + 1)]
    for who in others:
        pl.semaphore_signal(barrier, inc=1, device_id={"geo": who}, device_id_type=MESH)
    pl.semaphore_wait(barrier, ends)

    def whole_mask(k):
        return pltpu.make_async_remote_copy(
            src_ref=mask, dst_ref=seas.at[geo], send_sem=sea_send.at[k], recv_sem=sea_recv.at[k],
            device_id={"geo": others[k]}, device_id_type=MESH,
        )

    def copies(side):
        at = pl.ds(0, HALO) if side else pl.ds(rows - HALO, HALO)
        to = {"geo": geo - 1} if side else {"geo": geo + 1}
        pairs = [
            (spectrum.at[:, at], near.at[side]),
            (mask.at[at], near_mask.at[side]),
            (speed.at[at], near_speed.at[side]),
            (angle.at[at], near_angle.at[side]),
        ]
        return [
            pltpu.make_async_remote_copy(
                src_ref=src, dst_ref=dst, send_sem=send.at[side, k], recv_sem=recv.at[side, k],
                device_id=to, device_id_type=MESH,
            )
            for k, (src, dst) in enumerate(pairs)
        ]

    down, up = copies(1), copies(0)

    @pl.when(has_low)
    def _():
        for c in down:
            c.start()

    @pl.when(has_high)
    def _():
        for c in up:
            c.start()

    for k in range(ends):
        whole_mask(k).start()
    own = pltpu.make_async_copy(mask, seas.at[geo], sea_send.at[ends])
    own.start()

    for side, missing in ((0, geo == 0), (1, geo == ends)):

        @pl.when(missing)
        def _(side=side):
            for ref in (near, near_mask, near_speed, near_angle):
                ref[side] = jnp.zeros(ref.shape[1:], ref.dtype)

    @pl.when(has_low)
    def _():
        for c in down:
            c.wait_send()
        for c in up:
            c.wait_recv()

    @pl.when(has_high)
    def _():
        for c in up:
            c.wait_send()
        for c in down:
            c.wait_recv()

    for k in range(ends):
        whole_mask(k).wait()
    own.wait()


def geo_halo(spectrum, mask, speed, angle):
    comps, _, cols = spectrum.shape
    count = lax.axis_size("geo")
    flat = lambda a: jax.ShapeDtypeStruct((2, HALO, cols), a.dtype)
    seas = jax.ShapeDtypeStruct((count,) + mask.shape, mask.dtype)
    return pl.pallas_call(
        geo_halo_kernel,
        in_specs=[ANY] * 4,
        out_specs=[WHOLE] * 5,
        out_shape=[jax.ShapeDtypeStruct((2, comps, HALO, cols), spectrum.dtype), flat(mask), flat(speed), flat(angle), seas],
        scratch_shapes=[DMA((2, 4)), DMA((2, 4)), DMA((count,)), DMA((count,))],
        compiler_params=pltpu.CompilerParams(collective_id=1, has_side_effects=True),
        name="geo_halo",
    )(spectrum, mask, speed, angle)


def directions(comps, periodic):
    if not periodic:
        return True, True, True, True
    cos = [math.cos(2 * math.pi * c / ND) for c in comps]
    sin = [math.sin(2 * math.pi * c / ND) for c in comps]
    tiny = 1e-3
    south = any(s > -tiny and c % ND for s, c in zip(sin, comps))
    north = any(s < tiny and c % ND for s, c in zip(sin, comps))
    return any(c > -tiny for c in cos), any(c < tiny for c in cos), south, north


def column_terms(x, w, e, west, east):
    cols = x.shape[1]
    if west and east:
        return w * pltpu.roll(x, 1, 1) + e * pltpu.roll(x, cols - 1, 1)
    return w * pltpu.roll(x, 1, 1) if west else e * pltpu.roll(x, cols - 1, 1)


def group_sets(comps, periodic):
    groups = comps // 8
    count = max(k for k in range(1, 7) if groups % k == 0)
    sets = [list(range(k * count, (k + 1) * count)) for k in range(groups // count)]
    ways = [directions([8 * g + k for k in range(8)], periodic) for g in range(groups)]
    return sets, ways


def substeps(field, work, done, mask, coef, side, group_set, ways, top, base_of, done_at, stride):
    factor = {g: [coef[k, pl.ds(g * 8, 8), :] for k in range(5)] for g in group_set}
    size = len(group_set)
    plans = []
    for p in range(PROP_STEPS):
        trim = RUN // 2 if p >= PROP_STEPS - 2 else 0
        source = (field, base_of) if p == 0 else (work[(p - 1) % 2], 1)
        target = (done, done_at - trim) if p == PROP_STEPS - 1 else (work[p % 2], 1)
        plans.append((source, target, trim, (SPAN - 2 * trim) // RUN))

    def at(base, row, g):
        return pl.ds(pl.multiple_of((base + row) * stride + g * 8, 8), 8)

    def ahead(source, row):
        ref, base = source
        made = []
        for r in range(RUN):
            for g in group_set:
                west, east = ways[g][:2]
                made.append(column_terms(ref[at(base, row + r, g), :], factor[g][1], factor[g][2], west, east))
        return made

    def keep(made):
        for k, v in enumerate(made):
            side[k] = v

    def finish(source, target, row):
        ref, base = source
        out, out_base = target
        for j, g in enumerate(group_set):
            c, _, _, s, n = factor[g]
            south, north = ways[g][2:]
            held = ref[at(base, row - 1, g), :] if south else None
            here = ref[at(base, row, g), :]
            for r in range(RUN):
                after = ref[at(base, row + r + 1, g), :] if north or r < RUN - 1 else None
                v = c * here + side[r * size + j]
                if south:
                    v = v + s * held
                if north:
                    v = v + n * after
                out[at(out_base, row + r, g), :] = v * mask[top + row + r]
                held, here = here, after

    keep(ahead(plans[0][0], plans[0][2]))
    for p, (source, target, trim, trips) in enumerate(plans):

        def trip(t, carry, source=source, target=target, trim=trim):
            row = trim + t * RUN
            made = ahead(source, row + RUN)
            finish(source, target, row)
            keep(made)
            return carry

        lax.fori_loop(0, trips - 1, trip, 0)
        row = trim + (trips - 1) * RUN
        made = ahead(plans[p + 1][0], plans[p + 1][2]) if p + 1 < PROP_STEPS else None
        finish(source, target, row)
        if made is not None:
            keep(made)


def turn_in(spectrum, near, staged, field, sems, stride):
    comps, rows, cols = spectrum.shape
    slots, block = staged.shape[:2]
    blocks = comps // block
    for at in (0, (rows + 2 * HALO + 1) * stride):
        field[pl.ds(at, stride), :] = jnp.zeros((stride, cols), F32)

    def fetch(b):
        slot = lax.rem(b, slots)
        return pltpu.make_async_copy(spectrum.at[pl.ds(b * block, block)], staged.at[slot], sems.at[slot])

    for b in range(min(slots, blocks)):
        fetch(b).start()

    def turn(b, carry):
        fetch(b).wait()
        slot = lax.rem(b, slots)

        def one(k, carry):
            c = b * block + k
            v = jnp.concatenate(
                [near[0, c].astype(F32), staged[slot, k].astype(F32), near[1, c].astype(F32)], axis=0
            )
            field[pl.ds(stride + c, rows + 2 * HALO, stride=stride), :] = v
            return carry

        lax.fori_loop(0, block, one, 0)

        @pl.when(b + slots < blocks)
        def _():
            fetch(b + slots).start()

        return carry

    lax.fori_loop(0, blocks, turn, 0)


def band_at(k, bands):
    return jnp.where(k == 0, 0, jnp.where(k == 1, bands - 1, k - 1))


def partner(me, k, peers):
    if peers & (peers - 1):
        return lax.rem(me + k, peers)
    other, bit = me, 1
    while bit < peers:
        if k & bit:
            other = other + bit - 2 * bit * lax.rem(lax.div(other, bit), 2)
        bit *= 2
    return other


def one_hot(pos, first, count):
    cols = pos.shape[1]
    slot = lax.broadcasted_iota(jnp.int32, (count, cols), 0) + first
    at = jnp.broadcast_to(pos[None], (count // 8, 8, cols)).reshape(count, cols)
    return jnp.where(slot == at, 1.0, 0.0).astype(BF16)


def squeeze_block(rows_of, pos, at, factor, tiles, start, peers):
    count, _, cols = rows_of.shape
    for n in range(0, TILES, 2):
        wide = min(2, TILES - n)
        lanes = slice(n * cols, count * cols)
        for q in range(n, count):
            factor[: wide * cols, q * cols : (q + 1) * cols] = one_hot(pos[at + q], n * cols, wide * cols)
        x = jnp.concatenate([rows_of[q] for q in range(n, count)], axis=1)
        moved = lax.dot_general(
            x, factor[: wide * cols, lanes], (((1,), (1,)), ((), ())), preferred_element_type=F32
        ).astype(BF16)
        for h in range(wide):
            t = start + n + h
            tiles[lax.div(t, peers), lax.rem(t, peers)] = moved[:, h * cols : (h + 1) * cols]


def widen_rows(tiles, start, peers, pos, at, first, count, factor):
    cols = factor.shape[1] // 2
    reach = min(first + count, TILES)
    for n in range(reach):
        for q in range(count):
            factor[n * cols : (n + 1) * cols, q * cols : (q + 1) * cols] = one_hot(pos[at + q], n * cols, cols)
    x = []
    for n in range(reach):
        t = start + n
        x.append(tiles[lax.div(t, peers), lax.rem(t, peers)])
    x = jnp.concatenate(x, axis=1) if reach > 1 else x[0]
    return jnp.dot(x, factor[: reach * cols, : count * cols], preferred_element_type=F32).astype(BF16)


def advance_kernel(order, periodic, squeeze, spectrum, near, mask, coef, loss, first_in, second_in, merge_in, *refs):
    if squeeze:
        pos, edge_pos, *refs = refs
    density, back, edge, *refs = refs
    staged, field, work_a, work_b, done, side, tiles, spectra, incs, first, second, merge, merge_part, product, *refs = refs
    if squeeze:
        rows_of, home, edge_in, edge_out, flat, gather, spread, flat_sems, *refs = refs
    else:
        home = back
    stage_sems, density_sems, end_sems, weight_sems, send_sem, recv_sem, return_sem, back_sem, edge_send, edge_recv = refs
    peers = lax.axis_size("comp")
    me = lax.axis_index("comp")
    geo, ends = lax.axis_index("geo"), lax.axis_size("geo") - 1
    chunks, width, comps, cols = spectra.shape
    local = comps // peers
    terms = product.shape[0]
    has_low, has_high = geo > 0, geo < ends

    barrier = pltpu.get_barrier_semaphore()
    for k in range(1, peers):
        pl.semaphore_signal(barrier, inc=1, device_id={"comp": partner(me, k, peers)}, device_id_type=MESH)

    @pl.when(has_low)
    def _():
        pl.semaphore_signal(barrier, inc=1, device_id={"geo": geo - 1}, device_id_type=MESH)

    @pl.when(has_high)
    def _():
        pl.semaphore_signal(barrier, inc=1, device_id={"geo": geo + 1}, device_id_type=MESH)

    def part(who):
        return pl.ds(pl.multiple_of(who * local, 16), local)

    def outward(c, who):
        return pltpu.make_async_remote_copy(
            src_ref=tiles.at[pl.ds(c * width, width), who],
            dst_ref=spectra.at[c, :, part(me)],
            send_sem=send_sem, recv_sem=recv_sem.at[c],
            device_id={"comp": who}, device_id_type=MESH,
        )

    def homeward(c, who):
        return pltpu.make_async_remote_copy(
            src_ref=incs.at[c, :, part(who)],
            dst_ref=home.at[pl.ds(c * width, width), me],
            send_sem=return_sem, recv_sem=back_sem.at[c],
            device_id={"comp": who}, device_id_type=MESH,
        )

    def own_home(c):
        return pltpu.make_async_copy(incs.at[c, :, part(me)], back.at[pl.ds(c * width, width), me], back_sem.at[c])

    loads = [
        pltpu.make_async_copy(src, dst, weight_sems.at[k])
        for k, (src, dst) in enumerate(((first_in, first), (second_in, second)))
    ]
    rows = mask.shape[0] - 2 * HALO
    stride = stride_of(local) + 8
    bands = rows // BAND
    turn_in(spectrum, near, staged, field, stage_sems, stride)
    for load in loads:
        load.start()
    zeros = jnp.zeros((stride, cols), F32)
    for work in (work_a, work_b):
        work[pl.ds(0, stride), :] = zeros
        work[pl.ds((SPAN + 1) * stride, stride), :] = zeros
    pl.semaphore_wait(barrier, peers - 1 + jnp.minimum(geo, 1) + jnp.minimum(ends - geo, 1))

    sets, ways = group_sets(local, periodic)

    def whole(k):
        return pltpu.make_async_copy(
            done.at[pl.ds(2 * stride, BAND * stride)],
            density.at[pl.ds((band_at(k, bands) * BAND + 1) * stride, BAND * stride)],
            density_sems.at[k],
        )

    def end(far):
        row = rows + 1 if far else 0
        return pltpu.make_async_copy(
            done.at[pl.ds((BAND + 2 if far else 1) * stride, stride)],
            density.at[pl.ds(row * stride, stride)],
            end_sems.at[far],
        )

    far_band = min(1, bands - 1)

    def settle(k):
        whole(k).wait()

        @pl.when(k == 0)
        def _():
            end(0).wait()

        @pl.when(k == far_band)
        def _():
            end(1).wait()

    def ready(k):
        return lax.div(k * (rows // bands * TILES // BLOCK if squeeze else BAND), peers * width)

    def needed(k):
        return lax.div(k * (BAND // BLOCK * TILES) + peers * width - 1, peers * width)

    def form(k, carry):
        band = band_at(k, bands)

        @pl.when(k > 0)
        def _():
            settle(k - 1)

        for group_set in sets:
            substeps(
                field, (work_a, work_b), done, mask, coef, side, group_set, ways,
                band * BAND, band * BAND + 1, 0, stride,
            )
        whole(k).start()

        @pl.when(k == 0)
        def _():
            end(0).start()

        @pl.when(k == far_band)
        def _():
            end(1).start()

        if squeeze:

            def block(b, carry):
                def pack(q, carry):
                    r = b * BLOCK + q
                    r = jnp.where(k == 1, BAND - 1 - r, r)
                    from_at = pl.multiple_of((2 + r) * stride, 8)
                    rows_of[q] = done[pl.ds(from_at, local), :].astype(BF16)
                    return carry

                lax.fori_loop(0, BLOCK, pack, 0)
                whole_block = k * (BAND // BLOCK) + b
                squeeze_block(rows_of, pos, whole_block * BLOCK, gather, tiles, whole_block * TILES, peers)
                return carry

            lax.fori_loop(0, BAND // BLOCK, block, 0)
        else:

            def pack(r, carry):
                t = k * BAND + r
                from_at = pl.multiple_of((2 + r) * stride, 8)
                tiles[lax.div(t, peers), lax.rem(t, peers)] = done[pl.ds(from_at, local), :].astype(BF16)
                return carry

            lax.fori_loop(0, BAND, pack, 0)

        for group in order:

            def launch(c, carry, group=group):
                for who in group:
                    outward(c, partner(me, who, peers)).start()
                return carry

            lax.fori_loop(ready(k), ready(k + 1), launch, 0)

        def own(c, carry):
            for h in range(width):
                spectra[c, h, part(me), :] = tiles[c * width + h, me]
            return carry

        lax.fori_loop(ready(k), ready(k + 1), own, 0)
        return carry

    lax.fori_loop(0, bands, form, 0)

    def fetch(m):
        slot = lax.rem(m, 2)
        return pltpu.make_async_copy(
            merge_in.at[:, pl.ds(pl.multiple_of(m * cols, cols), cols)], merge_part.at[slot], weight_sems.at[2 + slot]
        )

    fetch(0).start()

    def flip(m, carry):
        @pl.when(m + 1 < comps // cols)
        def _():
            fetch(m + 1).start()

        fetch(m).wait()
        to = pl.ds(pl.multiple_of(m * cols, cols), cols)
        for t in range(0, terms, cols):
            size = min(cols, terms - t)
            merge[to, t : t + size] = merge_part[lax.rem(m, 2), t : t + size, :].T
        return carry

    lax.fori_loop(0, comps // cols, flip, 0)
    for load in loads:
        load.wait()

    tile = max(t for t in range(16, 600, 16) if terms % t == 0)
    step = max(g for g in range(1, peers + 1) if peers % g == 0 and g * local <= 600) * local

    def work(c, carry):
        arrived = spectra.at[c, :, pl.ds(0, comps - local)]
        pltpu.make_async_copy(arrived, arrived, recv_sem.at[c]).wait()

        def multiply(t, carry):
            at = pl.ds(pl.multiple_of(t * tile, 16), tile)
            x = jnp.concatenate([spectra[c, h] for h in range(width)], axis=1) if width > 1 else spectra[c, 0]
            one = jnp.dot(first[at, :], x, preferred_element_type=F32)
            two = jnp.dot(second[at, :], x, preferred_element_type=F32)
            product[at, :] = (one * two).astype(BF16)
            return carry

        lax.fori_loop(0, terms // tile, multiply, 0)
        roots = []
        for h in range(width):
            energy = jnp.sum(spectra[c, h].astype(F32), axis=0, keepdims=True)
            roots.append(jnp.sqrt(energy / comps + 1e-06))
        for d in range(0, comps, step):
            at = slice(d, d + step)
            moved = jnp.dot(merge[at, :], product[...], preferred_element_type=F32)
            for h in range(width):
                lanes = slice(h * cols, (h + 1) * cols)
                total = moved[:, lanes] - loss[at, :] * roots[h] * spectra[c, h, at, :].astype(F32)
                incs[c, h, at, :] = total.astype(BF16)
        for group in order:
            for k in group:
                homeward(c, partner(me, k, peers)).start()
        if squeeze:
            for h in range(width):
                home[c * width + h, me] = incs[c, h, part(me), :]
        else:
            own_home(c).start()
        return carry

    lax.fori_loop(0, chunks, work, 0)

    def land(c, carry):
        there = home.at[pl.ds(c * width, width), pl.ds(0, peers - 1 if squeeze else peers)]
        pltpu.make_async_copy(there, there, back_sem.at[c]).wait()
        return carry

    if squeeze:
        last = BAND // BLOCK * TILES
    else:
        last = min(2, bands) * BAND - 1
    landed = last // (peers * width) + 1
    lax.fori_loop(0, landed, land, 0)
    arriving = edge_in if squeeze else edge
    to_low = pltpu.make_async_remote_copy(
        src_ref=home.at[0, 0], dst_ref=arriving.at[1], send_sem=edge_send.at[1], recv_sem=edge_recv.at[1],
        device_id={"geo": geo - 1}, device_id_type=MESH,
    )
    to_high = pltpu.make_async_remote_copy(
        src_ref=home.at[last // peers, last % peers], dst_ref=arriving.at[0],
        send_sem=edge_send.at[0], recv_sem=edge_recv.at[0],
        device_id={"geo": geo + 1}, device_id_type=MESH,
    )

    @pl.when(has_low)
    def _():
        to_low.start()

    @pl.when(has_high)
    def _():
        to_high.start()

    if not squeeze:
        lax.fori_loop(landed, chunks, land, 0)
    settle(bands - 1)

    def edges_in():
        @pl.when(has_low)
        def _():
            to_low.wait_send()
            to_high.wait_recv()

        @pl.when(has_high)
        def _():
            to_high.wait_send()
            to_low.wait_recv()

    if squeeze:

        def put(k):
            return pltpu.make_async_copy(
                flat.at[lax.rem(k, 2)], back.at[pl.ds(k * BAND, BAND)], flat_sems.at[k]
            )

        def widen(k, carry):
            lax.fori_loop(jnp.maximum(needed(k), landed), jnp.maximum(needed(k + 1), landed), land, 0)

            @pl.when(k >= 2)
            def _():
                put(k - 2).wait()

            def block(b, carry):
                whole_block = k * (BAND // BLOCK) + b
                for j in range(0, BLOCK, 2):
                    made = widen_rows(
                        home, whole_block * TILES, peers, pos, whole_block * BLOCK + j, j, 2, spread
                    )
                    for h in range(2):
                        r = b * BLOCK + j + h
                        r = jnp.where(k == 1, BAND - 1 - r, r)
                        flat[lax.rem(k, 2), r] = made[:, h * cols : (h + 1) * cols]
                return carry

            lax.fori_loop(0, BAND // BLOCK, block, 0)
            put(k).start()
            return carry

        def edge_put(which):
            return pltpu.make_async_copy(edge_out.at[which], edge.at[which], end_sems.at[which])

        @pl.when(geo == 0)
        def _():
            edge_in[0] = jnp.zeros((local, cols), BF16)

        @pl.when(geo == ends)
        def _():
            edge_in[1] = jnp.zeros((local, cols), BF16)

        lax.fori_loop(0, bands - 1, widen, 0)
        edges_in()
        for which in range(2):
            spread[:cols, :cols] = one_hot(edge_pos[which], 0, cols)
            edge_out[which] = jnp.dot(
                edge_in[which], spread[:cols, :cols], preferred_element_type=F32
            ).astype(BF16)
            edge_put(which).start()
        lax.fori_loop(bands - 1, bands, widen, 0)
        for k in range(bands - 2, bands):
            put(k).wait()
        for which in range(2):
            edge_put(which).wait()
    else:
        edges_in()

    def sent(c, carry):
        for k in range(1, peers):
            outward(c, partner(me, k, peers)).wait_send()
            homeward(c, partner(me, k, peers)).wait_send()
        return carry

    lax.fori_loop(0, chunks, sent, 0)


def advance(spectrum, near, mask, coef, loss, first, second, merge, places, periodic):
    local, rows, cols = spectrum.shape
    peers = lax.axis_size("comp")
    squeeze = places is not None
    width = 1 if squeeze else CHUNK
    depth = (rows // BLOCK * TILES if squeeze else rows) // peers
    chunks = depth // width
    comps, terms = merge.shape
    stride = stride_of(local) + 8
    if peers == 8:
        order = [(1, 2, 3), (4, 5, 6, 7)]
    else:
        order = [tuple(range(1, peers))]
    sets, _ = group_sets(local, periodic)
    extra = []
    if squeeze:
        extra = [
            VMEM((BLOCK, local, cols), BF16),
            VMEM((depth, peers, local, cols), BF16),
            VMEM((2, local, cols), BF16),
            VMEM((2, local, cols), BF16),
            VMEM((2, BAND, local, cols), BF16),
            VMEM((2 * cols, BLOCK * cols), BF16),
            VMEM((TILES * cols, 2 * cols), BF16),
            DMA((rows // BAND,)),
        ]
    back_shape = (rows, local, cols) if squeeze else (depth, peers, local, cols)
    density, back, edge = pl.pallas_call(
        functools.partial(advance_kernel, order, periodic, squeeze),
        in_specs=[ANY, WHOLE, WHOLE, WHOLE, WHOLE, ANY, ANY, ANY] + ([WHOLE, WHOLE] if squeeze else []),
        out_specs=[ANY, ANY, ANY],
        out_shape=[
            jax.ShapeDtypeStruct(((rows + 2) * stride, cols), F32),
            jax.ShapeDtypeStruct(back_shape, BF16),
            jax.ShapeDtypeStruct((2, local, cols), BF16),
        ],
        scratch_shapes=[
            VMEM((2, 16, rows, cols), BF16),
            VMEM(((rows + 2 * HALO + 2) * stride, cols), F32),
            VMEM(((SPAN + 2) * stride, cols), F32),
            VMEM(((SPAN + 2) * stride, cols), F32),
            VMEM(((SPAN - RUN) * stride, cols), F32),
            VMEM((RUN * len(sets[0]), 8, cols), F32),
            VMEM((depth, peers, local, cols), BF16),
            VMEM((chunks, width, comps, cols), BF16),
            VMEM((chunks, width, comps, cols), BF16),
            VMEM((terms, comps), BF16),
            VMEM((terms, comps), BF16),
            VMEM((comps, terms), BF16),
            VMEM((2, terms, cols), BF16),
            VMEM((terms, width * cols), BF16),
        ]
        + extra
        + [
            DMA((2,)),
            DMA((rows // BAND,)),
            DMA((2,)),
            DMA((4,)),
            DMA,
            DMA((chunks,)),
            DMA,
            DMA((chunks,)),
            DMA((2,)),
            DMA((2,)),
        ],
        cost_estimate=pl.CostEstimate(
            flops=6 * comps * terms * depth * cols, bytes_accessed=6 * comps * terms, transcendentals=0
        ),
        compiler_params=pltpu.CompilerParams(
            collective_id=3 if squeeze else 2, has_side_effects=True, vmem_limit_bytes=67043328
        ),
        name="advance_sea" if squeeze else "advance_all",
    )(spectrum, near, mask, coef, loss, first, second, merge.T, *(places or ()))
    return density, back.reshape(rows, local, cols), edge


def sea_places(sea, near_low, near_high):
    rows, cols = sea.shape
    bands = rows // BAND
    parts = [sea[:BAND], jnp.flip(sea[rows - BAND :], axis=0), sea[BAND : rows - BAND]]
    sea = jnp.concatenate(parts)
    steps = jnp.triu(jnp.ones((cols, cols), F32))
    inner = jnp.dot(jnp.concatenate([sea, near_low, near_high]), steps)
    total = inner[:rows, cols - 1].reshape(rows // BLOCK, BLOCK)
    before = jnp.dot(total, jnp.triu(jnp.ones((BLOCK, BLOCK), F32), 1))
    place = jnp.where(sea > 0, inner[:rows] + before.reshape(rows, 1), 0.0) - 1.0
    edge = jnp.where(jnp.concatenate([near_low, near_high]) > 0, inner[rows:], 0.0) - 1.0
    return tall(place.astype(jnp.int32)), tall(edge.astype(jnp.int32))


def close_kernel(periodic, ends, density, back, edge, wind, mask, coef, out, cells, forced, turned, incs, side, staged, sems, out_sems):
    comps, rows, cols = staged.shape
    stride = stride_of(comps) + 8
    sets, ways = group_sets(comps, periodic)
    size = len(sets[0])
    bands = rows // BAND
    views = [ref.reshape(rows + 2, stride, cols) for ref in (density, cells)]

    def fetches(b):
        at = pl.ds(sets[b][0] * 8, size * 8)
        moves = [
            (views[0].at[:, at], views[1].at[:, at]),
            (edge.at[0, at], incs.at[0, at]),
            (back.at[pl.ds(0, BAND), at], incs.at[pl.ds(1, BAND), at]),
            (edge.at[1, at], incs.at[rows + 1, at]),
        ]
        if bands > 1:
            moves.append((back.at[pl.ds(BAND, BAND), at], incs.at[pl.ds(rows + 1 - BAND, BAND), at]))
        if bands > 2:
            between = rows - 2 * BAND
            moves.append((back.at[pl.ds(2 * BAND, between), at], incs.at[pl.ds(1 + BAND, between), at]))
        return [pltpu.make_async_copy(src, dst, sems.at[b, k]) for k, (src, dst) in enumerate(moves)]

    for b in range(len(sets)):
        for f in fetches(b):
            f.start()

    run = max(k for k in range(1, 17) if (rows + 2) % k == 0)
    trips = (rows + 2) // run

    def at(row, g):
        return pl.ds(pl.multiple_of(row * stride + g * 8, 8), 8)

    def set_of(b):
        group_set = sets[b]
        for f in fetches(b):
            f.wait()
        span = pl.ds(group_set[0] * 8, size * 8)
        for end, row in ((0, 0), (1, rows + 1)):

            @pl.when(ends[end] == 1)
            def _(row=row):
                incs[row, span, :] = jnp.zeros((size * 8, cols), BF16)

        factor = {g: [coef[k, pl.ds(g * 8, 8), :] for k in range(8)] for g in group_set}

        def ahead(row):
            made = []
            for r in range(run):
                blow, turn_x, turn_y = wind[0, row + r], wind[1, row + r], wind[2, row + r]
                for g in group_set:
                    if g % 2 == 0:
                        both = incs[row + r, pl.ds(g * 8, 16), :].astype(F32)
                    rate, cos_h, sin_h = factor[g][5:8]
                    d = cells[at(row + r, g), :]
                    facing = jnp.maximum(cos_h * turn_x + sin_h * turn_y, 0.0)
                    growth = rate * blow * (facing * facing)
                    new = d + growth * d + both[(g % 2) * 8 : (g % 2) * 8 + 8]
                    forced[at(row + r + 1, g), :] = new
                    west, east = ways[g][:2]
                    made.append(column_terms(new, factor[g][1], factor[g][2], west, east))
            return made

        def keep(made):
            for k, v in enumerate(made):
                side[k] = v

        def finish(row):
            for j, g in enumerate(group_set):
                c, _, _, s, n = factor[g][:5]
                south, north = ways[g][2:]
                held = forced[at(row, g), :] if south else None
                here = forced[at(row + 1, g), :]
                for r in range(run):
                    after = forced[at(row + r + 2, g), :] if north or r < run - 1 else None
                    v = c * here + side[r * size + j]
                    if south:
                        v = v + s * held
                    if north:
                        v = v + n * after
                    turned[at(row + r, g), :] = v * mask[row + r]
                    held, here = here, after

        def trip(t, carry):
            made = ahead((t + 1) * run)
            finish(t * run)
            keep(made)
            return carry

        keep(ahead(0))
        lax.fori_loop(0, trips - 1, trip, 0)
        finish((trips - 1) * run)

    def give(b):
        part = pl.ds(b * size * 8, size * 8)
        return pltpu.make_async_copy(staged.at[part], out.at[part], out_sems.at[b])

    zeros = jnp.zeros((stride, cols), F32)
    forced[pl.ds(0, stride), :] = zeros
    forced[pl.ds((rows + 3) * stride, stride), :] = zeros
    for b in range(len(sets)):
        set_of(b)

        def lift(k, carry, b=b):
            c = b * size * 8 + k
            staged[c] = turned[pl.ds(stride + c, rows, stride=stride), :].astype(BF16)
            return carry

        lax.fori_loop(0, size * 8, lift, 0)
        give(b).start()
    for b in range(len(sets)):
        give(b).wait()


def close(density, back, edge, wind, mask, coef, ends, periodic):
    rows, comps, cols = back.shape
    stride = stride_of(comps) + 8
    sets, _ = group_sets(comps, periodic)
    run = max(k for k in range(1, 17) if (rows + 2) % k == 0)
    return pl.pallas_call(
        functools.partial(close_kernel, periodic),
        in_specs=[pl.BlockSpec(memory_space=SMEM), ANY, ANY, ANY, WHOLE, WHOLE, WHOLE],
        out_specs=ANY,
        out_shape=jax.ShapeDtypeStruct((comps, rows, cols), BF16),
        scratch_shapes=[
            VMEM(((rows + 2) * stride, cols), F32),
            VMEM(((rows + 4) * stride, cols), F32),
            VMEM(((rows + 2) * stride, cols), F32),
            VMEM((rows + 2, comps, cols), BF16),
            VMEM((run * len(sets[0]), 8, cols), F32),
            VMEM((comps, rows, cols), BF16),
            DMA((len(sets), 6)),
            DMA((len(sets),)),
        ],
        compiler_params=pltpu.CompilerParams(vmem_limit_bytes=56 * 1024 * 1024),
        name="close",
    )(ends, density, back, edge, wind, mask, coef)


def tall(rows_of):
    return jnp.broadcast_to(rows_of[:, None, :], (rows_of.shape[0], 8, rows_of.shape[1]))


def body(spectrum, land_mask, wind_speed, wind_dir, input_rate, dissipation, pair_first, pair_second, merge_weight):
    local, rows, cols = spectrum.shape
    peers = lax.axis_size("comp")
    fits = local % 16 == 0 and rows % BAND == 0 and BAND % (peers * CHUNK) == 0 and cols == 128
    if not fits:
        return plain_body(
            spectrum, land_mask, wind_speed, wind_dir, input_rate, dissipation, pair_first, pair_second, merge_weight
        )
    periodic = local % ND == 0
    near, near_mask, near_speed, near_angle, seas = geo_halo(spectrum, land_mask, wind_speed, wind_dir)

    ids = lax.axis_index("comp") * local + jnp.arange(local, dtype=jnp.int32)
    frequency = (ids // ND).astype(F32)
    heading = 2.0 * math.pi * (ids % ND).astype(F32) / ND
    courant = 0.7 * jnp.power(F32(1.1), -frequency)
    cos_h, sin_h = jnp.cos(heading), jnp.sin(heading)
    west, east = jnp.maximum(courant * cos_h, 0.0), jnp.maximum(-courant * cos_h, 0.0)
    south, north = jnp.maximum(courant * sin_h, 0.0), jnp.maximum(-courant * sin_h, 0.0)
    center = 1.0 - west - east - south - north
    coef = jnp.stack([center, west, east, south, north, input_rate, cos_h, sin_h])
    coef = jnp.broadcast_to(coef[:, :, None], (8, local, cols))

    sea = jnp.concatenate([near_mask[0], land_mask, near_mask[1]]).astype(F32)
    sea = tall(sea)
    angle = jnp.concatenate([near_angle[0, HALO - 1 :], wind_dir, near_angle[1, :1]])
    speed = jnp.concatenate([near_speed[0, HALO - 1 :], wind_speed, near_speed[1, :1]])
    wind = jnp.stack([tall(speed), tall(jnp.cos(angle)), tall(jnp.sin(angle))])
    geo = lax.axis_index("geo")
    ends = jnp.stack([geo == 0, geo == lax.axis_size("geo") - 1]).astype(jnp.int32)

    given = (spectrum, near, sea, coef, dissipation[:, None], pair_first, pair_second, merge_weight)
    whole = lambda *a: advance(*a[:8], None, periodic)
    packed = lambda *a: advance(*a[:8], a[8:], periodic)
    count = rows // BLOCK * TILES
    if rows >= 2 * BAND and BLOCK == 16 and count % peers == 0 and local % 16 == 0:
        near_sea = near_mask.astype(F32)
        places = sea_places(land_mask.astype(F32), near_sea[0, HALO - 1 :], near_sea[1, :1])
        held = jnp.sum(seas.reshape(-1, BLOCK * cols), axis=1)
        density, back, edge = lax.cond(jnp.max(held) <= TILES * cols, packed, whole, *given, *places)
    else:
        density, back, edge = whole(*given)
    below = HALO - 1
    return close(density, back, edge, wind, sea[below : below + rows + 2], coef, ends, periodic)


def solution(mesh):
    placed = (P("comp", "geo", None), P("geo", None), P("geo", None), P("geo", None), P("comp"), P(), P(), P(), P())
    return jax.shard_map(
        body, mesh=mesh, in_specs=placed, out_specs=P("comp", "geo", None), check_vma=False
    )
```

```python
import functools
import math

import jax
import jax.numpy as jnp
from jax import lax
from jax.experimental import pallas as pl
from jax.experimental.pallas import tpu as pltpu
from jax.sharding import PartitionSpec as P

ND = 36
PROP_STEPS = 6
HALO = 8
SENDS = 3
RETURNS = 2
F32 = jnp.float32
BF16 = jnp.bfloat16
VMEM = pltpu.VMEM
ANY = pl.BlockSpec(memory_space=pl.ANY)
WHOLE = pl.BlockSpec(memory_space=pltpu.VMEM)
MESH = pl.DeviceIdType.MESH
DMA = pltpu.SemaphoreType.DMA
CHUNK = 2
BAND = 16
BLOCK = 16
TILES = 13
RUN = 8
SPAN = BAND + 2 * HALO
OFF = HALO - RUN // 2
SMEM = pltpu.SMEM


def edges(cells, axis_dim):
    count = lax.axis_size("geo")
    ends = count - 1
    size = cells.shape[axis_dim]
    head = lax.slice_in_dim(cells, 0, HALO, axis=axis_dim)
    tail = lax.slice_in_dim(cells, size - HALO, size, axis=axis_dim)
    lower = lax.ppermute(tail, "geo", [(i, i + 1) for i in range(ends)])
    upper = lax.ppermute(head, "geo", [(i + 1, i) for i in range(ends)])
    return lower, upper


def block_of(comps):
    return 16 if comps % 16 == 0 else comps


def stride_of(block):
    return -(-block // 8) * 8


def upwind(v, mask, coef, at):
    center, west, east, south, north = (coef[at + k] for k in range(5))
    rows = v.shape[0]
    moved = west * pltpu.roll(v, 1, 1) + east * pltpu.roll(v, v.shape[1] - 1, 1)
    moved = moved + south * pltpu.roll(v, 1, 0) + north * pltpu.roll(v, rows - 1, 0)
    return (center * v + moved) * mask


def prop_kernel(coef, lower, cells, upper, mask, density, outgoing, turned):
    block, rows, cols = cells.shape
    stride = stride_of(block)
    first = pl.program_id(0) * block

    def one(c, carry):
        v = jnp.concatenate(
            [lower[c].astype(F32), cells[c].astype(F32), upper[c].astype(F32)], axis=0
        )
        sea = mask[...]
        for _ in range(PROP_STEPS):
            v = upwind(v, sea, coef, (first + c) * 8)
        density[c] = v
        turned[pl.ds(c, rows, stride=stride), :] = v[HALO : HALO + rows]
        return carry

    lax.fori_loop(0, block, one, 0)

    def pack(r, carry):
        start = pl.multiple_of(r * stride, 8)
        outgoing[r] = turned[pl.ds(start, block), :].astype(BF16)
        return carry

    lax.fori_loop(0, rows, pack, 0, unroll=8)


def propagate(coef, lower, cells, upper, mask):
    comps, rows, cols = cells.shape
    block = block_of(comps)
    tall = rows + 2 * HALO
    return pl.pallas_call(
        prop_kernel,
        grid=(comps // block,),
        in_specs=[
            pl.BlockSpec(memory_space=SMEM),
            pl.BlockSpec((block, HALO, cols), lambda i: (i, 0, 0)),
            pl.BlockSpec((block, rows, cols), lambda i: (i, 0, 0)),
            pl.BlockSpec((block, HALO, cols), lambda i: (i, 0, 0)),
            pl.BlockSpec((tall, cols), lambda i: (0, 0)),
        ],
        out_specs=[
            pl.BlockSpec((block, tall, cols), lambda i: (i, 0, 0)),
            pl.BlockSpec((rows, block, cols), lambda i: (0, i, 0)),
        ],
        out_shape=[
            jax.ShapeDtypeStruct((comps, tall, cols), F32),
            jax.ShapeDtypeStruct((rows, comps, cols), BF16),
        ],
        scratch_shapes=[VMEM((rows * stride_of(block), cols), F32)],
        cost_estimate=pl.CostEstimate(
            flops=comps * tall * cols * 100,
            bytes_accessed=comps * tall * cols * 8,
            transcendentals=0,
        ),
        name="propagate",
    )(coef, lower, cells, upper, mask)


def point_kernel(sends, *refs):
    near, far = refs[:sends], refs[sends : 2 * sends]
    loss, first, second, merge, out, spectra, product = refs[2 * sends :]
    peers, _, part, cols = near[0].shape
    local = sends * part
    comps, terms = merge.shape
    for side, group in enumerate((near, far)):
        lanes = slice(side * cols, (side + 1) * cols)
        for k in range(sends):
            for s in range(peers):
                at = s * local + k * part
                spectra[at : at + part, lanes] = group[k][s, 0]
    tile = max(t for t in range(16, 600, 16) if terms % t == 0)

    def multiply(t, carry):
        rows = pl.ds(pl.multiple_of(t * tile, 16), tile)
        x = spectra[...]
        one = jnp.dot(first[rows, :], x, preferred_element_type=F32)
        two = jnp.dot(second[rows, :], x, preferred_element_type=F32)
        product[rows, :] = (one * two).astype(BF16)
        return carry

    lax.fori_loop(0, terms // tile, multiply, 0)
    energy = jnp.sum(spectra[...].astype(F32), axis=0, keepdims=True)
    root = jnp.sqrt(energy / comps + 1e-06)
    if peers == 1:
        step = max(t for t in range(16, 600, 16) if comps % t == 0)
        for d in range(0, comps, step):
            rows = slice(d, d + step)
            moved = jnp.dot(merge[rows, :], product[...], preferred_element_type=F32)
            total = moved - loss[rows, :] * root * spectra[rows, :].astype(F32)
            out[0, 0, rows] = total[:, :cols].astype(BF16)
            out[0, 1, rows] = total[:, cols:].astype(BF16)
        return
    share = max(g for g in range(1, peers + 1) if peers % g == 0 and g * local <= 600)
    for d in range(0, peers, share):
        rows = slice(d * local, (d + share) * local)
        moved = jnp.dot(merge[rows, :], product[...], preferred_element_type=F32)
        total = moved - loss[rows, :] * root * spectra[rows, :].astype(F32)
        for g in range(share):
            piece = total[g * local : (g + 1) * local].astype(BF16)
            out[d + g, 0] = piece[:, :cols]
            out[d + g, 1] = piece[:, cols:]


def point_terms(chunks, start, pairs, loss, first, second, merge):
    sends = len(chunks)
    peers, rows, part, cols = chunks[0].shape
    local = sends * part
    comps, terms = merge.shape
    whole = lambda shape: pl.BlockSpec(shape, lambda i: (0, 0))
    near = pl.BlockSpec((peers, 1, part, cols), lambda i: (0, start + i, 0, 0))
    far = pl.BlockSpec((peers, 1, part, cols), lambda i: (0, rows - 1 - start - i, 0, 0))
    return pl.pallas_call(
        functools.partial(point_kernel, sends),
        grid=(pairs,),
        in_specs=[near] * sends
        + [far] * sends
        + [whole((comps, 1)), whole((terms, comps)), whole((terms, comps)), whole((comps, terms))],
        out_specs=pl.BlockSpec((peers, 2, local, cols), lambda i: (0, i, 0, 0)),
        out_shape=jax.ShapeDtypeStruct((peers, 2 * pairs, local, cols), BF16),
        scratch_shapes=[VMEM((comps, 2 * cols), BF16), VMEM((terms, 2 * cols), BF16)],
        cost_estimate=pl.CostEstimate(
            flops=pairs * 12 * comps * terms * cols,
            bytes_accessed=6 * comps * terms + pairs * 8 * comps * cols,
            transcendentals=0,
        ),
        compiler_params=pltpu.CompilerParams(vmem_limit_bytes=60 * 1024 * 1024),
        name="points",
    )(*chunks, *chunks, loss, first, second, merge)


def final_kernel(returns, coef, density, low_inc, high_inc, wind, mask, *refs):
    incs = refs[:returns]
    out, turned = refs[returns:]
    block, rows, cols = out.shape
    peers, held = incs[0].shape[:2]
    band = rows // peers
    stride = stride_of(block)
    first = pl.program_id(0) * block

    def place(s, carry):
        for k in range(returns):
            for j in range(held):
                a = k * (held // 2) + j // 2
                row = a if j % 2 == 0 else band - 1 - a
                at = pl.multiple_of((s * band + row) * stride, 8)
                turned[pl.ds(at, block), :] = incs[k][s, j].astype(F32)
        return carry

    lax.fori_loop(0, peers, place, 0)

    def one(c, carry):
        at = (first + c) * 8
        inc = jnp.concatenate(
            [low_inc[c], turned[pl.ds(c, rows, stride=stride), :], high_inc[c]], axis=0
        )
        v = density[c]
        facing = jnp.maximum(coef[at + 6] * wind[1] + coef[at + 7] * wind[2], 0.0)
        growth = coef[at + 5] * wind[0] * facing * facing
        v = v + growth * v + inc
        v = upwind(v, mask[...], coef, at)
        out[c] = v[HALO : HALO + rows].astype(BF16)
        return carry

    lax.fori_loop(0, block, one, 0)


def finish(coef, density, low_inc, high_inc, wind, mask, incs, lead):
    local, tall, cols = density.shape
    rows = tall - 2 * HALO
    block = block_of(local)
    peers, held = incs[0].shape[:2]
    return pl.pallas_call(
        functools.partial(final_kernel, len(incs)),
        grid=(local // block,),
        in_specs=[
            pl.BlockSpec(memory_space=SMEM),
            pl.BlockSpec((block, tall, cols), lambda i: (i, 0, 0)),
            pl.BlockSpec((block, HALO, cols), lambda i: (i, 0, 0)),
            pl.BlockSpec((block, HALO, cols), lambda i: (i, 0, 0)),
            pl.BlockSpec((3, tall, cols), lambda i: (0, 0, 0)),
            pl.BlockSpec((tall, cols), lambda i: (0, 0)),
        ]
        + [pl.BlockSpec((peers, held, block, cols), lambda i: (0, 0, i, 0))] * len(incs),
        out_specs=pl.BlockSpec((block, rows, cols), lambda i: (i, 0, 0)),
        out_shape=jax.ShapeDtypeStruct((local, rows, cols), BF16),
        scratch_shapes=[VMEM((rows * stride_of(block), cols), F32)],
        name="finish",
    )(coef, density, low_inc, high_inc, wind, mask, *incs)


def plain_body(spectrum, land_mask, wind_speed, wind_dir, input_rate, dissipation, pair_first, pair_second, merge_weight):
    local, rows, cols = spectrum.shape
    peers = lax.axis_size("comp")
    band = rows // peers
    ids = lax.axis_index("comp") * local + jnp.arange(local, dtype=jnp.int32)
    frequency = (ids // ND).astype(F32)
    heading = 2.0 * math.pi * (ids % ND).astype(F32) / ND
    courant = 0.7 * jnp.power(F32(1.1), -frequency)
    cos_h, sin_h = jnp.cos(heading), jnp.sin(heading)
    west, east = jnp.maximum(courant * cos_h, 0.0), jnp.maximum(-courant * cos_h, 0.0)
    south, north = jnp.maximum(courant * sin_h, 0.0), jnp.maximum(-courant * sin_h, 0.0)
    center = 1.0 - west - east - south - north
    coef = jnp.stack([center, west, east, south, north, input_rate, cos_h, sin_h], axis=1).reshape(-1)

    lower, upper = edges(spectrum, 1)
    fields = jnp.stack([wind_speed, jnp.cos(wind_dir), jnp.sin(wind_dir), land_mask.astype(F32)])
    low_f, high_f = edges(fields, 1)
    fields = jnp.concatenate([low_f, fields, high_f], axis=1)
    wind, mask = fields[:3], fields[3]

    whole_tiles = local % (16 * SENDS) == 0
    sends = SENDS if whole_tiles else 1
    part = local // sends
    density, chunks = [], []
    for k in range(sends):
        cut = slice(k * part, (k + 1) * part)
        d, out = propagate(coef[k * part * 8 : (k + 1) * part * 8], lower[cut], spectrum[cut], upper[cut], mask)
        density.append(d)
        out = out.reshape(peers, band, part, cols)
        chunks.append(lax.all_to_all(out, "comp", split_axis=0, concat_axis=0, tiled=True))
    density = jnp.concatenate(density, axis=0)

    loss = dissipation[:, None]
    if not whole_tiles:
        chunks = [c.transpose(1, 0, 2, 3).reshape(1, band, peers * local, cols) for c in chunks]
    returns = max(1, min(RETURNS, band // 2))
    pairs = band // 2 // returns
    incs = []
    for k in range(returns):
        inc = point_terms(chunks, k * pairs, pairs, loss, pair_first, pair_second, merge_weight)
        if not whole_tiles:
            inc = inc.reshape(2 * pairs, peers, local, cols).transpose(1, 0, 2, 3)
        incs.append(lax.all_to_all(inc, "comp", split_axis=0, concat_axis=0, tiled=True))
    count = lax.axis_size("geo")
    ends = count - 1
    low = lax.ppermute(incs[0][peers - 1, 1], "geo", [(i, i + 1) for i in range(ends)])
    high = lax.ppermute(incs[0][0, 0], "geo", [(i + 1, i) for i in range(ends)])
    low = jnp.pad(low.astype(F32)[:, None], ((0, 0), (HALO - 1, 0), (0, 0)))
    high = jnp.pad(high.astype(F32)[:, None], ((0, 0), (0, HALO - 1), (0, 0)))
    return finish(coef, density, low, high, wind, mask, incs, HALO)


def geo_halo_kernel(
    spectrum, mask, speed, angle, held, near, near_mask, near_speed, near_angle, seas, send, recv, sea_send, sea_recv
):
    geo, ends = lax.axis_index("geo"), lax.axis_size("geo") - 1
    rows = spectrum.shape[1]
    barrier = pltpu.get_barrier_semaphore()
    has_low, has_high = geo > 0, geo < ends
    others = [lax.rem(geo + k, ends + 1) for k in range(1, ends + 1)]
    for who in others:
        pl.semaphore_signal(barrier, inc=1, device_id={"geo": who}, device_id_type=MESH)
    pl.semaphore_wait(barrier, ends)

    def most(k):
        return pltpu.make_async_remote_copy(
            src_ref=held, dst_ref=seas.at[geo], send_sem=sea_send.at[k], recv_sem=sea_recv.at[k],
            device_id={"geo": others[k]}, device_id_type=MESH,
        )

    def copies(side):
        at = pl.ds(0, HALO) if side else pl.ds(rows - HALO, HALO)
        to = {"geo": geo - 1} if side else {"geo": geo + 1}
        pairs = [
            (spectrum.at[:, at], near.at[side]),
            (mask.at[at], near_mask.at[side]),
            (speed.at[at], near_speed.at[side]),
            (angle.at[at], near_angle.at[side]),
        ]
        return [
            pltpu.make_async_remote_copy(
                src_ref=src, dst_ref=dst, send_sem=send.at[side, k], recv_sem=recv.at[side, k],
                device_id=to, device_id_type=MESH,
            )
            for k, (src, dst) in enumerate(pairs)
        ]

    down, up = copies(1), copies(0)

    @pl.when(has_low)
    def _():
        for c in down:
            c.start()

    @pl.when(has_high)
    def _():
        for c in up:
            c.start()

    for k in range(ends):
        most(k).start()
    own = pltpu.make_async_copy(held, seas.at[geo], sea_send.at[ends])
    own.start()

    for side, missing in ((0, geo == 0), (1, geo == ends)):

        @pl.when(missing)
        def _(side=side):
            for ref in (near, near_mask, near_speed, near_angle):
                ref[side] = jnp.zeros(ref.shape[1:], ref.dtype)

    @pl.when(has_low)
    def _():
        for c in down:
            c.wait_send()
        for c in up:
            c.wait_recv()

    @pl.when(has_high)
    def _():
        for c in up:
            c.wait_send()
        for c in down:
            c.wait_recv()

    for k in range(ends):
        most(k).wait()
    own.wait()


def geo_halo(spectrum, mask, speed, angle, held):
    comps, _, cols = spectrum.shape
    count = lax.axis_size("geo")
    flat = lambda a: jax.ShapeDtypeStruct((2, HALO, cols), a.dtype)
    seas = jax.ShapeDtypeStruct((count,) + held.shape, held.dtype)
    return pl.pallas_call(
        geo_halo_kernel,
        in_specs=[ANY] * 5,
        out_specs=[WHOLE] * 5,
        out_shape=[jax.ShapeDtypeStruct((2, comps, HALO, cols), spectrum.dtype), flat(mask), flat(speed), flat(angle), seas],
        scratch_shapes=[DMA((2, 4)), DMA((2, 4)), DMA((count,)), DMA((count,))],
        compiler_params=pltpu.CompilerParams(collective_id=1, has_side_effects=True),
        name="geo_halo",
    )(spectrum, mask, speed, angle, held)


def directions(comps, periodic):
    if not periodic:
        return True, True, True, True
    cos = [math.cos(2 * math.pi * c / ND) for c in comps]
    sin = [math.sin(2 * math.pi * c / ND) for c in comps]
    tiny = 1e-3
    south = any(s > -tiny and c % ND for s, c in zip(sin, comps))
    north = any(s < tiny and c % ND for s, c in zip(sin, comps))
    return any(c > -tiny for c in cos), any(c < tiny for c in cos), south, north


def column_terms(x, w, e, west, east):
    cols = x.shape[1]
    if west and east:
        return w * pltpu.roll(x, 1, 1) + e * pltpu.roll(x, cols - 1, 1)
    return w * pltpu.roll(x, 1, 1) if west else e * pltpu.roll(x, cols - 1, 1)


def group_sets(comps, periodic, limit):
    groups = comps // 8
    count = max(k for k in range(1, limit + 1) if groups % k == 0)
    sets = [list(range(k * count, (k + 1) * count)) for k in range(groups // count)]
    ways = [directions([8 * g + k for k in range(8)], periodic) for g in range(groups)]
    return sets, ways


def substeps(field, work, done, mask, coef, side, group_set, ways, top, base_of, done_at, stride):
    factor = {g: [coef[k, pl.ds(g * 8, 8), :] for k in range(5)] for g in group_set}
    size = len(group_set)
    plans = []
    for p in range(PROP_STEPS):
        trim = RUN // 2 if p >= PROP_STEPS - 2 else 0
        source = (field, base_of) if p == 0 else (work[(p - 1) % 2], 1)
        target = (done, done_at - trim) if p == PROP_STEPS - 1 else (work[p % 2], 1)
        plans.append((source, target, trim, (SPAN - 2 * trim) // RUN))

    def at(base, row, g):
        return pl.ds(pl.multiple_of((base + row) * stride + g * 8, 8), 8)

    def ahead(source, row):
        ref, base = source
        made = []
        for r in range(RUN):
            for g in group_set:
                west, east = ways[g][:2]
                made.append(column_terms(ref[at(base, row + r, g), :], factor[g][1], factor[g][2], west, east))
        return made

    def keep(made):
        for k, v in enumerate(made):
            side[k] = v

    def finish(source, target, row):
        ref, base = source
        out, out_base = target
        for j, g in enumerate(group_set):
            c, _, _, s, n = factor[g]
            south, north = ways[g][2:]
            held = ref[at(base, row - 1, g), :] if south else None
            here = ref[at(base, row, g), :]
            for r in range(RUN):
                after = ref[at(base, row + r + 1, g), :] if north or r < RUN - 1 else None
                v = c * here + side[r * size + j]
                if south:
                    v = v + s * held
                if north:
                    v = v + n * after
                out[at(out_base, row + r, g), :] = v * mask[top + row + r]
                held, here = here, after

    keep(ahead(plans[0][0], plans[0][2]))
    for p, (source, target, trim, trips) in enumerate(plans):

        def trip(t, carry, source=source, target=target, trim=trim):
            row = trim + t * RUN
            made = ahead(source, row + RUN)
            finish(source, target, row)
            keep(made)
            return carry

        lax.fori_loop(0, trips - 1, trip, 0)
        row = trim + (trips - 1) * RUN
        made = ahead(plans[p + 1][0], plans[p + 1][2]) if p + 1 < PROP_STEPS else None
        finish(source, target, row)
        if made is not None:
            keep(made)


class TurnIn:
    def __init__(self, spectrum, near, staged, field, sems, stride, side):
        self.spectrum, self.near, self.staged, self.field, self.sems = spectrum, near, staged, field, sems
        self.stride, self.side = stride, side
        comps, rows, _ = spectrum.shape
        slots, self.block = staged.shape[:2]
        self.blocks = comps // self.block
        self.begin, self.count = (SPAN - HALO, rows + HALO - SPAN) if side else (0, SPAN - HALO)
        self.per = 1 if side else rows // SPAN
        self.live = min(self.blocks, slots * self.per)

    def place(self, b):
        turn = lax.rem(b, self.live)
        return lax.div(turn, self.per), pl.multiple_of(lax.rem(turn, self.per) * SPAN, SPAN)

    def fetch(self, b):
        slot, row = self.place(b)
        return pltpu.make_async_copy(
            self.spectrum.at[pl.ds(b * self.block, self.block), pl.ds(self.begin, self.count)],
            self.staged.at[slot, :, pl.ds(row, self.count)],
            self.sems.at[lax.rem(b, self.live)],
        )

    def start(self):
        for b in range(self.live):
            self.fetch(b).start()

    def finish(self):
        side, stride, count = self.side, self.stride, self.count
        rows, cols = self.spectrum.shape[1:]
        to = SPAN + 1 if side else 1
        zeros = jnp.zeros((stride, cols), F32)
        for row in (rows + 2 * HALO + 1,) if side else (0, SPAN + 1):
            self.field[pl.ds(row * stride, stride), :] = zeros

        def turn(b, carry):
            self.fetch(b).wait()
            slot, row = self.place(b)

            def one(k, carry):
                c = b * self.block + k
                inner = self.staged[slot, k, pl.ds(row, count), :].astype(F32)
                outer = self.near[side, c].astype(F32)
                v = jnp.concatenate([inner, outer] if side else [outer, inner], axis=0)
                self.field[pl.ds(to * stride + c, count + HALO, stride=stride), :] = v
                return carry

            lax.fori_loop(0, self.block, one, 0)
            if self.live < self.blocks:

                @pl.when(b + self.live < self.blocks)
                def _():
                    self.fetch(b + self.live).start()

            return carry

        lax.fori_loop(0, self.blocks, turn, 0)


def spread_rows(to, first, rows_of):
    cols = rows_of.shape[1]

    count = rows_of.shape[0]
    unroll = max(k for k in range(1, 17) if count % k == 0)

    def several(t, carry):
        for u in range(unroll):
            i = t * unroll + u
            to[first + i] = jnp.broadcast_to(rows_of[pl.ds(i, 1), :].astype(F32), (8, cols))
        return carry

    lax.fori_loop(0, count // unroll, several, 0)


def find_places(land, near_land, places, edge_places):
    rows, cols = land.shape
    sea = land[...].astype(F32)
    i = lax.broadcasted_iota(jnp.int32, (rows, rows), 0)
    j = lax.broadcasted_iota(jnp.int32, (rows, rows), 1)
    same = lax.shift_right_logical(i, 4) == lax.shift_right_logical(j, 4)
    sooner = jnp.where(i >= rows - BAND, i - j, j - i) < 0
    before = jnp.where(jnp.logical_and(same, sooner), 1.0, 0.0).astype(BF16)
    k = lax.broadcasted_iota(jnp.int32, (cols, cols), 0)
    n = lax.broadcasted_iota(jnp.int32, (cols, cols), 1)
    steps = jnp.where(k <= n, 1.0, 0.0).astype(BF16)
    inner = jnp.dot(sea.astype(BF16), steps, preferred_element_type=F32)
    held = jnp.dot(before, sea.astype(BF16), preferred_element_type=F32).astype(BF16)
    ahead = jnp.dot(held, jnp.ones((cols, cols), BF16), preferred_element_type=F32)
    places[...] = jnp.where(sea > 0, inner + ahead - 1.0, -1.0).astype(jnp.int32)
    for side in range(2):
        sea = near_land[side].astype(F32)
        inner = jnp.dot(sea.astype(BF16), steps, preferred_element_type=F32)
        edge_places[side] = jnp.where(sea > 0, inner - 1.0, -1.0).astype(jnp.int32)


def band_at(k, bands):
    return jnp.where(k == 0, 0, jnp.where(k == 1, bands - 1, k - 1))


def partner(me, k, peers):
    if peers & (peers - 1):
        return lax.rem(me + k, peers)
    other, bit = me, 1
    while bit < peers:
        if k & bit:
            other = other + bit - 2 * bit * lax.rem(lax.div(other, bit), 2)
        bit *= 2
    return other


def one_hot(pos, first, count):
    cols = pos.shape[1]
    slot = lax.broadcasted_iota(jnp.int32, (count, cols), 0) + first
    return jnp.where(slot == jnp.broadcast_to(pos, (count, cols)), 1.0, 0.0).astype(BF16)


def squeeze_block(rows_of, places, row_at, factor, tiles, start, peers):
    count, _, cols = rows_of.shape
    for n in range(0, TILES, 2):
        wide = min(2, TILES - n)
        lanes = slice(n * cols, count * cols)
        for q in range(n, count):
            factor[: wide * cols, q * cols : (q + 1) * cols] = one_hot(
                places[pl.ds(row_at(q), 1), :], n * cols, wide * cols
            )
        x = jnp.concatenate([rows_of[q] for q in range(n, count)], axis=1)
        moved = lax.dot_general(
            x, factor[: wide * cols, lanes], (((1,), (1,)), ((), ())), preferred_element_type=F32
        ).astype(BF16)
        for h in range(wide):
            t = start + n + h
            tiles[lax.div(t, peers), lax.rem(t, peers)] = moved[:, h * cols : (h + 1) * cols]


def widen_rows(tiles, start, peers, places, row_at, first, count, factor):
    cols = factor.shape[1] // 2
    reach = min(first + count, TILES)
    for n in range(reach):
        for q in range(count):
            factor[n * cols : (n + 1) * cols, q * cols : (q + 1) * cols] = one_hot(
                places[pl.ds(row_at(first + q), 1), :], n * cols, cols
            )
    x = []
    for n in range(reach):
        t = start + n
        x.append(tiles[lax.div(t, peers), lax.rem(t, peers)])
    x = jnp.concatenate(x, axis=1) if reach > 1 else x[0]
    return jnp.dot(x, factor[: reach * cols, : count * cols], preferred_element_type=F32).astype(BF16)


def advance_kernel(
    order, periodic, squeeze, spectrum, near, land, near_land, coef, loss, first_in, second_in, merge_in, *refs
):
    density, back, edge, *refs = refs
    mask, staged, field, work_a, work_b, done, side, tiles, spectra, incs, first, second, merge, merge_part, product, *refs = refs
    if squeeze:
        places, edge_places, rows_of, home, edge_in, edge_out, flat, gather, spread, flat_sems, *refs = refs
    else:
        home = back
    stage_sems, density_sems, end_sems, weight_sems, send_sem, recv_sem, return_sem, back_sem, edge_send, edge_recv = refs
    peers = lax.axis_size("comp")
    me = lax.axis_index("comp")
    geo, ends = lax.axis_index("geo"), lax.axis_size("geo") - 1
    chunks, width, comps, cols = spectra.shape
    local = comps // peers
    terms = product.shape[0]
    has_low, has_high = geo > 0, geo < ends

    barrier = pltpu.get_barrier_semaphore()
    for k in range(1, peers):
        pl.semaphore_signal(barrier, inc=1, device_id={"comp": partner(me, k, peers)}, device_id_type=MESH)

    @pl.when(has_low)
    def _():
        pl.semaphore_signal(barrier, inc=1, device_id={"geo": geo - 1}, device_id_type=MESH)

    @pl.when(has_high)
    def _():
        pl.semaphore_signal(barrier, inc=1, device_id={"geo": geo + 1}, device_id_type=MESH)

    def part(who):
        return pl.ds(pl.multiple_of(who * local, 16), local)

    def outward(c, who):
        return pltpu.make_async_remote_copy(
            src_ref=tiles.at[pl.ds(c * width, width), who],
            dst_ref=spectra.at[c, :, part(me)],
            send_sem=send_sem, recv_sem=recv_sem.at[c],
            device_id={"comp": who}, device_id_type=MESH,
        )

    def homeward(c, who):
        return pltpu.make_async_remote_copy(
            src_ref=incs.at[c, :, part(who)],
            dst_ref=home.at[pl.ds(c * width, width), me],
            send_sem=return_sem, recv_sem=back_sem.at[c],
            device_id={"comp": who}, device_id_type=MESH,
        )

    def own_home(c):
        return pltpu.make_async_copy(incs.at[c, :, part(me)], back.at[pl.ds(c * width, width), me], back_sem.at[c])

    loads = [
        pltpu.make_async_copy(src, dst, weight_sems.at[k])
        for k, (src, dst) in enumerate(((first_in, first), (second_in, second)))
    ]
    rows = land.shape[0]
    stride = stride_of(local) + 8
    bands = rows // BAND
    opening = TurnIn(spectrum, near, staged, field, stage_sems, stride, 0)
    others = TurnIn(spectrum, near, staged, field, stage_sems, stride, 1)
    opening.start()
    spread_rows(mask, 0, near_land.at[0])
    spread_rows(mask, HALO, land)
    spread_rows(mask, rows + HALO, near_land.at[1])
    if squeeze:
        find_places(land, near_land, places, edge_places)
    opening.finish()
    others.start()
    zeros = jnp.zeros((stride, cols), F32)
    for work in (work_a, work_b):
        work[pl.ds(0, stride), :] = zeros
        work[pl.ds((SPAN + 1) * stride, stride), :] = zeros
    pl.semaphore_wait(barrier, peers - 1 + jnp.minimum(geo, 1) + jnp.minimum(ends - geo, 1))

    sets, ways = group_sets(local, periodic, 9)

    def whole(k):
        return pltpu.make_async_copy(
            done.at[pl.ds(OFF * stride, BAND * stride)],
            density.at[pl.ds((band_at(k, bands) * BAND + 1) * stride, BAND * stride)],
            density_sems.at[k],
        )

    def end(far):
        row = rows + 1 if far else 0
        return pltpu.make_async_copy(
            done.at[pl.ds((BAND + OFF if far else OFF - 1) * stride, stride)],
            density.at[pl.ds(row * stride, stride)],
            end_sems.at[far],
        )

    far_band = min(1, bands - 1)

    def settle(k):
        whole(k).wait()

        @pl.when(k == 0)
        def _():
            end(0).wait()

        @pl.when(k == far_band)
        def _():
            end(1).wait()

    def ready(k):
        return lax.div(k * (rows // bands * TILES // BLOCK if squeeze else BAND), peers * width)

    def needed(k):
        return lax.div(k * (BAND // BLOCK * TILES) + peers * width - 1, peers * width)

    def form(k, carry):
        band = band_at(k, bands)

        @pl.when(k > 0)
        def _():
            settle(k - 1)

        @pl.when(k == 1)
        def _():
            others.finish()
            for load in loads:
                load.start()

        for group_set in sets:
            substeps(
                field, (work_a, work_b), done, mask, coef, side, group_set, ways,
                band * BAND, band * BAND + 1, 0, stride,
            )
        whole(k).start()

        @pl.when(k == 0)
        def _():
            end(0).start()

        @pl.when(k == far_band)
        def _():
            end(1).start()

        if squeeze:

            def block(b, carry):
                def row_at(q):
                    r = b * BLOCK + q
                    return jnp.where(k == 1, BAND - 1 - r, r)

                def pack(q, carry):
                    from_at = pl.multiple_of((OFF + row_at(q)) * stride, 8)
                    rows_of[q] = done[pl.ds(from_at, local), :].astype(BF16)
                    return carry

                lax.fori_loop(0, BLOCK, pack, 0)
                squeeze_block(
                    rows_of, places, lambda q: band * BAND + row_at(q), gather, tiles,
                    (k * (BAND // BLOCK) + b) * TILES, peers,
                )
                return carry

            lax.fori_loop(0, BAND // BLOCK, block, 0)
        else:

            def pack(r, carry):
                t = k * BAND + r
                from_at = pl.multiple_of((OFF + r) * stride, 8)
                tiles[lax.div(t, peers), lax.rem(t, peers)] = done[pl.ds(from_at, local), :].astype(BF16)
                return carry

            lax.fori_loop(0, BAND, pack, 0)

        for group in order:

            def launch(c, carry, group=group):
                for who in group:
                    outward(c, partner(me, who, peers)).start()
                return carry

            lax.fori_loop(ready(k), ready(k + 1), launch, 0)

        def own(c, carry):
            for h in range(width):
                spectra[c, h, part(me), :] = tiles[c * width + h, me]
            return carry

        lax.fori_loop(ready(k), ready(k + 1), own, 0)
        return carry

    lax.fori_loop(0, bands, form, 0)

    def fetch(m):
        slot = lax.rem(m, 2)
        return pltpu.make_async_copy(
            merge_in.at[:, pl.ds(pl.multiple_of(m * cols, cols), cols)], merge_part.at[slot], weight_sems.at[2 + slot]
        )

    fetch(0).start()

    def flip(m, carry):
        @pl.when(m + 1 < comps // cols)
        def _():
            fetch(m + 1).start()

        fetch(m).wait()
        to = pl.ds(pl.multiple_of(m * cols, cols), cols)
        for t in range(0, terms, cols):
            size = min(cols, terms - t)
            merge[to, t : t + size] = merge_part[lax.rem(m, 2), t : t + size, :].T
        return carry

    lax.fori_loop(0, comps // cols, flip, 0)
    for load in loads:
        load.wait()

    tile = max(t for t in range(16, 600, 16) if terms % t == 0)
    step = max(g for g in range(1, peers + 1) if peers % g == 0 and g * local <= 600) * local

    def work(c, carry):
        arrived = spectra.at[c, :, pl.ds(0, comps - local)]
        pltpu.make_async_copy(arrived, arrived, recv_sem.at[c]).wait()

        def multiply(t, carry):
            at = pl.ds(pl.multiple_of(t * tile, 16), tile)
            x = jnp.concatenate([spectra[c, h] for h in range(width)], axis=1) if width > 1 else spectra[c, 0]
            one = jnp.dot(first[at, :], x, preferred_element_type=F32)
            two = jnp.dot(second[at, :], x, preferred_element_type=F32)
            product[at, :] = (one * two).astype(BF16)
            return carry

        lax.fori_loop(0, terms // tile, multiply, 0)
        roots = []
        for h in range(width):
            energy = jnp.sum(spectra[c, h].astype(F32), axis=0, keepdims=True)
            roots.append(jnp.sqrt(energy / comps + 1e-06))
        for d in range(0, comps, step):
            at = slice(d, d + step)
            moved = jnp.dot(merge[at, :], product[...], preferred_element_type=F32)
            for h in range(width):
                lanes = slice(h * cols, (h + 1) * cols)
                total = moved[:, lanes] - loss[at, :] * roots[h] * spectra[c, h, at, :].astype(F32)
                incs[c, h, at, :] = total.astype(BF16)
        for group in order:
            for k in group:
                homeward(c, partner(me, k, peers)).start()
        if squeeze:
            for h in range(width):
                home[c * width + h, me] = incs[c, h, part(me), :]
        else:
            own_home(c).start()
        return carry

    lax.fori_loop(0, chunks, work, 0)

    def land(c, carry):
        there = home.at[pl.ds(c * width, width), pl.ds(0, peers - 1 if squeeze else peers)]
        pltpu.make_async_copy(there, there, back_sem.at[c]).wait()
        return carry

    if squeeze:
        last = BAND // BLOCK * TILES
    else:
        last = min(2, bands) * BAND - 1
    landed = last // (peers * width) + 1
    lax.fori_loop(0, landed, land, 0)
    arriving = edge_in if squeeze else edge
    to_low = pltpu.make_async_remote_copy(
        src_ref=home.at[0, 0], dst_ref=arriving.at[1], send_sem=edge_send.at[1], recv_sem=edge_recv.at[1],
        device_id={"geo": geo - 1}, device_id_type=MESH,
    )
    to_high = pltpu.make_async_remote_copy(
        src_ref=home.at[last // peers, last % peers], dst_ref=arriving.at[0],
        send_sem=edge_send.at[0], recv_sem=edge_recv.at[0],
        device_id={"geo": geo + 1}, device_id_type=MESH,
    )

    @pl.when(has_low)
    def _():
        to_low.start()

    @pl.when(has_high)
    def _():
        to_high.start()

    if not squeeze:
        lax.fori_loop(landed, chunks, land, 0)
    settle(bands - 1)

    def edges_in():
        @pl.when(has_low)
        def _():
            to_low.wait_send()
            to_high.wait_recv()

        @pl.when(has_high)
        def _():
            to_high.wait_send()
            to_low.wait_recv()

    if squeeze:

        def put(k):
            return pltpu.make_async_copy(
                flat.at[lax.rem(k, 2)], back.at[pl.ds(k * BAND, BAND)], flat_sems.at[k]
            )

        def widen(k, carry):
            lax.fori_loop(jnp.maximum(needed(k), landed), jnp.maximum(needed(k + 1), landed), land, 0)

            @pl.when(k >= 2)
            def _():
                put(k - 2).wait()

            def block(b, carry):
                def row_at(q):
                    r = b * BLOCK + q
                    return jnp.where(k == 1, BAND - 1 - r, r)

                for j in range(0, BLOCK, 2):
                    made = widen_rows(
                        home, (k * (BAND // BLOCK) + b) * TILES, peers, places,
                        lambda q: band_at(k, bands) * BAND + row_at(q), j, 2, spread,
                    )
                    for h in range(2):
                        flat[lax.rem(k, 2), row_at(j + h)] = made[:, h * cols : (h + 1) * cols]
                return carry

            lax.fori_loop(0, BAND // BLOCK, block, 0)
            put(k).start()
            return carry

        def edge_put(which):
            return pltpu.make_async_copy(edge_out.at[which], edge.at[which], end_sems.at[which])

        @pl.when(geo == 0)
        def _():
            edge_in[0] = jnp.zeros((local, cols), BF16)

        @pl.when(geo == ends)
        def _():
            edge_in[1] = jnp.zeros((local, cols), BF16)

        lax.fori_loop(0, bands - 1, widen, 0)
        edges_in()
        for which in range(2):
            row = 0 if which else HALO - 1
            spread[:cols, :cols] = one_hot(edge_places[which, row : row + 1, :], 0, cols)
            edge_out[which] = jnp.dot(
                edge_in[which], spread[:cols, :cols], preferred_element_type=F32
            ).astype(BF16)
            edge_put(which).start()
        lax.fori_loop(bands - 1, bands, widen, 0)
        for k in range(bands - 2, bands):
            put(k).wait()
        for which in range(2):
            edge_put(which).wait()
    else:
        edges_in()

    def sent(c, carry):
        for k in range(1, peers):
            outward(c, partner(me, k, peers)).wait_send()
            homeward(c, partner(me, k, peers)).wait_send()
        return carry

    lax.fori_loop(0, chunks, sent, 0)


def advance(squeeze, periodic, spectrum, near, land, near_land, coef, loss, first, second, merge):
    local, rows, cols = spectrum.shape
    peers = lax.axis_size("comp")
    width = 1 if squeeze else CHUNK
    depth = (rows // BLOCK * TILES if squeeze else rows) // peers
    chunks = depth // width
    comps, terms = merge.shape
    stride = stride_of(local) + 8
    if peers == 8:
        order = [(1, 2, 3), (4, 5, 6, 7)]
    else:
        order = [tuple(range(1, peers))]
    slots = -(-(local // 16) // (rows // SPAN))
    sets, _ = group_sets(local, periodic, 9)
    extra = []
    if squeeze:
        extra = [
            VMEM((rows, cols), jnp.int32),
            VMEM((2, HALO, cols), jnp.int32),
            VMEM((BLOCK, local, cols), BF16),
            VMEM((depth, peers, local, cols), BF16),
            VMEM((2, local, cols), BF16),
            VMEM((2, local, cols), BF16),
            VMEM((2, BAND, local, cols), BF16),
            VMEM((2 * cols, BLOCK * cols), BF16),
            VMEM((TILES * cols, 2 * cols), BF16),
            DMA((rows // BAND,)),
        ]
    back_shape = (rows, local, cols) if squeeze else (depth, peers, local, cols)
    density, back, edge = pl.pallas_call(
        functools.partial(advance_kernel, order, periodic, squeeze),
        in_specs=[ANY, WHOLE, WHOLE, WHOLE, WHOLE, WHOLE, ANY, ANY, ANY],
        out_specs=[ANY, ANY, ANY],
        out_shape=[
            jax.ShapeDtypeStruct(((rows + 2) * stride, cols), F32),
            jax.ShapeDtypeStruct(back_shape, BF16),
            jax.ShapeDtypeStruct((2, local, cols), BF16),
        ],
        scratch_shapes=[
            VMEM((rows + 2 * HALO, 8, cols), F32),
            VMEM((slots, 16, rows, cols), BF16),
            VMEM(((rows + 2 * HALO + 2) * stride, cols), F32),
            VMEM(((SPAN + 2) * stride, cols), F32),
            VMEM(((SPAN + 2) * stride, cols), F32),
            VMEM(((SPAN - RUN) * stride, cols), F32),
            VMEM((RUN * len(sets[0]), 8, cols), F32),
            VMEM((depth, peers, local, cols), BF16),
            VMEM((chunks, width, comps, cols), BF16),
            VMEM((chunks, width, comps, cols), BF16),
            VMEM((terms, comps), BF16),
            VMEM((terms, comps), BF16),
            VMEM((comps, terms), BF16),
            VMEM((2, terms, cols), BF16),
            VMEM((terms, width * cols), BF16),
        ]
        + extra
        + [
            DMA((max(slots, local // 16),)),
            DMA((rows // BAND,)),
            DMA((2,)),
            DMA((4,)),
            DMA,
            DMA((chunks,)),
            DMA,
            DMA((chunks,)),
            DMA((2,)),
            DMA((2,)),
        ],
        cost_estimate=pl.CostEstimate(
            flops=6 * comps * terms * depth * cols, bytes_accessed=6 * comps * terms, transcendentals=0
        ),
        compiler_params=pltpu.CompilerParams(
            collective_id=3 if squeeze else 2, has_side_effects=True, vmem_limit_bytes=67043328
        ),
        name="advance_sea" if squeeze else "advance_all",
    )(spectrum, near, land, near_land, coef, loss, first, second, merge.T)
    return density, back.reshape(rows, local, cols), edge


def close_kernel(
    periodic, density, back, edge, speed, near_speed, angle, near_angle, land, near_land, coef, out,
    mask, wind, lines, cells, forced, turned, incs, side, staged, sems, out_sems,
):
    comps, rows, cols = staged.shape
    stride = stride_of(comps) + 8
    sets, ways = group_sets(comps, periodic, 6)
    size = len(sets[0])
    bands = rows // BAND
    views = [ref.reshape(rows + 2, stride, cols) for ref in (density, cells)]

    def fetches(b):
        at = pl.ds(sets[b][0] * 8, size * 8)
        moves = [
            (views[0].at[:, at], views[1].at[:, at]),
            (edge.at[0, at], incs.at[0, at]),
            (back.at[pl.ds(0, BAND), at], incs.at[pl.ds(1, BAND), at]),
            (edge.at[1, at], incs.at[rows + 1, at]),
        ]
        if bands > 1:
            moves.append((back.at[pl.ds(BAND, BAND), at], incs.at[pl.ds(rows + 1 - BAND, BAND), at]))
        if bands > 2:
            between = rows - 2 * BAND
            moves.append((back.at[pl.ds(2 * BAND, between), at], incs.at[pl.ds(1 + BAND, between), at]))
        return [pltpu.make_async_copy(src, dst, sems.at[b, k]) for k, (src, dst) in enumerate(moves)]

    for b in range(len(sets)):
        for f in fetches(b):
            f.start()

    def surround(kind, middle, near, change):
        for first, ref in ((0, near.at[0]), (HALO, middle), (rows + HALO, near.at[1])):
            lines[pl.ds(first, ref.shape[0]), :] = change(ref[...].astype(F32))
        spread_rows(kind, 0, lines.at[pl.ds(HALO - 1, rows + 2)])

    surround(mask, land, near_land, lambda v: v)
    surround(wind.at[0], speed, near_speed, lambda v: v)
    surround(wind.at[1], angle, near_angle, jnp.cos)
    surround(wind.at[2], angle, near_angle, jnp.sin)
    geo = lax.axis_index("geo")

    run = max(k for k in range(1, 17) if (rows + 2) % k == 0)
    trips = (rows + 2) // run

    def at(row, g):
        return pl.ds(pl.multiple_of(row * stride + g * 8, 8), 8)

    def set_of(b):
        group_set = sets[b]
        for f in fetches(b):
            f.wait()
        span = pl.ds(group_set[0] * 8, size * 8)
        for end, row in ((0, 0), (lax.axis_size("geo") - 1, rows + 1)):

            @pl.when(geo == end)
            def _(row=row):
                incs[row, span, :] = jnp.zeros((size * 8, cols), BF16)

        factor = {g: [coef[k, pl.ds(g * 8, 8), :] for k in range(8)] for g in group_set}

        def ahead(row):
            made = []
            for r in range(run):
                blow, turn_x, turn_y = wind[0, row + r], wind[1, row + r], wind[2, row + r]
                for g in group_set:
                    if g % 2 == 0:
                        both = incs[row + r, pl.ds(g * 8, 16), :].astype(F32)
                    rate, cos_h, sin_h = factor[g][5:8]
                    d = cells[at(row + r, g), :]
                    facing = jnp.maximum(cos_h * turn_x + sin_h * turn_y, 0.0)
                    growth = rate * blow * (facing * facing)
                    new = d + growth * d + both[(g % 2) * 8 : (g % 2) * 8 + 8]
                    forced[at(row + r + 1, g), :] = new
                    west, east = ways[g][:2]
                    made.append(column_terms(new, factor[g][1], factor[g][2], west, east))
            return made

        def keep(made):
            for k, v in enumerate(made):
                side[k] = v

        def finish(row):
            for j, g in enumerate(group_set):
                c, _, _, s, n = factor[g][:5]
                south, north = ways[g][2:]
                held = forced[at(row, g), :] if south else None
                here = forced[at(row + 1, g), :]
                for r in range(run):
                    after = forced[at(row + r + 2, g), :] if north or r < run - 1 else None
                    v = c * here + side[r * size + j]
                    if south:
                        v = v + s * held
                    if north:
                        v = v + n * after
                    turned[at(row + r, g), :] = v * mask[row + r]
                    held, here = here, after

        def trip(t, carry):
            made = ahead((t + 1) * run)
            finish(t * run)
            keep(made)
            return carry

        keep(ahead(0))
        lax.fori_loop(0, trips - 1, trip, 0)
        finish((trips - 1) * run)

    def give(b):
        part = pl.ds(b * size * 8, size * 8)
        return pltpu.make_async_copy(staged.at[part], out.at[part], out_sems.at[b])

    zeros = jnp.zeros((stride, cols), F32)
    forced[pl.ds(0, stride), :] = zeros
    forced[pl.ds((rows + 3) * stride, stride), :] = zeros
    for b in range(len(sets)):
        set_of(b)

        def lift(k, carry, b=b):
            c = b * size * 8 + k
            staged[c] = turned[pl.ds(stride + c, rows, stride=stride), :].astype(BF16)
            return carry

        lax.fori_loop(0, size * 8, lift, 0)
        give(b).start()
    for b in range(len(sets)):
        give(b).wait()


def close(periodic, density, back, edge, *fields):
    rows, comps, cols = back.shape
    stride = stride_of(comps) + 8
    sets, _ = group_sets(comps, periodic, 6)
    run = max(k for k in range(1, 17) if (rows + 2) % k == 0)
    return pl.pallas_call(
        functools.partial(close_kernel, periodic),
        in_specs=[ANY] * 3 + [WHOLE] * len(fields),
        out_specs=ANY,
        out_shape=jax.ShapeDtypeStruct((comps, rows, cols), BF16),
        scratch_shapes=[
            VMEM((rows + 2, 8, cols), F32),
            VMEM((3, rows + 2, 8, cols), F32),
            VMEM((rows + 2 * HALO, cols), F32),
            VMEM(((rows + 2) * stride, cols), F32),
            VMEM(((rows + 4) * stride, cols), F32),
            VMEM(((rows + 2) * stride, cols), F32),
            VMEM((rows + 2, comps, cols), BF16),
            VMEM((run * len(sets[0]), 8, cols), F32),
            VMEM((comps, rows, cols), BF16),
            DMA((len(sets), 6)),
            DMA((len(sets),)),
        ],
        compiler_params=pltpu.CompilerParams(vmem_limit_bytes=56 * 1024 * 1024),
        name="close",
    )(density, back, edge, *fields)


def body(spectrum, land_mask, wind_speed, wind_dir, input_rate, dissipation, pair_first, pair_second, merge_weight):
    local, rows, cols = spectrum.shape
    peers = lax.axis_size("comp")
    fits = local % 16 == 0 and rows % BAND == 0 and BAND % (peers * CHUNK) == 0 and cols == 128
    if not fits:
        return plain_body(
            spectrum, land_mask, wind_speed, wind_dir, input_rate, dissipation, pair_first, pair_second, merge_weight
        )
    periodic = local % ND == 0
    held = jnp.max(jnp.sum(land_mask.reshape(-1, min(BLOCK, rows) * cols), axis=1))
    held = jnp.broadcast_to(held, (8, cols))
    near, near_mask, near_speed, near_angle, seas = geo_halo(spectrum, land_mask, wind_speed, wind_dir, held)

    ids = lax.axis_index("comp") * local + jnp.arange(local, dtype=jnp.int32)
    frequency = (ids // ND).astype(F32)
    heading = 2.0 * math.pi * (ids % ND).astype(F32) / ND
    courant = 0.7 * jnp.power(F32(1.1), -frequency)
    cos_h, sin_h = jnp.cos(heading), jnp.sin(heading)
    west, east = jnp.maximum(courant * cos_h, 0.0), jnp.maximum(-courant * cos_h, 0.0)
    south, north = jnp.maximum(courant * sin_h, 0.0), jnp.maximum(-courant * sin_h, 0.0)
    center = 1.0 - west - east - south - north
    coef = jnp.stack([center, west, east, south, north, input_rate, cos_h, sin_h])
    coef = jnp.broadcast_to(coef[:, :, None], (8, local, cols))

    given = (
        spectrum, near, land_mask, near_mask, coef, dissipation[:, None], pair_first, pair_second, merge_weight
    )
    whole = functools.partial(advance, False, periodic)
    packed = functools.partial(advance, True, periodic)
    if rows >= 2 * BAND and rows // BLOCK * TILES % peers == 0:
        density, back, edge = lax.cond(jnp.max(seas) <= TILES * cols, packed, whole, *given)
    else:
        density, back, edge = whole(*given)
    return close(
        periodic, density, back, edge, wind_speed, near_speed, wind_dir, near_angle, land_mask, near_mask, coef
    )


def solution(mesh):
    placed = (P("comp", "geo", None), P("geo", None), P("geo", None), P("geo", None), P("comp"), P(), P(), P(), P())
    return jax.shard_map(
        body, mesh=mesh, in_specs=placed, out_specs=P("comp", "geo", None), check_vma=False
    )
```

```python
import functools
import math

import jax
import jax.numpy as jnp
from jax import lax
from jax.experimental import pallas as pl
from jax.experimental.pallas import tpu as pltpu
from jax.sharding import PartitionSpec as P

ND = 36
PROP_STEPS = 6
HALO = 8
SENDS = 3
RETURNS = 2
F32 = jnp.float32
BF16 = jnp.bfloat16
VMEM = pltpu.VMEM
ANY = pl.BlockSpec(memory_space=pl.ANY)
WHOLE = pl.BlockSpec(memory_space=pltpu.VMEM)
MESH = pl.DeviceIdType.MESH
DMA = pltpu.SemaphoreType.DMA
CHUNK = 2
BAND = 16
BLOCK = 16
TILES = 13
RUN = 8
SPAN = BAND + 2 * HALO
OFF = HALO - RUN // 2
LAG = 2
SMEM = pltpu.SMEM


def edges(cells, axis_dim):
    count = lax.axis_size("geo")
    ends = count - 1
    size = cells.shape[axis_dim]
    head = lax.slice_in_dim(cells, 0, HALO, axis=axis_dim)
    tail = lax.slice_in_dim(cells, size - HALO, size, axis=axis_dim)
    lower = lax.ppermute(tail, "geo", [(i, i + 1) for i in range(ends)])
    upper = lax.ppermute(head, "geo", [(i + 1, i) for i in range(ends)])
    return lower, upper


def block_of(comps):
    return 16 if comps % 16 == 0 else comps


def stride_of(block):
    return -(-block // 8) * 8


def upwind(v, mask, coef, at):
    center, west, east, south, north = (coef[at + k] for k in range(5))
    rows = v.shape[0]
    moved = west * pltpu.roll(v, 1, 1) + east * pltpu.roll(v, v.shape[1] - 1, 1)
    moved = moved + south * pltpu.roll(v, 1, 0) + north * pltpu.roll(v, rows - 1, 0)
    return (center * v + moved) * mask


def prop_kernel(coef, lower, cells, upper, mask, density, outgoing, turned):
    block, rows, cols = cells.shape
    stride = stride_of(block)
    first = pl.program_id(0) * block

    def one(c, carry):
        v = jnp.concatenate(
            [lower[c].astype(F32), cells[c].astype(F32), upper[c].astype(F32)], axis=0
        )
        sea = mask[...]
        for _ in range(PROP_STEPS):
            v = upwind(v, sea, coef, (first + c) * 8)
        density[c] = v
        turned[pl.ds(c, rows, stride=stride), :] = v[HALO : HALO + rows]
        return carry

    lax.fori_loop(0, block, one, 0)

    def pack(r, carry):
        start = pl.multiple_of(r * stride, 8)
        outgoing[r] = turned[pl.ds(start, block), :].astype(BF16)
        return carry

    lax.fori_loop(0, rows, pack, 0, unroll=8)


def propagate(coef, lower, cells, upper, mask):
    comps, rows, cols = cells.shape
    block = block_of(comps)
    tall = rows + 2 * HALO
    return pl.pallas_call(
        prop_kernel,
        grid=(comps // block,),
        in_specs=[
            pl.BlockSpec(memory_space=SMEM),
            pl.BlockSpec((block, HALO, cols), lambda i: (i, 0, 0)),
            pl.BlockSpec((block, rows, cols), lambda i: (i, 0, 0)),
            pl.BlockSpec((block, HALO, cols), lambda i: (i, 0, 0)),
            pl.BlockSpec((tall, cols), lambda i: (0, 0)),
        ],
        out_specs=[
            pl.BlockSpec((block, tall, cols), lambda i: (i, 0, 0)),
            pl.BlockSpec((rows, block, cols), lambda i: (0, i, 0)),
        ],
        out_shape=[
            jax.ShapeDtypeStruct((comps, tall, cols), F32),
            jax.ShapeDtypeStruct((rows, comps, cols), BF16),
        ],
        scratch_shapes=[VMEM((rows * stride_of(block), cols), F32)],
        cost_estimate=pl.CostEstimate(
            flops=comps * tall * cols * 100,
            bytes_accessed=comps * tall * cols * 8,
            transcendentals=0,
        ),
        name="propagate",
    )(coef, lower, cells, upper, mask)


def point_kernel(sends, *refs):
    near, far = refs[:sends], refs[sends : 2 * sends]
    loss, first, second, merge, out, spectra, product = refs[2 * sends :]
    peers, _, part, cols = near[0].shape
    local = sends * part
    comps, terms = merge.shape
    for side, group in enumerate((near, far)):
        lanes = slice(side * cols, (side + 1) * cols)
        for k in range(sends):
            for s in range(peers):
                at = s * local + k * part
                spectra[at : at + part, lanes] = group[k][s, 0]
    tile = max(t for t in range(16, 600, 16) if terms % t == 0)

    def multiply(t, carry):
        rows = pl.ds(pl.multiple_of(t * tile, 16), tile)
        x = spectra[...]
        one = jnp.dot(first[rows, :], x, preferred_element_type=F32)
        two = jnp.dot(second[rows, :], x, preferred_element_type=F32)
        product[rows, :] = (one * two).astype(BF16)
        return carry

    lax.fori_loop(0, terms // tile, multiply, 0)
    energy = jnp.sum(spectra[...].astype(F32), axis=0, keepdims=True)
    root = jnp.sqrt(energy / comps + 1e-06)
    if peers == 1:
        step = max(t for t in range(16, 600, 16) if comps % t == 0)
        for d in range(0, comps, step):
            rows = slice(d, d + step)
            moved = jnp.dot(merge[rows, :], product[...], preferred_element_type=F32)
            total = moved - loss[rows, :] * root * spectra[rows, :].astype(F32)
            out[0, 0, rows] = total[:, :cols].astype(BF16)
            out[0, 1, rows] = total[:, cols:].astype(BF16)
        return
    share = max(g for g in range(1, peers + 1) if peers % g == 0 and g * local <= 600)
    for d in range(0, peers, share):
        rows = slice(d * local, (d + share) * local)
        moved = jnp.dot(merge[rows, :], product[...], preferred_element_type=F32)
        total = moved - loss[rows, :] * root * spectra[rows, :].astype(F32)
        for g in range(share):
            piece = total[g * local : (g + 1) * local].astype(BF16)
            out[d + g, 0] = piece[:, :cols]
            out[d + g, 1] = piece[:, cols:]


def point_terms(chunks, start, pairs, loss, first, second, merge):
    sends = len(chunks)
    peers, rows, part, cols = chunks[0].shape
    local = sends * part
    comps, terms = merge.shape
    whole = lambda shape: pl.BlockSpec(shape, lambda i: (0, 0))
    near = pl.BlockSpec((peers, 1, part, cols), lambda i: (0, start + i, 0, 0))
    far = pl.BlockSpec((peers, 1, part, cols), lambda i: (0, rows - 1 - start - i, 0, 0))
    return pl.pallas_call(
        functools.partial(point_kernel, sends),
        grid=(pairs,),
        in_specs=[near] * sends
        + [far] * sends
        + [whole((comps, 1)), whole((terms, comps)), whole((terms, comps)), whole((comps, terms))],
        out_specs=pl.BlockSpec((peers, 2, local, cols), lambda i: (0, i, 0, 0)),
        out_shape=jax.ShapeDtypeStruct((peers, 2 * pairs, local, cols), BF16),
        scratch_shapes=[VMEM((comps, 2 * cols), BF16), VMEM((terms, 2 * cols), BF16)],
        cost_estimate=pl.CostEstimate(
            flops=pairs * 12 * comps * terms * cols,
            bytes_accessed=6 * comps * terms + pairs * 8 * comps * cols,
            transcendentals=0,
        ),
        compiler_params=pltpu.CompilerParams(vmem_limit_bytes=60 * 1024 * 1024),
        name="points",
    )(*chunks, *chunks, loss, first, second, merge)


def final_kernel(returns, coef, density, low_inc, high_inc, wind, mask, *refs):
    incs = refs[:returns]
    out, turned = refs[returns:]
    block, rows, cols = out.shape
    peers, held = incs[0].shape[:2]
    band = rows // peers
    stride = stride_of(block)
    first = pl.program_id(0) * block

    def place(s, carry):
        for k in range(returns):
            for j in range(held):
                a = k * (held // 2) + j // 2
                row = a if j % 2 == 0 else band - 1 - a
                at = pl.multiple_of((s * band + row) * stride, 8)
                turned[pl.ds(at, block), :] = incs[k][s, j].astype(F32)
        return carry

    lax.fori_loop(0, peers, place, 0)

    def one(c, carry):
        at = (first + c) * 8
        inc = jnp.concatenate(
            [low_inc[c], turned[pl.ds(c, rows, stride=stride), :], high_inc[c]], axis=0
        )
        v = density[c]
        facing = jnp.maximum(coef[at + 6] * wind[1] + coef[at + 7] * wind[2], 0.0)
        growth = coef[at + 5] * wind[0] * facing * facing
        v = v + growth * v + inc
        v = upwind(v, mask[...], coef, at)
        out[c] = v[HALO : HALO + rows].astype(BF16)
        return carry

    lax.fori_loop(0, block, one, 0)


def finish(coef, density, low_inc, high_inc, wind, mask, incs, lead):
    local, tall, cols = density.shape
    rows = tall - 2 * HALO
    block = block_of(local)
    peers, held = incs[0].shape[:2]
    return pl.pallas_call(
        functools.partial(final_kernel, len(incs)),
        grid=(local // block,),
        in_specs=[
            pl.BlockSpec(memory_space=SMEM),
            pl.BlockSpec((block, tall, cols), lambda i: (i, 0, 0)),
            pl.BlockSpec((block, HALO, cols), lambda i: (i, 0, 0)),
            pl.BlockSpec((block, HALO, cols), lambda i: (i, 0, 0)),
            pl.BlockSpec((3, tall, cols), lambda i: (0, 0, 0)),
            pl.BlockSpec((tall, cols), lambda i: (0, 0)),
        ]
        + [pl.BlockSpec((peers, held, block, cols), lambda i: (0, 0, i, 0))] * len(incs),
        out_specs=pl.BlockSpec((block, rows, cols), lambda i: (i, 0, 0)),
        out_shape=jax.ShapeDtypeStruct((local, rows, cols), BF16),
        scratch_shapes=[VMEM((rows * stride_of(block), cols), F32)],
        name="finish",
    )(coef, density, low_inc, high_inc, wind, mask, *incs)


def plain_body(spectrum, land_mask, wind_speed, wind_dir, input_rate, dissipation, pair_first, pair_second, merge_weight):
    local, rows, cols = spectrum.shape
    peers = lax.axis_size("comp")
    band = rows // peers
    ids = lax.axis_index("comp") * local + jnp.arange(local, dtype=jnp.int32)
    frequency = (ids // ND).astype(F32)
    heading = 2.0 * math.pi * (ids % ND).astype(F32) / ND
    courant = 0.7 * jnp.power(F32(1.1), -frequency)
    cos_h, sin_h = jnp.cos(heading), jnp.sin(heading)
    west, east = jnp.maximum(courant * cos_h, 0.0), jnp.maximum(-courant * cos_h, 0.0)
    south, north = jnp.maximum(courant * sin_h, 0.0), jnp.maximum(-courant * sin_h, 0.0)
    center = 1.0 - west - east - south - north
    coef = jnp.stack([center, west, east, south, north, input_rate, cos_h, sin_h], axis=1).reshape(-1)

    lower, upper = edges(spectrum, 1)
    fields = jnp.stack([wind_speed, jnp.cos(wind_dir), jnp.sin(wind_dir), land_mask.astype(F32)])
    low_f, high_f = edges(fields, 1)
    fields = jnp.concatenate([low_f, fields, high_f], axis=1)
    wind, mask = fields[:3], fields[3]

    whole_tiles = local % (16 * SENDS) == 0
    sends = SENDS if whole_tiles else 1
    part = local // sends
    density, chunks = [], []
    for k in range(sends):
        cut = slice(k * part, (k + 1) * part)
        d, out = propagate(coef[k * part * 8 : (k + 1) * part * 8], lower[cut], spectrum[cut], upper[cut], mask)
        density.append(d)
        out = out.reshape(peers, band, part, cols)
        chunks.append(lax.all_to_all(out, "comp", split_axis=0, concat_axis=0, tiled=True))
    density = jnp.concatenate(density, axis=0)

    loss = dissipation[:, None]
    if not whole_tiles:
        chunks = [c.transpose(1, 0, 2, 3).reshape(1, band, peers * local, cols) for c in chunks]
    returns = max(1, min(RETURNS, band // 2))
    pairs = band // 2 // returns
    incs = []
    for k in range(returns):
        inc = point_terms(chunks, k * pairs, pairs, loss, pair_first, pair_second, merge_weight)
        if not whole_tiles:
            inc = inc.reshape(2 * pairs, peers, local, cols).transpose(1, 0, 2, 3)
        incs.append(lax.all_to_all(inc, "comp", split_axis=0, concat_axis=0, tiled=True))
    count = lax.axis_size("geo")
    ends = count - 1
    low = lax.ppermute(incs[0][peers - 1, 1], "geo", [(i, i + 1) for i in range(ends)])
    high = lax.ppermute(incs[0][0, 0], "geo", [(i + 1, i) for i in range(ends)])
    low = jnp.pad(low.astype(F32)[:, None], ((0, 0), (HALO - 1, 0), (0, 0)))
    high = jnp.pad(high.astype(F32)[:, None], ((0, 0), (0, HALO - 1), (0, 0)))
    return finish(coef, density, low, high, wind, mask, incs, HALO)


def geo_halo_kernel(
    spectrum, mask, speed, angle, held, near, near_mask, near_speed, near_angle, seas, send, recv, sea_send, sea_recv
):
    geo, ends = lax.axis_index("geo"), lax.axis_size("geo") - 1
    rows = spectrum.shape[1]
    barrier = pltpu.get_barrier_semaphore()
    has_low, has_high = geo > 0, geo < ends
    others = [lax.rem(geo + k, ends + 1) for k in range(1, ends + 1)]
    for who in others:
        pl.semaphore_signal(barrier, inc=1, device_id={"geo": who}, device_id_type=MESH)
    pl.semaphore_wait(barrier, ends)

    def most(k):
        return pltpu.make_async_remote_copy(
            src_ref=held, dst_ref=seas.at[geo], send_sem=sea_send.at[k], recv_sem=sea_recv.at[k],
            device_id={"geo": others[k]}, device_id_type=MESH,
        )

    def copies(side):
        at = pl.ds(0, HALO) if side else pl.ds(rows - HALO, HALO)
        to = {"geo": geo - 1} if side else {"geo": geo + 1}
        pairs = [
            (spectrum.at[:, at], near.at[side]),
            (mask.at[at], near_mask.at[side]),
            (speed.at[at], near_speed.at[side]),
            (angle.at[at], near_angle.at[side]),
        ]
        return [
            pltpu.make_async_remote_copy(
                src_ref=src, dst_ref=dst, send_sem=send.at[side, k], recv_sem=recv.at[side, k],
                device_id=to, device_id_type=MESH,
            )
            for k, (src, dst) in enumerate(pairs)
        ]

    down, up = copies(1), copies(0)

    @pl.when(has_low)
    def _():
        for c in down:
            c.start()

    @pl.when(has_high)
    def _():
        for c in up:
            c.start()

    for k in range(ends):
        most(k).start()
    own = pltpu.make_async_copy(held, seas.at[geo], sea_send.at[ends])
    own.start()

    for side, missing in ((0, geo == 0), (1, geo == ends)):

        @pl.when(missing)
        def _(side=side):
            for ref in (near, near_mask, near_speed, near_angle):
                ref[side] = jnp.zeros(ref.shape[1:], ref.dtype)

    @pl.when(has_low)
    def _():
        for c in down:
            c.wait_send()
        for c in up:
            c.wait_recv()

    @pl.when(has_high)
    def _():
        for c in up:
            c.wait_send()
        for c in down:
            c.wait_recv()

    for k in range(ends):
        most(k).wait()
    own.wait()


def geo_halo(spectrum, mask, speed, angle, held):
    comps, _, cols = spectrum.shape
    count = lax.axis_size("geo")
    flat = lambda a: jax.ShapeDtypeStruct((2, HALO, cols), a.dtype)
    seas = jax.ShapeDtypeStruct((count,) + held.shape, held.dtype)
    return pl.pallas_call(
        geo_halo_kernel,
        in_specs=[ANY] * 5,
        out_specs=[WHOLE] * 5,
        out_shape=[jax.ShapeDtypeStruct((2, comps, HALO, cols), spectrum.dtype), flat(mask), flat(speed), flat(angle), seas],
        scratch_shapes=[DMA((2, 4)), DMA((2, 4)), DMA((count,)), DMA((count,))],
        compiler_params=pltpu.CompilerParams(collective_id=1, has_side_effects=True),
        name="geo_halo",
    )(spectrum, mask, speed, angle, held)


def directions(comps, periodic):
    if not periodic:
        return True, True, True, True
    cos = [math.cos(2 * math.pi * c / ND) for c in comps]
    sin = [math.sin(2 * math.pi * c / ND) for c in comps]
    tiny = 1e-3
    south = any(s > -tiny and c % ND for s, c in zip(sin, comps))
    north = any(s < tiny and c % ND for s, c in zip(sin, comps))
    return any(c > -tiny for c in cos), any(c < tiny for c in cos), south, north


def column_terms(x, w, e, west, east):
    cols = x.shape[1]
    if west and east:
        return w * pltpu.roll(x, 1, 1) + e * pltpu.roll(x, cols - 1, 1)
    return w * pltpu.roll(x, 1, 1) if west else e * pltpu.roll(x, cols - 1, 1)


def group_sets(comps, periodic, limit):
    groups = comps // 8
    count = max(k for k in range(1, limit + 1) if groups % k == 0)
    sets = [list(range(k * count, (k + 1) * count)) for k in range(groups // count)]
    ways = [directions([8 * g + k for k in range(8)], periodic) for g in range(groups)]
    return sets, ways


def substeps(field, work, done, mask, coef, side, group_set, ways, top, base_of, done_at, stride):
    factor = {g: [coef[k, pl.ds(g * 8, 8), :] for k in range(5)] for g in group_set}
    size = len(group_set)
    plans = []
    for p in range(PROP_STEPS):
        trim = RUN // 2 if p >= PROP_STEPS - 2 else 0
        source = (field, base_of) if p == 0 else (work[(p - 1) % 2], 1)
        target = (done, done_at - trim) if p == PROP_STEPS - 1 else (work[p % 2], 1)
        plans.append((source, target, trim, (SPAN - 2 * trim) // RUN))

    def at(base, row, g):
        return pl.ds(pl.multiple_of((base + row) * stride + g * 8, 8), 8)

    def ahead(source, row):
        ref, base = source
        made = []
        for r in range(RUN):
            for g in group_set:
                west, east = ways[g][:2]
                made.append(column_terms(ref[at(base, row + r, g), :], factor[g][1], factor[g][2], west, east))
        return made

    def keep(made):
        for k, v in enumerate(made):
            side[k] = v

    def finish(source, target, row):
        ref, base = source
        out, out_base = target
        for j, g in enumerate(group_set):
            c, _, _, s, n = factor[g]
            south, north = ways[g][2:]
            held = ref[at(base, row - 1, g), :] if south else None
            here = ref[at(base, row, g), :]
            for r in range(RUN):
                after = ref[at(base, row + r + 1, g), :] if north or r < RUN - 1 else None
                v = c * here + side[r * size + j]
                if south:
                    v = v + s * held
                if north:
                    v = v + n * after
                out[at(out_base, row + r, g), :] = v * mask[top + row + r]
                held, here = here, after

    keep(ahead(plans[0][0], plans[0][2]))
    for p, (source, target, trim, trips) in enumerate(plans):

        def trip(t, carry, source=source, target=target, trim=trim):
            row = trim + t * RUN
            made = ahead(source, row + RUN)
            finish(source, target, row)
            keep(made)
            return carry

        lax.fori_loop(0, trips - 1, trip, 0)
        row = trim + (trips - 1) * RUN
        made = ahead(plans[p + 1][0], plans[p + 1][2]) if p + 1 < PROP_STEPS else None
        finish(source, target, row)
        if made is not None:
            keep(made)


class TurnIn:
    def __init__(self, spectrum, near, staged, field, sems, stride, side):
        self.spectrum, self.near, self.staged, self.field, self.sems = spectrum, near, staged, field, sems
        self.stride, self.side = stride, side
        comps, rows, _ = spectrum.shape
        slots, self.block = staged.shape[:2]
        self.blocks = comps // self.block
        self.begin, self.count = (SPAN - HALO, rows + HALO - SPAN) if side else (0, SPAN - HALO)
        self.per = 1 if side else rows // SPAN
        self.live = min(self.blocks, slots * self.per)

    def place(self, b):
        turn = lax.rem(b, self.live)
        return lax.div(turn, self.per), pl.multiple_of(lax.rem(turn, self.per) * SPAN, SPAN)

    def fetch(self, b):
        slot, row = self.place(b)
        return pltpu.make_async_copy(
            self.spectrum.at[pl.ds(b * self.block, self.block), pl.ds(self.begin, self.count)],
            self.staged.at[slot, :, pl.ds(row, self.count)],
            self.sems.at[lax.rem(b, self.live)],
        )

    def start(self):
        for b in range(self.live):
            self.fetch(b).start()

    def finish(self):
        side, stride, count = self.side, self.stride, self.count
        rows, cols = self.spectrum.shape[1:]
        to = SPAN + 1 if side else 1
        zeros = jnp.zeros((stride, cols), F32)
        for row in (rows + 2 * HALO + 1,) if side else (0, SPAN + 1):
            self.field[pl.ds(row * stride, stride), :] = zeros

        def turn(b, carry):
            self.fetch(b).wait()
            slot, row = self.place(b)

            def one(k, carry):
                c = b * self.block + k
                inner = self.staged[slot, k, pl.ds(row, count), :].astype(F32)
                outer = self.near[side, c].astype(F32)
                v = jnp.concatenate([inner, outer] if side else [outer, inner], axis=0)
                self.field[pl.ds(to * stride + c, count + HALO, stride=stride), :] = v
                return carry

            lax.fori_loop(0, self.block, one, 0)
            if self.live < self.blocks:

                @pl.when(b + self.live < self.blocks)
                def _():
                    self.fetch(b + self.live).start()

            return carry

        lax.fori_loop(0, self.blocks, turn, 0)


def spread_rows(to, first, rows_of):
    cols = rows_of.shape[1]

    count = rows_of.shape[0]
    unroll = max(k for k in range(1, 17) if count % k == 0)

    def several(t, carry):
        for u in range(unroll):
            i = t * unroll + u
            to[first + i] = jnp.broadcast_to(rows_of[pl.ds(i, 1), :].astype(F32), (8, cols))
        return carry

    lax.fori_loop(0, count // unroll, several, 0)


def find_places(land, near_land, places, edge_places):
    rows, cols = land.shape
    sea = land[...].astype(F32)
    i = lax.broadcasted_iota(jnp.int32, (rows, rows), 0)
    j = lax.broadcasted_iota(jnp.int32, (rows, rows), 1)
    same = lax.shift_right_logical(i, 4) == lax.shift_right_logical(j, 4)
    sooner = jnp.where(i >= rows - BAND, i - j, j - i) < 0
    before = jnp.where(jnp.logical_and(same, sooner), 1.0, 0.0).astype(BF16)
    k = lax.broadcasted_iota(jnp.int32, (cols, cols), 0)
    n = lax.broadcasted_iota(jnp.int32, (cols, cols), 1)
    steps = jnp.where(k <= n, 1.0, 0.0).astype(BF16)
    inner = jnp.dot(sea.astype(BF16), steps, preferred_element_type=F32)
    held = jnp.dot(before, sea.astype(BF16), preferred_element_type=F32).astype(BF16)
    ahead = jnp.dot(held, jnp.ones((cols, cols), BF16), preferred_element_type=F32)
    places[...] = jnp.where(sea > 0, inner + ahead - 1.0, -1.0).astype(jnp.int32)
    for side in range(2):
        sea = near_land[side].astype(F32)
        inner = jnp.dot(sea.astype(BF16), steps, preferred_element_type=F32)
        edge_places[side] = jnp.where(sea > 0, inner - 1.0, -1.0).astype(jnp.int32)


def band_at(k, bands):
    return jnp.where(k == 0, 0, jnp.where(k == 1, bands - 1, k - 1))


def partner(me, k, peers):
    if peers & (peers - 1):
        return lax.rem(me + k, peers)
    other, bit = me, 1
    while bit < peers:
        if k & bit:
            other = other + bit - 2 * bit * lax.rem(lax.div(other, bit), 2)
        bit *= 2
    return other


def one_hot(pos, first, count):
    cols = pos.shape[1]
    slot = lax.broadcasted_iota(jnp.int32, (count, cols), 0) + first
    return jnp.where(slot == jnp.broadcast_to(pos, (count, cols)), 1.0, 0.0).astype(BF16)


def squeeze_block(rows_of, places, row_at, factor, tiles, start, peers):
    count, _, cols = rows_of.shape
    for n in range(0, TILES, 2):
        wide = min(2, TILES - n)
        lanes = slice(n * cols, count * cols)
        for q in range(n, count):
            factor[: wide * cols, q * cols : (q + 1) * cols] = one_hot(
                places[pl.ds(row_at(q), 1), :], n * cols, wide * cols
            )
        x = jnp.concatenate([rows_of[q] for q in range(n, count)], axis=1)
        moved = lax.dot_general(
            x, factor[: wide * cols, lanes], (((1,), (1,)), ((), ())), preferred_element_type=F32
        ).astype(BF16)
        for h in range(wide):
            t = start + n + h
            tiles[lax.div(t, peers), lax.rem(t, peers)] = moved[:, h * cols : (h + 1) * cols]


def widen_rows(tiles, start, peers, places, row_at, first, count, factor):
    cols = factor.shape[1] // 2
    reach = min(first + count, TILES)
    for n in range(reach):
        for q in range(count):
            factor[n * cols : (n + 1) * cols, q * cols : (q + 1) * cols] = one_hot(
                places[pl.ds(row_at(first + q), 1), :], n * cols, cols
            )
    x = []
    for n in range(reach):
        t = start + n
        x.append(tiles[lax.div(t, peers), lax.rem(t, peers)])
    x = jnp.concatenate(x, axis=1) if reach > 1 else x[0]
    return jnp.dot(x, factor[: reach * cols, : count * cols], preferred_element_type=F32).astype(BF16)


def advance_kernel(
    order, periodic, squeeze, spectrum, near, land, near_land, coef, loss, first_in, second_in, merge_in, *refs
):
    density, back, edge, *refs = refs
    mask, staged, field, work_a, work_b, done, side, tiles, spectra, incs, first, second, merge, merge_part, product, *refs = refs
    if squeeze:
        places, edge_places, rows_of, home, edge_in, edge_out, flat, gather, spread, flat_sems, *refs = refs
    else:
        home = back
    stage_sems, density_sems, end_sems, weight_sems, send_sem, recv_sem, return_sem, back_sem, edge_send, edge_recv = refs
    peers = lax.axis_size("comp")
    me = lax.axis_index("comp")
    geo, ends = lax.axis_index("geo"), lax.axis_size("geo") - 1
    chunks, width, comps, cols = spectra.shape
    local = comps // peers
    terms = product.shape[0]
    has_low, has_high = geo > 0, geo < ends

    barrier = pltpu.get_barrier_semaphore()
    for k in range(1, peers):
        pl.semaphore_signal(barrier, inc=1, device_id={"comp": partner(me, k, peers)}, device_id_type=MESH)

    @pl.when(has_low)
    def _():
        pl.semaphore_signal(barrier, inc=1, device_id={"geo": geo - 1}, device_id_type=MESH)

    @pl.when(has_high)
    def _():
        pl.semaphore_signal(barrier, inc=1, device_id={"geo": geo + 1}, device_id_type=MESH)

    def part(who):
        return pl.ds(pl.multiple_of(who * local, 16), local)

    def outward(c, who):
        return pltpu.make_async_remote_copy(
            src_ref=tiles.at[pl.ds(c * width, width), who],
            dst_ref=spectra.at[c, :, part(me)],
            send_sem=send_sem, recv_sem=recv_sem.at[c],
            device_id={"comp": who}, device_id_type=MESH,
        )

    def homeward(c, who):
        return pltpu.make_async_remote_copy(
            src_ref=incs.at[c, :, part(who)],
            dst_ref=home.at[pl.ds(c * width, width), me],
            send_sem=return_sem, recv_sem=back_sem.at[c],
            device_id={"comp": who}, device_id_type=MESH,
        )

    def own_home(c):
        return pltpu.make_async_copy(incs.at[c, :, part(me)], back.at[pl.ds(c * width, width), me], back_sem.at[c])

    loads = [
        pltpu.make_async_copy(src, dst, weight_sems.at[k])
        for k, (src, dst) in enumerate(((first_in, first), (second_in, second)))
    ]
    rows = land.shape[0]
    stride = stride_of(local) + 8
    bands = rows // BAND
    opening = TurnIn(spectrum, near, staged, field, stage_sems, stride, 0)
    others = TurnIn(spectrum, near, staged, field, stage_sems, stride, 1)
    opening.start()
    spread_rows(mask, 0, near_land.at[0])
    spread_rows(mask, HALO, land)
    spread_rows(mask, rows + HALO, near_land.at[1])
    if squeeze:
        find_places(land, near_land, places, edge_places)
    opening.finish()
    others.start()
    zeros = jnp.zeros((stride, cols), F32)
    for work in (work_a, work_b):
        work[pl.ds(0, stride), :] = zeros
        work[pl.ds((SPAN + 1) * stride, stride), :] = zeros
    pl.semaphore_wait(barrier, peers - 1 + jnp.minimum(geo, 1) + jnp.minimum(ends - geo, 1))

    sets, ways = group_sets(local, periodic, 9)

    def whole(k):
        return pltpu.make_async_copy(
            done.at[pl.ds(OFF * stride, BAND * stride)],
            density.at[pl.ds((band_at(k, bands) * BAND + 1) * stride, BAND * stride)],
            density_sems.at[k],
        )

    def end(far):
        row = rows + 1 if far else 0
        return pltpu.make_async_copy(
            done.at[pl.ds((BAND + OFF if far else OFF - 1) * stride, stride)],
            density.at[pl.ds(row * stride, stride)],
            end_sems.at[far],
        )

    far_band = min(1, bands - 1)

    def settle(k):
        whole(k).wait()

        @pl.when(k == 0)
        def _():
            end(0).wait()

        @pl.when(k == far_band)
        def _():
            end(1).wait()

    def ready(k):
        return lax.div(k * (rows // bands * TILES // BLOCK if squeeze else BAND), peers * width)

    def needed(k):
        return lax.div(k * (BAND // BLOCK * TILES) + peers * width - 1, peers * width)

    def fetch(m):
        slot = lax.rem(m, 2)
        return pltpu.make_async_copy(
            merge_in.at[:, pl.ds(pl.multiple_of(m * cols, cols), cols)], merge_part.at[slot], weight_sems.at[2 + slot]
        )

    def flip(m, carry):
        @pl.when(m + 1 < comps // cols)
        def _():
            fetch(m + 1).start()

        fetch(m).wait()
        to = pl.ds(pl.multiple_of(m * cols, cols), cols)
        for t in range(0, terms, cols):
            size = min(cols, terms - t)
            merge[to, t : t + size] = merge_part[lax.rem(m, 2), t : t + size, :].T
        return carry

    def weights():
        fetch(0).start()
        lax.fori_loop(0, comps // cols, flip, 0)
        for load in loads:
            load.wait()

    tile = max(t for t in range(16, 600, 16) if terms % t == 0)
    step = max(g for g in range(1, peers + 1) if peers % g == 0 and g * local <= 600) * local

    def work(c, carry):
        arrived = spectra.at[c, :, pl.ds(0, comps - local)]
        pltpu.make_async_copy(arrived, arrived, recv_sem.at[c]).wait()

        def multiply(t, carry):
            at = pl.ds(pl.multiple_of(t * tile, 16), tile)
            x = jnp.concatenate([spectra[c, h] for h in range(width)], axis=1) if width > 1 else spectra[c, 0]
            one = jnp.dot(first[at, :], x, preferred_element_type=F32)
            two = jnp.dot(second[at, :], x, preferred_element_type=F32)
            product[at, :] = (one * two).astype(BF16)
            return carry

        lax.fori_loop(0, terms // tile, multiply, 0)
        roots = []
        for h in range(width):
            energy = jnp.sum(spectra[c, h].astype(F32), axis=0, keepdims=True)
            roots.append(jnp.sqrt(energy / comps + 1e-06))
        for d in range(0, comps, step):
            at = slice(d, d + step)
            moved = jnp.dot(merge[at, :], product[...], preferred_element_type=F32)
            for h in range(width):
                lanes = slice(h * cols, (h + 1) * cols)
                total = moved[:, lanes] - loss[at, :] * roots[h] * spectra[c, h, at, :].astype(F32)
                incs[c, h, at, :] = total.astype(BF16)
        for group in order:
            for k in group:
                homeward(c, partner(me, k, peers)).start()
        if squeeze:
            for h in range(width):
                home[c * width + h, me] = incs[c, h, part(me), :]
        else:
            own_home(c).start()
        return carry

    def form(k, carry):
        band = band_at(k, bands)

        @pl.when(k > 0)
        def _():
            settle(k - 1)

        @pl.when(k == 1)
        def _():
            others.finish()
            for load in loads:
                load.start()

        for group_set in sets:
            substeps(
                field, (work_a, work_b), done, mask, coef, side, group_set, ways,
                band * BAND, band * BAND + 1, 0, stride,
            )
        whole(k).start()

        @pl.when(k == 0)
        def _():
            end(0).start()

        @pl.when(k == far_band)
        def _():
            end(1).start()

        if squeeze:

            def block(b, carry):
                def row_at(q):
                    r = b * BLOCK + q
                    return jnp.where(k == 1, BAND - 1 - r, r)

                def pack(q, carry):
                    from_at = pl.multiple_of((OFF + row_at(q)) * stride, 8)
                    rows_of[q] = done[pl.ds(from_at, local), :].astype(BF16)
                    return carry

                lax.fori_loop(0, BLOCK, pack, 0)
                squeeze_block(
                    rows_of, places, lambda q: band * BAND + row_at(q), gather, tiles,
                    (k * (BAND // BLOCK) + b) * TILES, peers,
                )
                return carry

            lax.fori_loop(0, BAND // BLOCK, block, 0)
        else:

            def pack(r, carry):
                t = k * BAND + r
                from_at = pl.multiple_of((OFF + r) * stride, 8)
                tiles[lax.div(t, peers), lax.rem(t, peers)] = done[pl.ds(from_at, local), :].astype(BF16)
                return carry

            lax.fori_loop(0, BAND, pack, 0)

        for group in order:

            def launch(c, carry, group=group):
                for who in group:
                    outward(c, partner(me, who, peers)).start()
                return carry

            lax.fori_loop(ready(k), ready(k + 1), launch, 0)

        def own(c, carry):
            for h in range(width):
                spectra[c, h, part(me), :] = tiles[c * width + h, me]
            return carry

        lax.fori_loop(ready(k), ready(k + 1), own, 0)

        @pl.when(k == LAG)
        def _():
            weights()

        lax.fori_loop(ready(jnp.maximum(k - LAG, 0)), ready(jnp.maximum(k - LAG + 1, 0)), work, 0)
        return carry

    lax.fori_loop(0, bands, form, 0)
    if bands <= LAG:
        weights()

    lax.fori_loop(ready(max(bands - LAG, 0)), chunks, work, 0)

    def land(c, carry):
        there = home.at[pl.ds(c * width, width), pl.ds(0, peers - 1 if squeeze else peers)]
        pltpu.make_async_copy(there, there, back_sem.at[c]).wait()
        return carry

    if squeeze:
        last = BAND // BLOCK * TILES
    else:
        last = min(2, bands) * BAND - 1
    landed = last // (peers * width) + 1
    lax.fori_loop(0, landed, land, 0)
    arriving = edge_in if squeeze else edge
    to_low = pltpu.make_async_remote_copy(
        src_ref=home.at[0, 0], dst_ref=arriving.at[1], send_sem=edge_send.at[1], recv_sem=edge_recv.at[1],
        device_id={"geo": geo - 1}, device_id_type=MESH,
    )
    to_high = pltpu.make_async_remote_copy(
        src_ref=home.at[last // peers, last % peers], dst_ref=arriving.at[0],
        send_sem=edge_send.at[0], recv_sem=edge_recv.at[0],
        device_id={"geo": geo + 1}, device_id_type=MESH,
    )

    @pl.when(has_low)
    def _():
        to_low.start()

    @pl.when(has_high)
    def _():
        to_high.start()

    if not squeeze:
        lax.fori_loop(landed, chunks, land, 0)
    settle(bands - 1)

    def edges_in():
        @pl.when(has_low)
        def _():
            to_low.wait_send()
            to_high.wait_recv()

        @pl.when(has_high)
        def _():
            to_high.wait_send()
            to_low.wait_recv()

    if squeeze:

        def put(k):
            return pltpu.make_async_copy(
                flat.at[lax.rem(k, 2)], back.at[pl.ds(k * BAND, BAND)], flat_sems.at[k]
            )

        def widen(k, carry):
            lax.fori_loop(jnp.maximum(needed(k), landed), jnp.maximum(needed(k + 1), landed), land, 0)

            @pl.when(k >= 2)
            def _():
                put(k - 2).wait()

            def block(b, carry):
                def row_at(q):
                    r = b * BLOCK + q
                    return jnp.where(k == 1, BAND - 1 - r, r)

                for j in range(0, BLOCK, 2):
                    made = widen_rows(
                        home, (k * (BAND // BLOCK) + b) * TILES, peers, places,
                        lambda q: band_at(k, bands) * BAND + row_at(q), j, 2, spread,
                    )
                    for h in range(2):
                        flat[lax.rem(k, 2), row_at(j + h)] = made[:, h * cols : (h + 1) * cols]
                return carry

            lax.fori_loop(0, BAND // BLOCK, block, 0)
            put(k).start()
            return carry

        def edge_put(which):
            return pltpu.make_async_copy(edge_out.at[which], edge.at[which], end_sems.at[which])

        @pl.when(geo == 0)
        def _():
            edge_in[0] = jnp.zeros((local, cols), BF16)

        @pl.when(geo == ends)
        def _():
            edge_in[1] = jnp.zeros((local, cols), BF16)

        lax.fori_loop(0, bands - 1, widen, 0)
        edges_in()
        for which in range(2):
            row = 0 if which else HALO - 1
            spread[:cols, :cols] = one_hot(edge_places[which, row : row + 1, :], 0, cols)
            edge_out[which] = jnp.dot(
                edge_in[which], spread[:cols, :cols], preferred_element_type=F32
            ).astype(BF16)
            edge_put(which).start()
        lax.fori_loop(bands - 1, bands, widen, 0)
        for k in range(bands - 2, bands):
            put(k).wait()
        for which in range(2):
            edge_put(which).wait()
    else:
        edges_in()

    def sent(c, carry):
        for k in range(1, peers):
            outward(c, partner(me, k, peers)).wait_send()
            homeward(c, partner(me, k, peers)).wait_send()
        return carry

    lax.fori_loop(0, chunks, sent, 0)


def advance(squeeze, periodic, spectrum, near, land, near_land, coef, loss, first, second, merge):
    local, rows, cols = spectrum.shape
    peers = lax.axis_size("comp")
    width = 1 if squeeze else CHUNK
    depth = (rows // BLOCK * TILES if squeeze else rows) // peers
    chunks = depth // width
    comps, terms = merge.shape
    stride = stride_of(local) + 8
    if peers == 8:
        order = [(1, 2, 3), (4, 5, 6, 7)]
    else:
        order = [tuple(range(1, peers))]
    slots = -(-(local // 16) // (rows // SPAN))
    sets, _ = group_sets(local, periodic, 9)
    extra = []
    if squeeze:
        extra = [
            VMEM((rows, cols), jnp.int32),
            VMEM((2, HALO, cols), jnp.int32),
            VMEM((BLOCK, local, cols), BF16),
            VMEM((depth, peers, local, cols), BF16),
            VMEM((2, local, cols), BF16),
            VMEM((2, local, cols), BF16),
            VMEM((2, BAND, local, cols), BF16),
            VMEM((2 * cols, BLOCK * cols), BF16),
            VMEM((TILES * cols, 2 * cols), BF16),
            DMA((rows // BAND,)),
        ]
    back_shape = (rows, local, cols) if squeeze else (depth, peers, local, cols)
    density, back, edge = pl.pallas_call(
        functools.partial(advance_kernel, order, periodic, squeeze),
        in_specs=[ANY, WHOLE, WHOLE, WHOLE, WHOLE, WHOLE, ANY, ANY, ANY],
        out_specs=[ANY, ANY, ANY],
        out_shape=[
            jax.ShapeDtypeStruct(((rows + 2) * stride, cols), F32),
            jax.ShapeDtypeStruct(back_shape, BF16),
            jax.ShapeDtypeStruct((2, local, cols), BF16),
        ],
        scratch_shapes=[
            VMEM((rows + 2 * HALO, 8, cols), F32),
            VMEM((slots, 16, rows, cols), BF16),
            VMEM(((rows + 2 * HALO + 2) * stride, cols), F32),
            VMEM(((SPAN + 2) * stride, cols), F32),
            VMEM(((SPAN + 2) * stride, cols), F32),
            VMEM(((SPAN - RUN) * stride, cols), F32),
            VMEM((RUN * len(sets[0]), 8, cols), F32),
            VMEM((depth, peers, local, cols), BF16),
            VMEM((chunks, width, comps, cols), BF16),
            VMEM((chunks, width, comps, cols), BF16),
            VMEM((terms, comps), BF16),
            VMEM((terms, comps), BF16),
            VMEM((comps, terms), BF16),
            VMEM((2, terms, cols), BF16),
            VMEM((terms, width * cols), BF16),
        ]
        + extra
        + [
            DMA((max(slots, local // 16),)),
            DMA((rows // BAND,)),
            DMA((2,)),
            DMA((4,)),
            DMA,
            DMA((chunks,)),
            DMA,
            DMA((chunks,)),
            DMA((2,)),
            DMA((2,)),
        ],
        cost_estimate=pl.CostEstimate(
            flops=6 * comps * terms * depth * cols, bytes_accessed=6 * comps * terms, transcendentals=0
        ),
        compiler_params=pltpu.CompilerParams(
            collective_id=3 if squeeze else 2, has_side_effects=True, vmem_limit_bytes=67043328
        ),
        name="advance_sea" if squeeze else "advance_all",
    )(spectrum, near, land, near_land, coef, loss, first, second, merge.T)
    return density, back.reshape(rows, local, cols), edge


def close_kernel(
    periodic, density, back, edge, speed, near_speed, angle, near_angle, land, near_land, coef, out,
    mask, wind, lines, cells, forced, turned, incs, side, staged, sems, out_sems,
):
    comps, rows, cols = staged.shape
    stride = stride_of(comps) + 8
    sets, ways = group_sets(comps, periodic, 6)
    size = len(sets[0])
    bands = rows // BAND
    views = [ref.reshape(rows + 2, stride, cols) for ref in (density, cells)]

    def fetches(b):
        at = pl.ds(sets[b][0] * 8, size * 8)
        moves = [
            (views[0].at[:, at], views[1].at[:, at]),
            (edge.at[0, at], incs.at[0, at]),
            (back.at[pl.ds(0, BAND), at], incs.at[pl.ds(1, BAND), at]),
            (edge.at[1, at], incs.at[rows + 1, at]),
        ]
        if bands > 1:
            moves.append((back.at[pl.ds(BAND, BAND), at], incs.at[pl.ds(rows + 1 - BAND, BAND), at]))
        if bands > 2:
            between = rows - 2 * BAND
            moves.append((back.at[pl.ds(2 * BAND, between), at], incs.at[pl.ds(1 + BAND, between), at]))
        return [pltpu.make_async_copy(src, dst, sems.at[b, k]) for k, (src, dst) in enumerate(moves)]

    for b in range(len(sets)):
        for f in fetches(b):
            f.start()

    def surround(kind, middle, near, change):
        for first, ref in ((0, near.at[0]), (HALO, middle), (rows + HALO, near.at[1])):
            lines[pl.ds(first, ref.shape[0]), :] = change(ref[...].astype(F32))
        spread_rows(kind, 0, lines.at[pl.ds(HALO - 1, rows + 2)])

    surround(mask, land, near_land, lambda v: v)
    surround(wind.at[0], speed, near_speed, lambda v: v)
    surround(wind.at[1], angle, near_angle, jnp.cos)
    surround(wind.at[2], angle, near_angle, jnp.sin)
    geo = lax.axis_index("geo")

    run = max(k for k in range(1, 17) if (rows + 2) % k == 0)
    trips = (rows + 2) // run

    def at(row, g):
        return pl.ds(pl.multiple_of(row * stride + g * 8, 8), 8)

    def set_of(b):
        group_set = sets[b]
        for f in fetches(b):
            f.wait()
        span = pl.ds(group_set[0] * 8, size * 8)
        for end, row in ((0, 0), (lax.axis_size("geo") - 1, rows + 1)):

            @pl.when(geo == end)
            def _(row=row):
                incs[row, span, :] = jnp.zeros((size * 8, cols), BF16)

        factor = {g: [coef[k, pl.ds(g * 8, 8), :] for k in range(8)] for g in group_set}

        def ahead(row):
            made = []
            for r in range(run):
                blow, turn_x, turn_y = wind[0, row + r], wind[1, row + r], wind[2, row + r]
                for g in group_set:
                    if g % 2 == 0:
                        both = incs[row + r, pl.ds(g * 8, 16), :].astype(F32)
                    rate, cos_h, sin_h = factor[g][5:8]
                    d = cells[at(row + r, g), :]
                    facing = jnp.maximum(cos_h * turn_x + sin_h * turn_y, 0.0)
                    growth = rate * blow * (facing * facing)
                    new = d + growth * d + both[(g % 2) * 8 : (g % 2) * 8 + 8]
                    forced[at(row + r + 1, g), :] = new
                    west, east = ways[g][:2]
                    made.append(column_terms(new, factor[g][1], factor[g][2], west, east))
            return made

        def keep(made):
            for k, v in enumerate(made):
                side[k] = v

        def finish(row):
            for j, g in enumerate(group_set):
                c, _, _, s, n = factor[g][:5]
                south, north = ways[g][2:]
                held = forced[at(row, g), :] if south else None
                here = forced[at(row + 1, g), :]
                for r in range(run):
                    after = forced[at(row + r + 2, g), :] if north or r < run - 1 else None
                    v = c * here + side[r * size + j]
                    if south:
                        v = v + s * held
                    if north:
                        v = v + n * after
                    turned[at(row + r, g), :] = v * mask[row + r]
                    held, here = here, after

        def trip(t, carry):
            made = ahead((t + 1) * run)
            finish(t * run)
            keep(made)
            return carry

        keep(ahead(0))
        lax.fori_loop(0, trips - 1, trip, 0)
        finish((trips - 1) * run)

    def give(b):
        part = pl.ds(b * size * 8, size * 8)
        return pltpu.make_async_copy(staged.at[part], out.at[part], out_sems.at[b])

    zeros = jnp.zeros((stride, cols), F32)
    forced[pl.ds(0, stride), :] = zeros
    forced[pl.ds((rows + 3) * stride, stride), :] = zeros
    for b in range(len(sets)):
        set_of(b)

        def lift(k, carry, b=b):
            c = b * size * 8 + k
            staged[c] = turned[pl.ds(stride + c, rows, stride=stride), :].astype(BF16)
            return carry

        lax.fori_loop(0, size * 8, lift, 0)
        give(b).start()
    for b in range(len(sets)):
        give(b).wait()


def close(periodic, density, back, edge, *fields):
    rows, comps, cols = back.shape
    stride = stride_of(comps) + 8
    sets, _ = group_sets(comps, periodic, 6)
    run = max(k for k in range(1, 17) if (rows + 2) % k == 0)
    return pl.pallas_call(
        functools.partial(close_kernel, periodic),
        in_specs=[ANY] * 3 + [WHOLE] * len(fields),
        out_specs=ANY,
        out_shape=jax.ShapeDtypeStruct((comps, rows, cols), BF16),
        scratch_shapes=[
            VMEM((rows + 2, 8, cols), F32),
            VMEM((3, rows + 2, 8, cols), F32),
            VMEM((rows + 2 * HALO, cols), F32),
            VMEM(((rows + 2) * stride, cols), F32),
            VMEM(((rows + 4) * stride, cols), F32),
            VMEM(((rows + 2) * stride, cols), F32),
            VMEM((rows + 2, comps, cols), BF16),
            VMEM((run * len(sets[0]), 8, cols), F32),
            VMEM((comps, rows, cols), BF16),
            DMA((len(sets), 6)),
            DMA((len(sets),)),
        ],
        compiler_params=pltpu.CompilerParams(vmem_limit_bytes=56 * 1024 * 1024),
        name="close",
    )(density, back, edge, *fields)


def body(spectrum, land_mask, wind_speed, wind_dir, input_rate, dissipation, pair_first, pair_second, merge_weight):
    local, rows, cols = spectrum.shape
    peers = lax.axis_size("comp")
    fits = local % 16 == 0 and rows % BAND == 0 and rows >= 2 * BAND and BAND % (peers * CHUNK) == 0 and cols == 128
    if not fits:
        return plain_body(
            spectrum, land_mask, wind_speed, wind_dir, input_rate, dissipation, pair_first, pair_second, merge_weight
        )
    periodic = local % ND == 0
    held = jnp.max(jnp.sum(land_mask.reshape(-1, min(BLOCK, rows) * cols), axis=1))
    held = jnp.broadcast_to(held, (8, cols))
    near, near_mask, near_speed, near_angle, seas = geo_halo(spectrum, land_mask, wind_speed, wind_dir, held)

    ids = lax.axis_index("comp") * local + jnp.arange(local, dtype=jnp.int32)
    frequency = (ids // ND).astype(F32)
    heading = 2.0 * math.pi * (ids % ND).astype(F32) / ND
    courant = 0.7 * jnp.power(F32(1.1), -frequency)
    cos_h, sin_h = jnp.cos(heading), jnp.sin(heading)
    west, east = jnp.maximum(courant * cos_h, 0.0), jnp.maximum(-courant * cos_h, 0.0)
    south, north = jnp.maximum(courant * sin_h, 0.0), jnp.maximum(-courant * sin_h, 0.0)
    center = 1.0 - west - east - south - north
    coef = jnp.stack([center, west, east, south, north, input_rate, cos_h, sin_h])
    coef = jnp.broadcast_to(coef[:, :, None], (8, local, cols))

    given = (
        spectrum, near, land_mask, near_mask, coef, dissipation[:, None], pair_first, pair_second, merge_weight
    )
    whole = functools.partial(advance, False, periodic)
    packed = functools.partial(advance, True, periodic)
    if rows >= 2 * BAND and rows // BLOCK * TILES % peers == 0:
        density, back, edge = lax.cond(jnp.max(seas) <= TILES * cols, packed, whole, *given)
    else:
        density, back, edge = whole(*given)
    return close(
        periodic, density, back, edge, wind_speed, near_speed, wind_dir, near_angle, land_mask, near_mask, coef
    )


def solution(mesh):
    placed = (P("comp", "geo", None), P("geo", None), P("geo", None), P("geo", None), P("comp"), P(), P(), P(), P())
    return jax.shard_map(
        body, mesh=mesh, in_specs=placed, out_specs=P("comp", "geo", None), check_vma=False
    )
```
